32 devices in a mesh: grp: 2 (over y), dec: 4 (over z), stg: 2 (over x), tp: 2 (over core).
Axes of the slice: x: 2, y: 2, z: 4, core: 2. Of those that a mesh axis runs over, the one named last changes fastest.
Arguments:
- hidden_x: bfloat16 [3072, 7168], P(('grp', 'dec'), ('stg', 'tp')), parts along dimension 0, may hold values from -8 to 8
- proj_weight: bfloat16 [7168, 2112], P(('stg', 'tp'), 'dec'), may hold values from -0.0625 to 0.0625
- q_gain: float32 [1536], replicated, may hold values from 0.25 to 1.75
- kv_gain: float32 [512], replicated, may hold values from 0.25 to 1.75
- old_cache: bfloat16 [256, 32, 576], P(('grp', 'dec')), parts along dimension 0, may hold values from -6 to 6
- page_plan: int32 [96, 2], P(('grp', 'dec')), parts along dimension 0, may hold values from 0 to 31, as said below
- block_table: int32 [8, 4, 8], P(('grp', 'dec')), parts along dimension 0, may hold values from 0 to 31, as said below
- split_lens: int32 [8, 4], P('grp', 'dec'), parts along dimension 0, may hold values from 2 to 256, as said below
- dec_query: bfloat16 [8, 128, 576], P('grp', ('stg', 'tp')), parts along dimension 0, may hold values from -66 to 66
- new_key: bfloat16 [8, 576], P('grp'), parts along dimension 0, may hold values from -12 to 12
Outputs:
- q_latent: bfloat16 [3072, 1536], P(('grp', 'dec'), ('stg', 'tp')), parts along dimension 0
- attn_latent: bfloat16 [8, 128, 512], P('grp', ('stg', 'tp')), parts along dimension 0
The draws below stay inside these ranges and needn't reach their ends.
There are 2 independent parts, one for each index of `grp`. The reference program is written for one: setup_inputs(seed, part) draws one part's arguments, and reference() takes and returns one part's arrays. A program takes and returns all parts, laid end to end along the dimension named above; an argument that names none is the same for every part. Nothing has to cross between parts.
Inputs may be any that keep to these rules, and one draw needn't show every extreme that they name: `page_plan`: column 0 is the owner of prefill page g, column 1 its slot among the owner's 32; no two pages share owner and slot; in each aligned block of 12 rows (one index of dec) no owner appears more than 3 times and some owner exactly 3 times; no page goes to a slot block_table[o, r, 0]. `block_table`: for each owner the 4 x 8 entries are its 32 slots, each once. `split_lens`: each request has exactly 256 tokens on at least one owner.
All inputs are finite; a program needn't handle non-finite values.
Results may differ from the reference program's by a relative error of at most 0.0054.
Values may be sent and summed in bfloat16 or wider, within the bound.
No kernel may reach another device: no remote copies, remote signals or barrier semaphores. Data moves between devices by JAX's collectives and lax.ppermute only.
A program may use at most 64 MiB of HBM per device.

```python
import jax
import jax.numpy as jnp
from jax import lax

D = 7168
QL = 1536
KVL = 512
ROPE = 64
H = 128
PAGE = 32
REQS = 4
PPR = 8
KVW = 576
PROJ = 2112
TOKENS = 1536
PPS = 12
NPG = 48
CAPP = 3
GROUPS = 4
SLOTS = 32
N_DEC = 4


def plan_tables(key):
    shuffle = jax.random.permutation(jax.random.fold_in(key, 11), N_DEC)

    def block_owners(source):
        shuffled = jax.random.permutation(jax.random.fold_in(jax.random.fold_in(key, 12), source), PPS)
        return shuffle[(source * GROUPS + shuffled // CAPP) % N_DEC]
    owners = jax.vmap(block_owners)(jnp.arange(N_DEC, dtype=jnp.int32)).reshape(NPG)
    onehot = (owners[:, None] == jnp.arange(N_DEC, dtype=jnp.int32)[None, :]).astype(jnp.int32)
    before = jnp.cumsum(onehot, axis=0) - onehot
    arrival = jnp.sum(before * onehot, axis=1)

    def owner_slots(owner):
        return jax.random.permutation(jax.random.fold_in(jax.random.fold_in(key, 13), owner), SLOTS)
    slot_orders = jax.vmap(owner_slots)(jnp.arange(N_DEC, dtype=jnp.int32))
    plan_slots = slot_orders[owners, REQS + arrival]
    page_table = jnp.stack([owners, plan_slots], axis=1).astype(jnp.int32)
    slot_table = jnp.transpose(slot_orders.reshape(N_DEC, PPR, REQS), (0, 2, 1)).astype(jnp.int32)
    longest = PPR * PAGE
    spread = longest - 1
    draw_first = jax.random.randint(jax.random.fold_in(key, 14), (REQS, N_DEC), 0, spread)
    draw_second = jax.random.randint(jax.random.fold_in(key, 15), (REQS, N_DEC), 0, spread)
    length_table = longest - draw_first * draw_second // spread
    longest_owner = jax.random.randint(jax.random.fold_in(key, 16), (REQS,), 0, N_DEC)
    length_table = jnp.where(jnp.arange(N_DEC, dtype=jnp.int32)[None, :] == longest_owner[:, None], longest, length_table)
    return (page_table, slot_table, length_table.astype(jnp.int32))


def draw_page_plan(key, part):
    return plan_tables(key)[0]


def draw_block_table(key, part):
    return plan_tables(key)[1]


def draw_split_lens(key, part):
    return plan_tables(key)[2]


def draw_old_cache(key, part):
    extent = (N_DEC * SLOTS, PAGE, KVW)
    values_out = jnp.clip(jax.random.normal(jax.random.fold_in(key, 21), extent, jnp.float32), -6.0, 6.0)
    return values_out.astype(jnp.bfloat16)


def draw_dec_query(key, part):
    extent = (REQS, H, KVW)
    values_out = jnp.clip(1.5 * jax.random.normal(jax.random.fold_in(key, 31), extent, jnp.float32), -9.0, 9.0)
    return values_out.astype(jnp.bfloat16)


def draw_hidden_x(key, part):
    extent = (TOKENS, D)
    baseline = jnp.clip(jax.random.normal(jax.random.fold_in(key, 41), extent, jnp.float32), -4.0, 4.0)
    row_scale = jnp.exp(jax.random.uniform(jax.random.fold_in(key, 42), (TOKENS,), jnp.float32, -0.69, 0.69))
    return (baseline * row_scale[:, None]).astype(jnp.bfloat16)


def steps_of(stream_key, shape, shards, low, largest):
    level, own = 1.0, jax.random.fold_in(stream_key, 6)
    for dim, shards_of in shards:
        steps = jnp.exp(jax.random.uniform(jax.random.fold_in(own, dim), (shards_of,), jnp.float32, low / len(shards), largest / len(shards)))
        level = level * jnp.repeat(steps, shape[dim] // shards_of).reshape([-1 if axis == dim else 1 for axis in range(len(shape))])
    return level


def gaussian(key, dims, scale, most, shards=(), kind=jnp.bfloat16):
    array = jax.random.normal(key, dims, jnp.float32) * scale
    if len(shards) > 0:
        array = steps_of(key, dims, shards, -0.22, 0.18) * array
    return jnp.clip(array, min=-most, max=most).astype(kind)


def setup_inputs(seed: int = 0, part: int = 0) -> dict:
    arg_keys = jax.random.split(jax.random.key(seed), 11)
    own_keys = jax.random.split(jax.random.fold_in(arg_keys[10], part), 11)
    hidden_x = draw_hidden_x(jax.random.fold_in(jax.random.fold_in(arg_keys[10], part), 71), part)
    proj_weight = gaussian(arg_keys[1], (D, PROJ), D ** -0.5, 0.0625, ((0, 4), (1, 4)))
    q_gain = jnp.clip(1.0 + 0.15 * jax.random.normal(arg_keys[2], (QL,), jnp.float32), 0.25, 1.75)
    kv_gain = jnp.clip(1.0 + 0.15 * jax.random.normal(arg_keys[3], (KVL,), jnp.float32), 0.25, 1.75)
    old_cache = draw_old_cache(jax.random.fold_in(jax.random.fold_in(arg_keys[10], part), 71), part)
    page_plan = draw_page_plan(jax.random.fold_in(jax.random.fold_in(arg_keys[10], part), 71), part)
    block_table = draw_block_table(jax.random.fold_in(jax.random.fold_in(arg_keys[10], part), 71), part)
    split_lens = draw_split_lens(jax.random.fold_in(jax.random.fold_in(arg_keys[10], part), 71), part)
    dec_query = draw_dec_query(jax.random.fold_in(jax.random.fold_in(arg_keys[10], part), 71), part)
    new_key = gaussian(own_keys[9], (REQS, KVW), 2.0, 12.0)
    return {"hidden_x": hidden_x, "proj_weight": proj_weight, "q_gain": q_gain, "kv_gain": kv_gain, "old_cache": old_cache, "page_plan": page_plan, "block_table": block_table, "split_lens": split_lens, "dec_query": dec_query, "new_key": new_key}


softmax_scale = 192.0 ** (-0.5)
norm_eps = 1e-06

def rope_rotate(matrix, col_start, positions):
    col_count = matrix.shape[1]
    columns = col_start + jnp.arange(col_count, dtype=jnp.int32)
    is_rope = columns >= KVL
    pair_index = jnp.maximum(columns - KVL, 0) // 2
    frequency = jnp.power(jnp.float32(10000.0), -(2 * pair_index).astype(jnp.float32) / ROPE)
    angles = positions[:, None] * frequency[None, :]
    cosine = jnp.where(is_rope[None, :], jnp.cos(angles), 1.0)
    sine_part = jnp.where(is_rope[None, :], jnp.sin(angles), 0.0)
    paired = matrix.reshape(matrix.shape[0], col_count // 2, 2)
    partner = jnp.stack([-paired[:, :, 1], paired[:, :, 0]], axis=2).reshape(matrix.shape)
    return matrix * cosine + partner * sine_part

def kv_finish(matrix, col_start, latent_sq, kv_gain, positions):
    col_count = matrix.shape[1]
    columns = col_start + jnp.arange(col_count, dtype=jnp.int32)
    gain_full = jnp.concatenate([kv_gain, jnp.ones((ROPE,), jnp.float32)])
    gain_cols = lax.dynamic_slice_in_dim(gain_full, col_start, col_count)
    inverse = lax.rsqrt(latent_sq / KVL + norm_eps)
    row_scale = jnp.where(columns[None, :] < KVL, inverse[:, None] * gain_cols[None, :], 1.0)
    return rope_rotate(matrix * row_scale, col_start, positions).astype(jnp.bfloat16)

def reference(hidden_x, proj_weight, q_gain, kv_gain, old_cache, page_plan, block_table, split_lens, dec_query, new_key):
    projected = jnp.dot(hidden_x, proj_weight, preferred_element_type=jnp.float32)
    query_part = projected[:, :QL]
    query_sq = lax.optimization_barrier(jnp.sum(query_part * query_part, axis=1))
    q_latent = (query_part * lax.rsqrt(query_sq / QL + norm_eps)[:, None] * q_gain[None, :]).astype(jnp.bfloat16)
    kv_part = projected[:, QL:]
    latent_sq = lax.optimization_barrier(jnp.sum(kv_part[:, :KVL] * kv_part[:, :KVL], axis=1))
    positions = jnp.arange(TOKENS, dtype=jnp.int32).astype(jnp.float32)
    new_rows = kv_finish(kv_part, 0, latent_sq, kv_gain, positions)
    new_pages = new_rows.reshape(NPG, PAGE, KVW)
    targets = page_plan[:, 0] * SLOTS + page_plan[:, 1]
    cache = old_cache.at[targets].set(new_pages)
    query = dec_query.astype(jnp.float32)

    def owner_partial(owner):
        slot_rows = block_table[owner]
        key_rows = cache[owner * SLOTS + slot_rows].reshape(REQS, PPR * PAGE, KVW).astype(jnp.float32)
        scores = jnp.einsum('rhc,rlc->rhl', query, key_rows) * softmax_scale
        live_mask = jnp.arange(PPR * PAGE, dtype=jnp.int32)[None, :] < split_lens[:, owner][:, None]
        scores = jnp.where(live_mask[:, None, :], scores, -1e+30)
        row_peak = lax.optimization_barrier(jnp.max(scores, axis=2))
        weights = jnp.where(live_mask[:, None, :], jnp.exp(scores - row_peak[:, :, None]), 0.0)
        row_total = lax.optimization_barrier(jnp.sum(weights, axis=2))
        rounded = lax.optimization_barrier(weights.astype(jnp.bfloat16)).astype(jnp.float32)
        partial_out = jnp.einsum('rhl,rlc->rhc', rounded, key_rows[:, :, :KVL])
        return (row_peak, row_total, partial_out)
    peaks, totals, partials = lax.map(owner_partial, jnp.arange(N_DEC, dtype=jnp.int32))
    self_score = jnp.einsum('rhc,rc->rh', query, new_key.astype(jnp.float32)) * softmax_scale
    overall = jnp.maximum(lax.optimization_barrier(jnp.max(peaks, axis=0)), self_score)
    factor = jnp.exp(peaks - overall[None])
    self_weight = jnp.exp(self_score - overall)
    denom = lax.optimization_barrier(jnp.sum(totals * factor, axis=0)) + self_weight
    numer = lax.optimization_barrier(jnp.sum(partials * factor[..., None], axis=0)) + self_weight[..., None] * new_key[:, None, :KVL].astype(jnp.float32)
    attn_latent = (numer / denom[..., None]).astype(jnp.bfloat16)
    return (q_latent, attn_latent)
```

```python
import jax
import jax.numpy as jnp
from jax import lax
from jax.sharding import PartitionSpec as P

QL = 1536
KVL = 512
ROPE = 64
PAGE = 32
KVW = KVL + ROPE
MASKED = -1e30
LINE_MAX = 8

softmax_scale = 192.0 ** (-0.5)
norm_eps = 1e-06


def swap(a, axis):
    return lax.ppermute(a, axis, [(0, 1), (1, 0)])


def pick(index, choices):
    out = choices[-1]
    for i in range(len(choices) - 2, -1, -1):
        out = jnp.where(index == i, choices[i], out)
    return out


def gather_small(a, axis):
    n = lax.axis_size(axis)
    return [a] + [lax.ppermute(a, axis, [((i + s) % n, i) for i in range(n)]) for s in range(1, n)]


def line_broadcast(own, source, n, index):
    at = {source: own}
    for step in (-1, 1):
        here, cur = source, own
        while 0 <= here + step < n:
            cur = lax.ppermute(cur, "dec", [(here, here + step)])
            here += step
            at[here] = cur
    return pick(index, [at[i] for i in range(n)])


def spread_weights(weight, pieces, chunks, index, group, groups):
    n = lax.axis_size("dec")
    rows = weight.shape[0] // groups
    mine = lax.dynamic_slice_in_dim(weight, group * rows, rows)
    theirs = lax.dynamic_slice_in_dim(weight, (groups - 1 - group) * rows, rows) if groups > 1 else None
    step = rows // chunks
    out = []
    for c in range(chunks):
        got = []
        for source, lo, hi in pieces:
            block = mine[c * step : (c + 1) * step, lo:hi]
            full = line_broadcast(block, source, n, index)
            if groups > 1:
                pairs = [
                    (g * n + i, (1 - g) * n + i) for g in range(2) for i in range(n) if i != source
                ]
                other = lax.ppermute(full, ("grp", "dec"), pairs)
                other = jnp.where(index == source, theirs[c * step : (c + 1) * step, lo:hi], other)
            else:
                other = None
            got.append((full, other))
        out.append(got)
    return out


def dot32(a, b):
    return jnp.dot(a, b, preferred_element_type=jnp.float32)


def project(hidden_x, weight, index):
    n = lax.axis_size("dec")
    width = weight.shape[1]
    groups = lax.axis_size("grp")
    if n > LINE_MAX or groups > 2:
        full = lax.all_gather(weight, "dec", axis=1, tiled=True)
        projected = dot32(hidden_x, full)
        return projected[:, :QL], projected[:, QL:]
    group = lax.axis_index("grp")
    share = hidden_x.shape[1] // groups
    mine = lax.dynamic_slice_in_dim(hidden_x, group * share, share, axis=1)
    theirs = lax.dynamic_slice_in_dim(hidden_x, (groups - 1 - group) * share, share, axis=1)
    cut = [min(max(QL - b * width, 0), width) for b in range(n)]
    kv_pieces = [(b, cut[b], width) for b in range(n) if cut[b] < width]
    q_pieces = [(b, 0, cut[b]) for b in range(n) if cut[b] > 0]

    def sums(pieces, chunks):
        spread = spread_weights(weight, pieces, chunks, index, group, groups)
        step = share // chunks
        total = [0.0] * len(pieces)
        for c in range(chunks):
            for p in range(len(pieces)):
                full, other = spread[c][p]
                total[p] = total[p] + dot32(mine[:, c * step : (c + 1) * step], full)
                if other is not None:
                    total[p] = total[p] + dot32(theirs[:, c * step : (c + 1) * step], other)
        return total

    kv_sums = sums(kv_pieces, 4)
    q_sums = sums(q_pieces, 2)
    return jnp.concatenate(q_sums, axis=1), jnp.concatenate(kv_sums, axis=1)


def sum_over(a, axis):
    if lax.axis_size(axis) == 2:
        return a + swap(a.astype(jnp.bfloat16), axis).astype(jnp.float32)
    return lax.psum(a, axis)


def scatter_sum(pieces, axis, kind):
    n = lax.axis_size(axis)
    index = lax.axis_index(axis)
    if n == 2:
        away = jnp.where(index == 0, pieces[1], pieces[0]).astype(kind)
        return jnp.where(index == 0, pieces[0], pieces[1]) + swap(away, axis).astype(jnp.float32)
    return lax.psum_scatter(jnp.stack(pieces), axis, scatter_dimension=0, tiled=False)


def exact_sum(a, axis):
    return a + swap(a, axis) if lax.axis_size(axis) == 2 else lax.psum(a, axis)


def kv_finish(raw, positions, kv_gain):
    latent = raw[:, :KVL]
    inverse = lax.rsqrt(jnp.sum(latent * latent, axis=1) / KVL + norm_eps)
    latent = latent * inverse[:, None] * kv_gain[None, :]
    rope = raw[:, KVL:]
    pair = jnp.arange(ROPE, dtype=jnp.int32) // 2
    frequency = jnp.power(jnp.float32(10000.0), -(2 * pair).astype(jnp.float32) / ROPE)
    angles = positions[:, None] * frequency[None, :]
    paired = rope.reshape(rope.shape[0], ROPE // 2, 2)
    partner = jnp.stack([-paired[:, :, 1], paired[:, :, 0]], axis=2).reshape(rope.shape)
    rope = rope * jnp.cos(angles) + partner * jnp.sin(angles)
    return jnp.concatenate([latent, rope], axis=1).astype(jnp.bfloat16)


def slot_places(slot_table, slots):
    flat = slot_table.reshape(-1)
    hits = flat[None, :] == slots[:, None]
    at = jnp.sum(jnp.where(hits, jnp.arange(flat.shape[0], dtype=jnp.int32)[None, :], 0), axis=1)
    return at // slot_table.shape[1], at % slot_table.shape[1]


def token_mask(request, place, length, ok, requests):
    offset = place[:, None] * PAGE + jnp.arange(PAGE, dtype=jnp.int32)[None, :]
    live = (offset < length[:, None]) & ok[:, None]
    mine = request[None, :] == jnp.arange(requests, dtype=jnp.int32)[:, None]
    return (mine[:, :, None] & live[None]).reshape(requests, -1)


def body(
    hidden_x,
    proj_weight,
    q_gain,
    kv_gain,
    old_cache,
    page_plan,
    block_table,
    split_lens,
    dec_query,
    new_key,
):
    n = lax.axis_size("dec")
    index = lax.axis_index("dec")
    tokens = hidden_x.shape[0]
    slots = old_cache.shape[0]
    requests, heads, _ = dec_query.shape
    table = block_table[0]
    q_part, kv_part = project(hidden_x, proj_weight, index)

    pages = page_plan.shape[0]
    packed = jnp.concatenate(
        [page_plan.reshape(-1), table.reshape(-1), split_lens.reshape(-1)]
    ).reshape(1, -1)
    all_tables = (
        gather_small(packed, "dec") if n <= LINE_MAX else None
    )
    if all_tables is None:
        everyone = lax.all_gather(packed[0], "dec")
        all_tables = [
            lax.dynamic_slice_in_dim(everyone, (index + s) % n, 1) for s in range(n)
        ]
    tables = jnp.concatenate(all_tables, axis=0)
    plans = tables[:, : 2 * pages].reshape(n, pages, 2)
    taken = (plans[:, :, 0] == index).reshape(-1)[None, :] & (
        plans[:, :, 1].reshape(-1)[None, :] == jnp.arange(slots, dtype=jnp.int32)[:, None]
    )
    kept = ~jnp.any(taken, axis=1)

    request, place = slot_places(table, jnp.arange(slots, dtype=jnp.int32))
    one_hot = request[:, None] == jnp.arange(requests, dtype=jnp.int32)[None, :]
    length = jnp.sum(jnp.where(one_hot, split_lens[:, 0][None, :], 0), axis=1)
    old_mask = token_mask(request, place, length, kept, requests)
    query = dec_query.reshape(requests * heads, -1)
    old_rows = old_cache.reshape(-1, KVW)

    def scores_of(rows, mask):
        raw = lax.dot_general(
            query, rows, (((1,), (1,)), ((), ())), preferred_element_type=jnp.float32
        )
        return jnp.where(jnp.repeat(mask, heads, axis=0), raw * softmax_scale, MASKED)

    def attend(rows, scores, peak):
        weights = jnp.where(scores > MASKED, jnp.exp(scores - peak[:, None]), 0.0)
        return jnp.sum(weights, axis=1), dot32(weights.astype(jnp.bfloat16), rows[:, :KVL])

    own_score = (
        jnp.einsum("rhc,rc->rh", dec_query, new_key, preferred_element_type=jnp.float32)
        * softmax_scale
    ).reshape(-1)
    own_score = jnp.where(index == 0, own_score, MASKED)
    old_scores = scores_of(old_rows, old_mask)
    old_peak = jnp.maximum(jnp.max(old_scores, axis=1), own_score)
    old_total, old_out = attend(old_rows, old_scores, old_peak)
    own_weight = jnp.where(index == 0, jnp.exp(own_score - old_peak), 0.0)
    old_total = old_total + own_weight
    own_latent = jnp.repeat(new_key[:, :KVL].astype(jnp.float32), heads, axis=0)
    old_out = old_out + own_weight[:, None] * own_latent

    owner = page_plan[:, 0]
    owner_at = jnp.remainder(owner - index, n)
    owner_hot = owner_at[:, None] == jnp.arange(n, dtype=jnp.int32)[None, :]
    base = 2 * pages
    owner_rows = jnp.sum(jnp.where(owner_hot[:, :, None], tables[None, :, base:], 0), axis=1)
    hits = owner_rows[:, : table.size] == page_plan[:, 1][:, None]
    at = jnp.sum(jnp.where(hits, jnp.arange(table.size, dtype=jnp.int32)[None, :], 0), axis=1)
    new_request, new_place = at // table.shape[1], at % table.shape[1]
    new_hot = new_request[:, None] == jnp.arange(requests, dtype=jnp.int32)[None, :]
    new_length = jnp.sum(jnp.where(new_hot, owner_rows[:, table.size :], 0), axis=1)
    new_mask = token_mask(new_request, new_place, new_length, new_length > 0, requests)

    cores = lax.axis_size("tp")
    core = lax.axis_index("tp")
    rows_each = tokens // cores
    raw = scatter_sum(
        [kv_part[i * rows_each : (i + 1) * rows_each] for i in range(cores)], "tp", jnp.float32
    )
    raw = sum_over(raw, "stg")
    positions = (
        index * tokens + core * rows_each + jnp.arange(rows_each, dtype=jnp.int32)
    ).astype(jnp.float32)
    rows_here = kv_finish(raw, positions, kv_gain)
    shares = gather_small(rows_here, "tp")
    new_rows = jnp.concatenate(shares, axis=0)
    mask_shares = new_mask.reshape(requests, cores, rows_each)
    new_mask = jnp.concatenate(
        [
            lax.dynamic_index_in_dim(mask_shares, (core + s) % cores, 1, False)
            for s in range(cores)
        ],
        axis=1,
    )
    new_scores = scores_of(new_rows, new_mask)
    peak = jnp.maximum(old_peak, jnp.max(new_scores, axis=1))
    total, out = attend(new_rows, new_scores, peak)
    carried = jnp.exp(old_peak - peak)
    total = total + old_total * carried
    out = (out + old_out * carried[:, None]) / total[:, None]
    level = peak + jnp.log(total)

    if n <= LINE_MAX:
        outs = gather_small(out.astype(jnp.bfloat16), "dec")
        levels = gather_small(level, "dec")
        outs[0] = out
    else:
        stacked = lax.all_gather(out.astype(jnp.bfloat16), "dec")
        stacked_levels = lax.all_gather(level, "dec")
        outs = [stacked[i] for i in range(n)]
        levels = [stacked_levels[i] for i in range(n)]
    top = levels[0]
    for other in levels[1:]:
        top = jnp.maximum(top, other)
    shares_of = [jnp.exp(other - top) for other in levels]
    denom = sum(shares_of)
    numer = sum(s[:, None] * o.astype(jnp.float32) for s, o in zip(shares_of, outs))
    attn_latent = (
        (numer / denom[:, None]).astype(jnp.bfloat16).reshape(requests, heads, KVL)
    )

    stages = lax.axis_size("stg")
    stage = lax.axis_index("stg")
    query_width = QL // (stages * cores)
    by_core = [
        jnp.concatenate(
            [
                q_part[:, (s * cores + c) * query_width : (s * cores + c + 1) * query_width]
                for s in range(stages)
            ],
            axis=1,
        )
        for c in range(cores)
    ]
    half = scatter_sum(by_core, "tp", jnp.bfloat16)
    cols = scatter_sum(
        [half[:, s * query_width : (s + 1) * query_width] for s in range(stages)],
        "stg",
        jnp.bfloat16,
    )
    query_sq = exact_sum(exact_sum(jnp.sum(cols * cols, axis=1), "tp"), "stg")
    gain = lax.dynamic_slice_in_dim(q_gain, (stage * cores + core) * query_width, query_width)
    q_latent = (cols * lax.rsqrt(query_sq / QL + norm_eps)[:, None] * gain[None, :]).astype(
        jnp.bfloat16
    )
    return (q_latent, attn_latent)


def solution(mesh):
    return jax.shard_map(
        body,
        mesh=mesh,
        in_specs=(
            P(("grp", "dec"), ("stg", "tp")),
            P(("stg", "tp"), "dec"),
            P(),
            P(),
            P(("grp", "dec"), None, None),
            P(("grp", "dec"), None),
            P(("grp", "dec"), None, None),
            P("grp", "dec"),
            P("grp", ("stg", "tp"), None),
            P("grp", None),
        ),
        out_specs=(P(("grp", "dec"), ("stg", "tp")), P("grp", ("stg", "tp"), None)),
        check_vma=False,
    )
```

```python
import functools

import jax
import jax.numpy as jnp
from jax import lax
from jax.experimental import pallas as pl
from jax.experimental.pallas import tpu as pltpu
from jax.sharding import PartitionSpec as P

QL = 1536
KVL = 512
ROPE = 64
PAGE = 32
KVW = KVL + ROPE
MASKED = -1e30

softmax_scale = 192.0 ** (-0.5)
norm_eps = 1e-06


def combined_all(part, axis, combine):
    gathered = jax.tree.map(lambda a: lax.all_gather(a, axis), part)

    def take(source):
        return jax.tree.map(lambda a: lax.dynamic_index_in_dim(a, source, 0, False), gathered)

    return lax.fori_loop(
        1, lax.axis_size(axis), lambda source, state: combine(state, take(source)), take(0)
    )


def rope_rotate(matrix, col_start, positions):
    col_count = matrix.shape[1]
    columns = col_start + jnp.arange(col_count, dtype=jnp.int32)
    is_rope = columns >= KVL
    pair_index = jnp.maximum(columns - KVL, 0) // 2
    frequency = jnp.power(jnp.float32(10000.0), -(2 * pair_index).astype(jnp.float32) / ROPE)
    angles = positions[:, None] * frequency[None, :]
    cosine = jnp.where(is_rope[None, :], jnp.cos(angles), 1.0)
    sine_part = jnp.where(is_rope[None, :], jnp.sin(angles), 0.0)
    paired = matrix.reshape(matrix.shape[0], col_count // 2, 2)
    partner = jnp.stack([-paired[:, :, 1], paired[:, :, 0]], axis=2).reshape(matrix.shape)
    return matrix * cosine + partner * sine_part


def kv_finish(matrix, col_start, latent_sq, kv_gain, positions):
    col_count = matrix.shape[1]
    columns = col_start + jnp.arange(col_count, dtype=jnp.int32)
    gain_full = jnp.concatenate([kv_gain, jnp.ones((ROPE,), jnp.float32)])
    gain_cols = lax.dynamic_slice_in_dim(gain_full, col_start, col_count)
    inverse = lax.rsqrt(latent_sq / KVL + norm_eps)
    row_scale = jnp.where(columns[None, :] < KVL, inverse[:, None] * gain_cols[None, :], 1.0)
    return rope_rotate(matrix * row_scale, col_start, positions).astype(jnp.bfloat16)


def pack_pages(kv_pages, page_table, owner_count, capacity):
    owners = page_table[:, 0]
    slot_ids = page_table[:, 1]
    page_ids = jnp.arange(kv_pages.shape[0], dtype=jnp.int32)
    earlier = (owners[:, None] == owners[None, :]) & (page_ids[None, :] < page_ids[:, None])
    ranking = jnp.sum(earlier.astype(jnp.int32), axis=1)
    targets = owners * capacity + ranking
    places = jnp.arange(owner_count * capacity, dtype=jnp.int32)
    matches = targets[None, :] == places[:, None]
    source_ids = jnp.sum(jnp.where(matches, page_ids[None, :], 0), axis=1)
    filled = jnp.any(matches, axis=1)
    chosen = jnp.where(
        filled[:, None, None], jnp.take(kv_pages, source_ids, axis=0), jnp.zeros((), kv_pages.dtype)
    )
    labels = jnp.where(filled, jnp.take(slot_ids, source_ids), -1).astype(jnp.bfloat16)
    return (
        chosen.reshape(owner_count, capacity, kv_pages.shape[1], kv_pages.shape[2]),
        labels.reshape(owner_count, capacity),
    )


def place_pages(old_cache, got_pages, got_labels):
    flat_pages = got_pages.reshape(-1, old_cache.shape[1], old_cache.shape[2])
    label_ids = got_labels.reshape(-1).astype(jnp.int32)
    slot_ids = jnp.arange(old_cache.shape[0], dtype=jnp.int32)
    arrival_ids = jnp.arange(label_ids.shape[0], dtype=jnp.int32)
    matches = label_ids[None, :] == slot_ids[:, None]
    source_ids = jnp.sum(jnp.where(matches, arrival_ids[None, :], 0), axis=1)
    arrived = jnp.any(matches, axis=1)
    return jnp.where(arrived[:, None, None], jnp.take(flat_pages, source_ids, axis=0), old_cache)


def combine_parts(former, latter):
    overall = jnp.maximum(former[0], latter[0])
    front_scale = jnp.exp(former[0] - overall)
    back_scale = jnp.exp(latter[0] - overall)
    return (
        overall,
        former[1] * front_scale + latter[1] * back_scale,
        former[2] * front_scale[:, :, None] + latter[2] * back_scale[:, :, None],
    )


def body_general(
    hidden_x,
    proj_weight,
    q_gain,
    kv_gain,
    old_cache,
    page_plan,
    block_table,
    split_lens,
    dec_query,
    new_key,
):
    projected = jnp.dot(
        hidden_x,
        lax.all_gather(proj_weight, "dec", axis=1, tiled=True),
        preferred_element_type=jnp.float32,
    )
    query_part = projected[:, :QL]
    kv_part = projected[:, QL:]
    tokens_here = hidden_x.shape[0]
    positions = (
        lax.axis_index("dec") * tokens_here + jnp.arange(tokens_here, dtype=jnp.int32)
    ).astype(jnp.float32)
    lane_count = lax.axis_size(("stg", "tp"))
    lane_index = lax.axis_index(("stg", "tp"))
    owner_count = lax.axis_size("dec")
    page_count = page_plan.shape[0]
    capacity = max(2, -(-page_count // owner_count))
    query_width = QL // lane_count
    query_cols, kv_cols = (
        lax.psum_scatter(query_part, ("stg", "tp"), scatter_dimension=1, tiled=True),
        lax.psum_scatter(kv_part, ("stg", "tp"), scatter_dimension=1, tiled=True),
    )
    kv_width = kv_cols.shape[1]
    col_start = lane_index * kv_width
    columns = col_start + jnp.arange(kv_width, dtype=jnp.int32)
    latent_part_sq = jnp.sum(jnp.where(columns[None, :] < KVL, kv_cols * kv_cols, 0.0), axis=1)
    query_sq, latent_sq = lax.psum(
        (jnp.sum(query_cols * query_cols, axis=1), latent_part_sq), ("stg", "tp")
    )
    kv_rows = kv_finish(kv_cols, col_start, latent_sq, kv_gain, positions)
    kv_pages = kv_rows.reshape(page_count, PAGE, kv_width)
    send_pages, send_labels = pack_pages(kv_pages, page_plan, owner_count, capacity)
    got_slices, got_labels = (
        lax.all_to_all(send_pages, "dec", split_axis=0, concat_axis=0, tiled=True),
        lax.all_to_all(send_labels, "dec", split_axis=0, concat_axis=0, tiled=True),
    )
    got_pages = lax.all_gather(got_slices, ("stg", "tp"), axis=3, tiled=True)
    query_gain = lax.dynamic_slice_in_dim(q_gain, lane_index * query_width, query_width)
    q_latent = (
        query_cols * lax.rsqrt(query_sq / QL + norm_eps)[:, None] * query_gain[None, :]
    ).astype(jnp.bfloat16)
    cache = place_pages(old_cache, got_pages, got_labels)
    slot_table = block_table[0]
    request_count = slot_table.shape[0]
    key_rows = jnp.take(cache, slot_table.reshape(-1), axis=0).reshape(
        request_count, -1, cache.shape[2]
    )
    scores = (
        jnp.einsum("rhc,rlc->rhl", dec_query, key_rows, preferred_element_type=jnp.float32)
        * softmax_scale
    )
    live_mask = jnp.arange(key_rows.shape[1], dtype=jnp.int32)[None, :] < split_lens[:, 0][:, None]
    scores = jnp.where(live_mask[:, None, :], scores, -1e30)
    row_peak = jnp.max(scores, axis=2)
    weights = jnp.where(live_mask[:, None, :], jnp.exp(scores - row_peak[:, :, None]), 0.0)
    row_total = jnp.sum(weights, axis=2)
    rounded = weights.astype(jnp.bfloat16)
    partial_out = jnp.einsum(
        "rhl,rlc->rhc", rounded, key_rows[:, :, :KVL], preferred_element_type=jnp.float32
    )
    peak_all, total_all, output_all = combined_all(
        (row_peak, row_total, partial_out), "dec", combine_parts
    )
    self_score = (
        jnp.einsum("rhc,rc->rh", dec_query, new_key, preferred_element_type=jnp.float32)
        * softmax_scale
    )
    overall = jnp.maximum(peak_all, self_score)
    carried = jnp.exp(peak_all - overall)
    self_weight = jnp.exp(self_score - overall)
    denom = total_all * carried + self_weight
    numer = output_all * carried[:, :, None] + self_weight[:, :, None] * new_key[
        :, None, :KVL
    ].astype(jnp.float32)
    attn_latent = (numer / denom[:, :, None]).astype(jnp.bfloat16)
    return (q_latent, attn_latent)


VMEM = pl.BlockSpec(memory_space=pltpu.VMEM)
SMEM = pl.BlockSpec(memory_space=pltpu.SMEM)
F32 = jnp.float32
BF16 = jnp.bfloat16


def swap(a, axis):
    return lax.ppermute(a, axis, [(0, 1), (1, 0)])


def dot_t(a, b, **kw):
    return lax.dot_general(a, b, (((1,), (1,)), ((), ())), preferred_element_type=F32, **kw)


def dot_n(a, b, **kw):
    return lax.dot_general(a, b, (((1,), (0,)), ((), ())), preferred_element_type=F32, **kw)


def matmul_kernel(ids, x_ref, wz_ref, wy_ref, send_ref, keep_ref):
    group = ids[0]
    half = wz_ref.shape[1]
    here = pl.ds(pl.multiple_of(group * half, 128), half)
    there = pl.ds(pl.multiple_of((1 - group) * half, 128), half)
    out = dot_t(x_ref[:, here], wz_ref[...]) + dot_t(x_ref[:, there], wy_ref[...])

    @pl.when(pl.program_id(0) == 0)
    def _():
        send_ref[...] = out

    @pl.when(pl.program_id(0) == 1)
    def _():
        keep_ref[...] = out


def matmul(ids, x, wz, wy):
    rows, feats = x.shape
    cols = wz.shape[0]
    tile = rows // 2
    shape = jax.ShapeDtypeStruct((tile, cols), F32)
    whole = pl.BlockSpec((cols, wz.shape[1]), lambda i, ids: (0, 0))
    flat = pl.BlockSpec((tile, cols), lambda i, ids: (0, 0))
    return pl.pallas_call(
        matmul_kernel,
        grid_spec=pltpu.PrefetchScalarGridSpec(
            num_scalar_prefetch=1,
            grid=(2,),
            in_specs=[
                pl.BlockSpec((tile, feats), lambda i, ids: ((ids[1] + 1 + i) % 2, 0)),
                whole,
                whole,
            ],
            out_specs=[flat, flat],
        ),
        out_shape=[shape, shape],
        cost_estimate=pl.CostEstimate(
            flops=2 * rows * feats * cols, bytes_accessed=8 * rows * cols, transcendentals=0
        ),
        name="project",
    )(ids, x, wz, wy)


def old_kernel(pages, ids, tab, query_ref, rows_ref, own_ref, peak_ref, total_ref, out_ref, bias_ref):
    n, index, core = tab.shape[0], ids[2], ids[1]
    query = query_ref[...]
    keys = rows_ref.shape[0]
    requests = own_ref.shape[0] // 4
    heads = query.shape[0] // requests
    base = 2 * pages
    slots = tab.shape[1] - base - requests
    per = slots // requests

    def columns(width):
        col = lax.broadcasted_iota(jnp.int32, (8, width), 1)
        return col // PAGE, col % PAGE

    page, offset = columns(keys)
    limit = jnp.zeros((8, keys), jnp.int32)
    reader = jnp.zeros((8, keys), jnp.int32)
    for f in range(slots):
        hit = page == tab[0, base + f]
        limit = jnp.where(hit, tab[0, base + slots + f // per] - PAGE * (f % per), limit)
        reader = jnp.where(hit, f // per, reader)
    for s in range(n):
        for p in range(pages):
            taken = jnp.where(tab[s, 2 * p] == index, tab[s, 2 * p + 1], -1)
            limit = jnp.where(page == taken, 0, limit)
    live = offset < limit
    row = lax.broadcasted_iota(jnp.int32, (8, keys), 0)
    bias = jnp.where(live & (reader == row), 0.0, MASKED)
    wide = jnp.concatenate(
        [jnp.broadcast_to(bias[r : r + 1], (heads, keys)) for r in range(requests)], axis=0
    )
    scores = dot_t(query, rows_ref[...]) * softmax_scale + wide
    own = dot_t(query, own_ref[...]) * softmax_scale
    mine = (
        lax.broadcasted_iota(jnp.int32, own.shape, 0) // heads
        == lax.broadcasted_iota(jnp.int32, own.shape, 1)
    )
    own = jnp.sum(jnp.where(mine, own, 0.0), axis=1, keepdims=True)
    own = jnp.where(index == 0, own, MASKED)
    peak = jnp.maximum(jnp.max(scores, axis=1, keepdims=True), own)
    weights = jnp.where(wide < 0.0, 0.0, jnp.exp(scores - peak))
    own_weight = jnp.where(index == 0, jnp.exp(own - peak), 0.0)
    peak_ref[...] = peak
    total_ref[...] = jnp.sum(weights, axis=1, keepdims=True) + own_weight
    out = dot_n(weights.astype(BF16), rows_ref[:, :KVL])
    own_rows = own_ref[:, :KVL].astype(F32)
    latent = jnp.concatenate(
        [jnp.broadcast_to(own_rows[r : r + 1], (heads, KVL)) for r in range(requests)], axis=0
    )
    out_ref[...] = out + own_weight * latent

    width = bias_ref.shape[1]
    page, offset = columns(width)
    limit = jnp.zeros((8, width), jnp.int32)
    reader = jnp.zeros((8, width), jnp.int32)
    half = pages // 2
    for k in range(2 * pages):
        other_core, within = divmod(k, pages)
        partner, place = divmod(within, half)
        at = (n - 1) * partner
        which = jnp.where(other_core == 1, 1 - core, core) * half + place
        owner, slot = tab[at, 2 * which], tab[at, 2 * which + 1]
        where = (owner - index + n) % n

        def look(f, state):
            hit = tab[where, base + f] == slot
            new_limit = tab[where, base + slots + f // per] - PAGE * (f % per)
            return jnp.where(hit, new_limit, state[0]), jnp.where(hit, f // per, state[1])

        found = lax.fori_loop(0, slots, look, (jnp.int32(0), jnp.int32(0)))
        reads = jnp.where(index % 2 == 1, found[0], 0)
        limit = jnp.where(page == k, reads, limit)
        reader = jnp.where(page == k, found[1], reader)
    row = lax.broadcasted_iota(jnp.int32, (8, width), 0)
    bias_ref[...] = jnp.where((offset < limit) & (reader == row), 0.0, MASKED)


def middle_kernel(ids, *refs):
    (ak, ar, bk, br, pak, par, pbk, pbr, kv_send, kv_keep, q_send, q_keep) = refs
    first, stage = ids[2] < 2, ids[3]
    rows, cols = ak.shape
    cut = QL - 2 * cols
    quarter = rows // 2
    for i, (a0, a1, b0, b1) in enumerate(((ak, ar, bk, br), (pak, par, pbk, pbr))):
        a = a0[...] + a1[...]
        b = b0[...] + b1[...]
        low, high = jnp.where(first, b, a), jnp.where(first, a, b)
        tail = jnp.concatenate([low[:, cut:], high], axis=1)
        at = slice(i * rows, (i + 1) * rows)
        kv_keep[at, :] = tail
        kv_send[at, :] = tail.astype(BF16)
        top, bottom = low[:quarter, :cut], low[quarter:, :cut]
        at = slice(i * quarter, (i + 1) * quarter)
        q_keep[at, :] = jnp.where(stage == 0, top, bottom)
        q_send[at, :] = jnp.where(stage == 0, bottom, top).astype(BF16)


def keys_kernel(keep, got, cos, sin, turn, gain, out):
    raw = keep[...] + got[...].astype(F32)
    latent = raw[:, :KVL]
    inverse = lax.rsqrt(jnp.sum(latent * latent, axis=1, keepdims=True) / KVL + norm_eps)
    out[:, :KVL] = (latent * inverse * gain[...]).astype(BF16)
    rope = raw[:, KVL:]
    partner = dot_n(rope, turn[...], precision=lax.Precision.HIGHEST)
    out[:, KVL:] = (rope * cos[...] + partner * sin[...]).astype(BF16)


def attend_kernel(query_ref, k0_ref, k1_ref, bias_ref, peak_ref, total_ref, out_ref, packed_ref):
    query = query_ref[...]
    keys = k0_ref.shape[0]
    rows = query.shape[0]
    requests = bias_ref.shape[0] // 2
    heads = rows // requests
    bias = bias_ref[...]
    wide = jnp.concatenate(
        [jnp.broadcast_to(bias[r : r + 1], (heads, 2 * keys)) for r in range(requests)], axis=0
    )
    scores = jnp.concatenate([dot_t(query, k0_ref[...]), dot_t(query, k1_ref[...])], axis=1)
    scores = scores * softmax_scale + wide
    old_peak = peak_ref[...]
    peak = jnp.maximum(old_peak, jnp.max(scores, axis=1, keepdims=True))
    weights = jnp.where(wide < 0.0, 0.0, jnp.exp(scores - peak))
    carried = jnp.exp(old_peak - peak)
    total = jnp.sum(weights, axis=1, keepdims=True) + total_ref[...] * carried
    rounded = weights.astype(BF16)
    out = dot_n(rounded[:, :keys], k0_ref[:, :KVL]) + dot_n(rounded[:, keys:], k1_ref[:, :KVL])
    out = (out + out_ref[...] * carried) / total
    level = peak + jnp.log(total)
    packed_ref[:, :KVL] = out.astype(BF16)
    lead = level.astype(BF16).astype(F32)
    rest = (level - lead).astype(BF16).astype(F32)
    last = level - lead - rest
    lane = lax.broadcasted_iota(jnp.int32, (rows, 128), 1)
    tail = jnp.where(lane == 0, lead, jnp.where(lane == 1, rest, jnp.where(lane == 2, last, 0.0)))
    packed_ref[:, KVL:] = tail.astype(BF16)


def combine_kernel(*refs):
    parts, out = refs[:-1], refs[-1]
    levels = [jnp.sum(p[:, KVL:].astype(F32), axis=1, keepdims=True) for p in parts]
    top = functools.reduce(jnp.maximum, levels)
    shares = [jnp.exp(level - top) for level in levels]
    numer = sum(s * p[:, :KVL].astype(F32) for s, p in zip(shares, parts))
    out[...] = (numer / sum(shares)).astype(BF16)


def return_kernel(ids, kv_keep, kv_got, q_keep, q_got, low, high, send):
    stage = ids[3]
    rows = kv_keep.shape[0] // 2
    quarter = rows // 2
    start = pl.multiple_of(stage * quarter, 32)
    for i in range(2):
        at = pl.ds(i * rows + start, quarter)
        wide = kv_keep[at, :] + kv_got[at, :].astype(F32)
        near = slice(i * quarter, (i + 1) * quarter)
        short = q_keep[near, :] + q_got[near, :].astype(F32)
        if i == 0:
            low[...] = short
            high[...] = wide
        else:
            send[:, : short.shape[1]] = short.astype(BF16)
            send[:, short.shape[1] :] = wide.astype(BF16)


def query_kernel(ids, low, high, got, gain, send, keep):
    odd = ids[2] % 2 == 1
    cut = low.shape[1]
    got_low, got_high = got[:, :cut].astype(F32), got[:, cut:].astype(F32)
    first = jnp.where(odd, got_low, low[...])
    second = jnp.where(odd, got_high, high[...])
    third = jnp.where(odd, low[...], got_low)
    rows = jnp.concatenate([first, second, third], axis=1)
    inverse = lax.rsqrt(jnp.sum(rows * rows, axis=1, keepdims=True) / QL + norm_eps)
    rows = (rows * inverse * gain[...]).astype(BF16)
    width = QL // 4
    core = ids[1]
    for s in range(2):
        zero = rows[:, 2 * s * width : (2 * s + 1) * width]
        one = rows[:, (2 * s + 1) * width : (2 * s + 2) * width]
        keep[s] = jnp.where(core == 0, zero, one)
        send[s] = jnp.where(core == 0, one, zero)


def call(kernel, shapes, specs, name, args):
    return pl.pallas_call(
        kernel,
        out_shape=shapes,
        in_specs=specs,
        out_specs=[VMEM] * len(shapes) if isinstance(shapes, list) else VMEM,
        cost_estimate=pl.CostEstimate(flops=20_000_000, bytes_accessed=2_000_000, transcendentals=0),
        name=name,
    )(*args)


def shaped(*dims, kind=F32):
    return jax.ShapeDtypeStruct(dims, kind)


def body_pairs(
    hidden_x,
    proj_weight,
    q_gain,
    kv_gain,
    old_cache,
    page_plan,
    block_table,
    split_lens,
    dec_query,
    new_key,
):
    n = lax.axis_size("dec")
    group, index = lax.axis_index("grp"), lax.axis_index("dec")
    stage, core = lax.axis_index("stg"), lax.axis_index("tp")
    ids = jnp.stack([group, core, index, stage]).astype(jnp.int32)
    tokens, feats = hidden_x.shape
    cols = proj_weight.shape[1]
    cut = QL - 2 * cols
    half = feats // 2
    pages = page_plan.shape[0]
    requests, heads, _ = dec_query.shape
    queries = requests * heads

    weight = lax.dynamic_slice_in_dim(proj_weight.T, group * half, half, axis=1)
    part = cols // 2
    a_pairs = [(0, 2), (3, 1), (1, 0), (2, 3)]
    b_pairs = [(0, 0), (1, 2), (2, 1), (3, 3)]
    a_z = lax.ppermute(weight, "dec", a_pairs)
    x_far = lax.ppermute(hidden_x, "dec", [(0, 1), (1, 0), (2, 3), (3, 2)])
    packed = jnp.concatenate(
        [page_plan.reshape(-1), block_table.reshape(-1), split_lens.reshape(-1)]
    ).reshape(1, -1)
    tables = [packed] + [
        lax.ppermute(packed, "dec", [((i + s) % n, i) for i in range(n)]) for s in range(1, n)
    ]
    tables = jnp.concatenate(tables, axis=0)
    held, a_z = lax.optimization_barrier((weight, a_z))
    b_z = lax.ppermute(held, "dec", b_pairs)
    a_y = swap(a_z, "grp")
    b_y = swap(b_z, "grp")

    query = dec_query.reshape(queries, KVW)
    padded_key = jnp.pad(new_key, ((0, 3 * requests), (0, 0)))
    peak, total, out, bias = call(
        functools.partial(old_kernel, pages),
        [shaped(queries, 1), shaped(queries, 1), shaped(queries, KVL), shaped(8, 2 * tokens)],
        [SMEM, SMEM, VMEM, VMEM, VMEM],
        "old_pages",
        (ids, tables, query, old_cache.reshape(-1, KVW), padded_key),
    )

    a_near = matmul(ids, hidden_x, a_z, a_y)
    b_near = matmul(ids, hidden_x, b_z, b_y)
    a_far = matmul(ids, x_far, a_z, a_y)
    b_far = matmul(ids, x_far, b_z, b_y)
    sums = []
    for send, keep in (a_near, b_near, a_far, b_far):
        sums += [keep, swap(send, "tp")]
    rows = tokens // 2
    quarter = rows // 2
    kv_send, kv_keep, q_send, q_keep = call(
        middle_kernel,
        [
            shaped(2 * rows, KVW, kind=BF16),
            shaped(2 * rows, KVW),
            shaped(rows, cut, kind=BF16),
            shaped(rows, cut),
        ],
        [SMEM] + [VMEM] * 8,
        "split_sums",
        (ids, *sums),
    )
    kv_got = swap(kv_send, "stg")
    q_got = swap(q_send, "stg")

    partner = index + 1 - 2 * (index % 2)
    place = core * rows + jnp.arange(rows, dtype=jnp.int32)
    positions = jnp.concatenate([index * tokens + place, partner * tokens + place]).astype(F32)
    pair = jnp.arange(ROPE, dtype=jnp.int32) // 2
    frequency = jnp.power(F32(10000.0), -(2 * pair).astype(F32) / ROPE)
    angles = positions[:, None] * frequency[None, :]
    source = jnp.arange(ROPE, dtype=jnp.int32)[:, None]
    target = jnp.arange(ROPE, dtype=jnp.int32)[None, :]
    turn = jnp.where(
        source == target + 1,
        jnp.where(target % 2 == 0, -1.0, 0.0),
        jnp.where((source + 1 == target) & (target % 2 == 1), 1.0, 0.0),
    )
    key_rows = call(
        keys_kernel,
        shaped(2 * rows, KVW, kind=BF16),
        [VMEM] * 6,
        "finish_keys",
        (kv_keep, kv_got, jnp.cos(angles), jnp.sin(angles), turn, kv_gain.reshape(1, -1)),
    )
    far_keys = swap(key_rows, "tp")
    part_out = call(
        attend_kernel,
        shaped(queries, KVL + 128, kind=BF16),
        [VMEM] * 7,
        "new_pages",
        (query, key_rows, far_keys, bias, peak, total, out),
    )
    parts = [part_out] + [
        lax.ppermute(part_out, "dec", [((i + s) % n, i) for i in range(n)]) for s in range(1, n)
    ]
    attn = call(
        combine_kernel, shaped(queries, KVL, kind=BF16), [VMEM] * n, "combine", tuple(parts)
    )

    low, high, back = call(
        return_kernel,
        [shaped(quarter, cut), shaped(quarter, KVW), shaped(quarter, cut + KVW, kind=BF16)],
        [SMEM] + [VMEM] * 4,
        "return_rows",
        (ids, kv_keep, kv_got, q_keep, q_got),
    )
    back = lax.ppermute(back, "dec", [(0, 1), (1, 0), (2, 3), (3, 2)])
    width = QL // 4
    tile = shaped(2, quarter, width, kind=BF16)
    core_send, core_keep = call(
        query_kernel,
        [tile, tile],
        [SMEM] + [VMEM] * 4,
        "finish_queries",
        (ids, low, high, back, q_gain.reshape(1, -1)),
    )
    core_got = swap(core_send, "tp")
    both = jnp.where(
        core == 0, jnp.stack([core_keep, core_got]), jnp.stack([core_got, core_keep])
    )
    mine = jnp.where(stage == 0, both[:, 0], both[:, 1])
    away = jnp.where(stage == 0, both[:, 1], both[:, 0])
    got = swap(away, "stg")
    q_latent = jnp.where(
        stage == 0, jnp.stack([mine, got], axis=1), jnp.stack([got, mine], axis=1)
    ).reshape(tokens, width)
    return (q_latent, attn.reshape(requests, heads, KVL))


def solution(mesh):
    sizes = dict(mesh.shape)
    pairs = sizes["dec"] == 4 and sizes["grp"] == sizes["stg"] == sizes["tp"] == 2
    return jax.shard_map(
        body_pairs if pairs else body_general,
        mesh=mesh,
        in_specs=(
            P(("grp", "dec"), ("stg", "tp")),
            P(("stg", "tp"), "dec"),
            P(),
            P(),
            P(("grp", "dec"), None, None),
            P(("grp", "dec"), None),
            P(("grp", "dec"), None, None),
            P("grp", "dec"),
            P("grp", ("stg", "tp"), None),
            P("grp", None),
        ),
        out_specs=(P(("grp", "dec"), ("stg", "tp")), P("grp", ("stg", "tp"), None)),
        check_vma=False,
    )
```

```python
import functools

import jax
import jax.numpy as jnp
from jax import lax
from jax.experimental import pallas as pl
from jax.experimental.pallas import tpu as pltpu
from jax.sharding import PartitionSpec as P


QL = 1536
KVL = 512
ROPE = 64
PAGE = 32
KVW = KVL + ROPE
MASKED = -1e30

softmax_scale = 192.0 ** (-0.5)
norm_eps = 1e-06


def combined_all(part, axis, combine):
    gathered = jax.tree.map(lambda a: lax.all_gather(a, axis), part)

    def take(source):
        return jax.tree.map(lambda a: lax.dynamic_index_in_dim(a, source, 0, False), gathered)

    return lax.fori_loop(
        1, lax.axis_size(axis), lambda source, state: combine(state, take(source)), take(0)
    )


def rope_rotate(matrix, col_start, positions):
    col_count = matrix.shape[1]
    columns = col_start + jnp.arange(col_count, dtype=jnp.int32)
    is_rope = columns >= KVL
    pair_index = jnp.maximum(columns - KVL, 0) // 2
    frequency = jnp.power(jnp.float32(10000.0), -(2 * pair_index).astype(jnp.float32) / ROPE)
    angles = positions[:, None] * frequency[None, :]
    cosine = jnp.where(is_rope[None, :], jnp.cos(angles), 1.0)
    sine_part = jnp.where(is_rope[None, :], jnp.sin(angles), 0.0)
    paired = matrix.reshape(matrix.shape[0], col_count // 2, 2)
    partner = jnp.stack([-paired[:, :, 1], paired[:, :, 0]], axis=2).reshape(matrix.shape)
    return matrix * cosine + partner * sine_part


def kv_finish(matrix, col_start, latent_sq, kv_gain, positions):
    col_count = matrix.shape[1]
    columns = col_start + jnp.arange(col_count, dtype=jnp.int32)
    gain_full = jnp.concatenate([kv_gain, jnp.ones((ROPE,), jnp.float32)])
    gain_cols = lax.dynamic_slice_in_dim(gain_full, col_start, col_count)
    inverse = lax.rsqrt(latent_sq / KVL + norm_eps)
    row_scale = jnp.where(columns[None, :] < KVL, inverse[:, None] * gain_cols[None, :], 1.0)
    return rope_rotate(matrix * row_scale, col_start, positions).astype(jnp.bfloat16)


def pack_pages(kv_pages, page_table, owner_count, capacity):
    owners = page_table[:, 0]
    slot_ids = page_table[:, 1]
    page_ids = jnp.arange(kv_pages.shape[0], dtype=jnp.int32)
    earlier = (owners[:, None] == owners[None, :]) & (page_ids[None, :] < page_ids[:, None])
    ranking = jnp.sum(earlier.astype(jnp.int32), axis=1)
    targets = owners * capacity + ranking
    places = jnp.arange(owner_count * capacity, dtype=jnp.int32)
    matches = targets[None, :] == places[:, None]
    source_ids = jnp.sum(jnp.where(matches, page_ids[None, :], 0), axis=1)
    filled = jnp.any(matches, axis=1)
    chosen = jnp.where(
        filled[:, None, None], jnp.take(kv_pages, source_ids, axis=0), jnp.zeros((), kv_pages.dtype)
    )
    labels = jnp.where(filled, jnp.take(slot_ids, source_ids), -1).astype(jnp.bfloat16)
    return (
        chosen.reshape(owner_count, capacity, kv_pages.shape[1], kv_pages.shape[2]),
        labels.reshape(owner_count, capacity),
    )


def place_pages(old_cache, got_pages, got_labels):
    flat_pages = got_pages.reshape(-1, old_cache.shape[1], old_cache.shape[2])
    label_ids = got_labels.reshape(-1).astype(jnp.int32)
    slot_ids = jnp.arange(old_cache.shape[0], dtype=jnp.int32)
    arrival_ids = jnp.arange(label_ids.shape[0], dtype=jnp.int32)
    matches = label_ids[None, :] == slot_ids[:, None]
    source_ids = jnp.sum(jnp.where(matches, arrival_ids[None, :], 0), axis=1)
    arrived = jnp.any(matches, axis=1)
    return jnp.where(arrived[:, None, None], jnp.take(flat_pages, source_ids, axis=0), old_cache)


def combine_parts(former, latter):
    overall = jnp.maximum(former[0], latter[0])
    front_scale = jnp.exp(former[0] - overall)
    back_scale = jnp.exp(latter[0] - overall)
    return (
        overall,
        former[1] * front_scale + latter[1] * back_scale,
        former[2] * front_scale[:, :, None] + latter[2] * back_scale[:, :, None],
    )


def body_general(
    hidden_x,
    proj_weight,
    q_gain,
    kv_gain,
    old_cache,
    page_plan,
    block_table,
    split_lens,
    dec_query,
    new_key,
):
    projected = jnp.dot(
        hidden_x,
        lax.all_gather(proj_weight, "dec", axis=1, tiled=True),
        preferred_element_type=jnp.float32,
    )
    query_part = projected[:, :QL]
    kv_part = projected[:, QL:]
    tokens_here = hidden_x.shape[0]
    positions = (
        lax.axis_index("dec") * tokens_here + jnp.arange(tokens_here, dtype=jnp.int32)
    ).astype(jnp.float32)
    lane_count = lax.axis_size(("stg", "tp"))
    lane_index = lax.axis_index(("stg", "tp"))
    owner_count = lax.axis_size("dec")
    page_count = page_plan.shape[0]
    capacity = max(2, -(-page_count // owner_count))
    query_width = QL // lane_count
    query_cols, kv_cols = (
        lax.psum_scatter(query_part, ("stg", "tp"), scatter_dimension=1, tiled=True),
        lax.psum_scatter(kv_part, ("stg", "tp"), scatter_dimension=1, tiled=True),
    )
    kv_width = kv_cols.shape[1]
    col_start = lane_index * kv_width
    columns = col_start + jnp.arange(kv_width, dtype=jnp.int32)
    latent_part_sq = jnp.sum(jnp.where(columns[None, :] < KVL, kv_cols * kv_cols, 0.0), axis=1)
    query_sq, latent_sq = lax.psum(
        (jnp.sum(query_cols * query_cols, axis=1), latent_part_sq), ("stg", "tp")
    )
    kv_rows = kv_finish(kv_cols, col_start, latent_sq, kv_gain, positions)
    kv_pages = kv_rows.reshape(page_count, PAGE, kv_width)
    send_pages, send_labels = pack_pages(kv_pages, page_plan, owner_count, capacity)
    got_slices, got_labels = (
        lax.all_to_all(send_pages, "dec", split_axis=0, concat_axis=0, tiled=True),
        lax.all_to_all(send_labels, "dec", split_axis=0, concat_axis=0, tiled=True),
    )
    got_pages = lax.all_gather(got_slices, ("stg", "tp"), axis=3, tiled=True)
    query_gain = lax.dynamic_slice_in_dim(q_gain, lane_index * query_width, query_width)
    q_latent = (
        query_cols * lax.rsqrt(query_sq / QL + norm_eps)[:, None] * query_gain[None, :]
    ).astype(jnp.bfloat16)
    cache = place_pages(old_cache, got_pages, got_labels)
    slot_table = block_table[0]
    request_count = slot_table.shape[0]
    key_rows = jnp.take(cache, slot_table.reshape(-1), axis=0).reshape(
        request_count, -1, cache.shape[2]
    )
    scores = (
        jnp.einsum("rhc,rlc->rhl", dec_query, key_rows, preferred_element_type=jnp.float32)
        * softmax_scale
    )
    live_mask = jnp.arange(key_rows.shape[1], dtype=jnp.int32)[None, :] < split_lens[:, 0][:, None]
    scores = jnp.where(live_mask[:, None, :], scores, -1e30)
    row_peak = jnp.max(scores, axis=2)
    weights = jnp.where(live_mask[:, None, :], jnp.exp(scores - row_peak[:, :, None]), 0.0)
    row_total = jnp.sum(weights, axis=2)
    rounded = weights.astype(jnp.bfloat16)
    partial_out = jnp.einsum(
        "rhl,rlc->rhc", rounded, key_rows[:, :, :KVL], preferred_element_type=jnp.float32
    )
    peak_all, total_all, output_all = combined_all(
        (row_peak, row_total, partial_out), "dec", combine_parts
    )
    self_score = (
        jnp.einsum("rhc,rc->rh", dec_query, new_key, preferred_element_type=jnp.float32)
        * softmax_scale
    )
    overall = jnp.maximum(peak_all, self_score)
    carried = jnp.exp(peak_all - overall)
    self_weight = jnp.exp(self_score - overall)
    denom = total_all * carried + self_weight
    numer = output_all * carried[:, :, None] + self_weight[:, :, None] * new_key[
        :, None, :KVL
    ].astype(jnp.float32)
    attn_latent = (numer / denom[:, :, None]).astype(jnp.bfloat16)
    return (q_latent, attn_latent)


VMEM = pl.BlockSpec(memory_space=pltpu.VMEM)
SMEM = pl.BlockSpec(memory_space=pltpu.SMEM)
VMEM_GRANT = 16 * 2**20
F32 = jnp.float32
BF16 = jnp.bfloat16


def swap(a, axis):
    return lax.ppermute(a, axis, [(0, 1), (1, 0)])


def dot_t(a, b, **kw):
    return lax.dot_general(a, b, (((1,), (1,)), ((), ())), preferred_element_type=F32, **kw)


def dot_n(a, b, **kw):
    return lax.dot_general(a, b, (((1,), (0,)), ((), ())), preferred_element_type=F32, **kw)


def matmul_kernel(blocks, ids, *refs):
    group, core = ids[0], ids[1]
    xs, (head_z, tail_z, head_y, tail_y), outs = refs[:blocks], refs[blocks : blocks + 4], refs[blocks + 4 :]
    half = head_z.shape[1]
    split = head_z.shape[0]
    here = pl.ds(pl.multiple_of(group * half, 128), half)
    there = pl.ds(pl.multiple_of((1 - group) * half, 128), half)
    for i, x_ref in enumerate(xs):
        send, keep = outs[2 * i], outs[2 * i + 1]
        rows = send.shape[0]
        near, far = x_ref[:, here], x_ref[:, there]
        for z, y, at in ((head_z, head_y, slice(0, split)), (tail_z, tail_y, slice(split, None))):
            out = dot_t(near, z[...]) + dot_t(far, y[...])
            top, bottom = out[:rows], out[rows:]
            send[:, at] = jnp.where(core == 0, bottom, top)
            keep[:, at] = jnp.where(core == 0, top, bottom)


def matmul(ids, xs, weights):
    rows, feats = xs[0].shape
    cols = weights[0].shape[0] + weights[1].shape[0]
    blocks = len(xs)
    return pl.pallas_call(
        functools.partial(matmul_kernel, blocks),
        in_specs=[SMEM] + [VMEM] * (blocks + 4),
        out_specs=[VMEM] * (2 * blocks),
        out_shape=[jax.ShapeDtypeStruct((rows // 2, cols), F32)] * (2 * blocks),
        cost_estimate=pl.CostEstimate(
            flops=2 * rows * feats * cols * blocks,
            bytes_accessed=8 * rows * cols * blocks,
            transcendentals=0,
        ),
        compiler_params=pltpu.CompilerParams(vmem_limit_bytes=VMEM_GRANT),
        name="project",
    )(ids, *xs, *weights)


def old_kernel(n, pages, ids, tab_ref, query_ref, rows_ref, own_ref, peak_ref, total_ref, out_ref, bias_ref):
    index, core = ids[2], ids[1]
    query = query_ref[...]
    keys = rows_ref.shape[0]
    requests = own_ref.shape[0] // 4
    heads = query.shape[0] // requests
    base = 2 * pages
    slots = keys // PAGE
    per = slots // requests

    def iota(rows, cols, axis):
        return lax.broadcasted_iota(jnp.int32, (rows, cols), axis)

    size = tab_ref.shape[1]
    diagonal = iota(size, size, 0) == iota(size, size, 1)
    columns = [
        jnp.sum(jnp.where(diagonal, tab_ref[s : s + 1, :], 0), axis=1, keepdims=True)
        for s in range(n)
    ]
    entry = iota(slots, 1, 0)
    readers = entry // per

    def limits(column):
        lengths = jnp.zeros((slots, 1), jnp.int32)
        for r in range(requests):
            at = base + slots + r
            lengths = jnp.where(readers == r, column[at : at + 1, :], lengths)
        return lengths - PAGE * (entry % per)

    def lookup(hit, values):
        return jnp.sum(jnp.where(hit, values, 0), axis=0, keepdims=True)

    page = iota(1, keys, 1) // PAGE
    hit = columns[0][base : base + slots, :] == page
    limit = lookup(hit, limits(columns[0]))
    reader = lookup(hit, readers)
    is_slot = iota(base, 1, 0) % 2 == 1
    taken = jnp.zeros((1, keys), jnp.int32)
    odd_row = iota(base, base, 0)
    follows = (iota(base, base, 1) == odd_row - 1) & (odd_row % 2 == 1)
    for s in range(n):
        plan = columns[s][:base, :]
        owners = jnp.sum(jnp.where(follows, tab_ref[s : s + 1, :base], 0), axis=1, keepdims=True)
        here = is_slot & (owners == index)
        taken = taken + jnp.sum(jnp.where(here & (plan == page), 1, 0), axis=0, keepdims=True)
    limit = jnp.where(taken > 0, 0, limit)
    live = (iota(1, keys, 1) % PAGE) < limit
    bias = jnp.where(live & (reader == iota(8, keys, 0)), 0.0, MASKED)
    wide = jnp.concatenate(
        [jnp.broadcast_to(bias[r : r + 1], (heads, keys)) for r in range(requests)], axis=0
    )
    scores = dot_t(query, rows_ref[...]) * softmax_scale + wide
    own = dot_t(query, own_ref[...]) * softmax_scale
    mine = iota(*own.shape, 0) // heads == iota(*own.shape, 1)
    own = jnp.sum(jnp.where(mine, own, 0.0), axis=1, keepdims=True)
    own = jnp.where(index == 0, own, MASKED)
    peak = jnp.maximum(jnp.max(scores, axis=1, keepdims=True), own)
    weights = jnp.where(wide < 0.0, 0.0, jnp.exp(scores - peak))
    own_weight = jnp.where(index == 0, jnp.exp(own - peak), 0.0)
    peak_ref[...] = peak
    total_ref[...] = jnp.sum(weights, axis=1, keepdims=True) + own_weight
    out = dot_n(weights.astype(BF16), rows_ref[:, :KVL])
    own_rows = own_ref[:, :KVL].astype(F32)
    latent = jnp.concatenate(
        [jnp.broadcast_to(own_rows[r : r + 1], (heads, KVL)) for r in range(requests)], axis=0
    )
    out_ref[...] = out + own_weight * latent

    width = bias_ref.shape[1]
    half = pages // 2
    spot = iota(1, width, 1) // PAGE
    which = jnp.where(spot // pages == 1, 1 - core, core) * half + spot % half
    partner = (spot % pages) // half == 1
    line = iota(base, width, 0)
    plan = jnp.where(partner, columns[n - 1][:base, :], columns[0][:base, :])
    plan = jnp.where(line % 2 == 1, plan, plan * (2 * slots))
    code = jnp.sum(jnp.where(line // 2 == which, plan, 0), axis=0, keepdims=True)
    limit = jnp.zeros((1, width), jnp.int32)
    reader = jnp.zeros((1, width), jnp.int32)
    for s in range(n):
        owner = (index + s) % n
        hit = columns[s][base : base + slots, :] + owner * (2 * slots) == code
        limit = limit + lookup(hit, limits(columns[s]))
        reader = reader + lookup(hit, readers)
    limit = jnp.where(index % 2 == 1, limit, 0)
    live = (iota(1, width, 1) % PAGE) < limit
    bias_ref[...] = jnp.where(live & (reader == iota(8, width, 0)), 0.0, MASKED)


def middle_kernel(ids, *refs):
    (ak, ar, bk, br, pak, par, pbk, pbr, kv_send, kv_keep, q_send, q_keep) = refs
    first, stage = ids[2] < 2, ids[3]
    rows, cols = ak.shape
    cut = QL - 2 * cols
    quarter = rows // 2
    for i, (a0, a1, b0, b1) in enumerate(((ak, ar, bk, br), (pak, par, pbk, pbr))):
        a = a0[...] + a1[...]
        b = b0[...] + b1[...]
        low, high = jnp.where(first, b, a), jnp.where(first, a, b)
        tail = jnp.concatenate([low[:, cut:], high], axis=1)
        at = slice(i * rows, (i + 1) * rows)
        kv_keep[at, :] = tail
        kv_send[at, :] = tail.astype(BF16)
        top, bottom = low[:quarter, :cut], low[quarter:, :cut]
        at = slice(i * quarter, (i + 1) * quarter)
        q_keep[at, :] = jnp.where(stage == 0, top, bottom)
        q_send[at, :] = jnp.where(stage == 0, bottom, top).astype(BF16)


def keys_kernel(keep, got, cos, sin, turn, gain, out):
    raw = keep[...] + got[...].astype(F32)
    latent = raw[:, :KVL]
    inverse = lax.rsqrt(jnp.sum(latent * latent, axis=1, keepdims=True) / KVL + norm_eps)
    out[:, :KVL] = (latent * inverse * gain[...]).astype(BF16)
    rope = raw[:, KVL:]
    partner = dot_n(rope, turn[...], precision=lax.Precision.HIGHEST)
    out[:, KVL:] = (rope * cos[...] + partner * sin[...]).astype(BF16)


def attend_kernel(query_ref, k0_ref, k1_ref, bias_ref, peak_ref, total_ref, out_ref, packed_ref):
    query = query_ref[...]
    keys = k0_ref.shape[0]
    rows = query.shape[0]
    requests = bias_ref.shape[0] // 2
    heads = rows // requests
    bias = bias_ref[...]
    wide = jnp.concatenate(
        [jnp.broadcast_to(bias[r : r + 1], (heads, 2 * keys)) for r in range(requests)], axis=0
    )
    scores = jnp.concatenate([dot_t(query, k0_ref[...]), dot_t(query, k1_ref[...])], axis=1)
    scores = scores * softmax_scale + wide
    old_peak = peak_ref[...]
    peak = jnp.maximum(old_peak, jnp.max(scores, axis=1, keepdims=True))
    weights = jnp.where(wide < 0.0, 0.0, jnp.exp(scores - peak))
    carried = jnp.exp(old_peak - peak)
    total = jnp.sum(weights, axis=1, keepdims=True) + total_ref[...] * carried
    rounded = weights.astype(BF16)
    out = dot_n(rounded[:, :keys], k0_ref[:, :KVL]) + dot_n(rounded[:, keys:], k1_ref[:, :KVL])
    out = (out + out_ref[...] * carried) / total
    level = peak + jnp.log(total)
    packed_ref[:, :KVL] = out.astype(BF16)
    lead = level.astype(BF16).astype(F32)
    rest = (level - lead).astype(BF16).astype(F32)
    last = level - lead - rest
    lane = lax.broadcasted_iota(jnp.int32, (rows, 128), 1)
    tail = jnp.where(lane == 0, lead, jnp.where(lane == 1, rest, jnp.where(lane == 2, last, 0.0)))
    packed_ref[:, KVL:] = tail.astype(BF16)


def combine_kernel(*refs):
    parts, out = refs[:-1], refs[-1]
    levels = [jnp.sum(p[:, KVL:].astype(F32), axis=1, keepdims=True) for p in parts]
    top = functools.reduce(jnp.maximum, levels)
    shares = [jnp.exp(level - top) for level in levels]
    numer = sum(s * p[:, :KVL].astype(F32) for s, p in zip(shares, parts))
    out[...] = (numer / sum(shares)).astype(BF16)


def return_kernel(ids, kv_keep, kv_got, q_keep, q_got, low, high, send):
    stage = ids[3]
    rows = kv_keep.shape[0] // 2
    quarter = rows // 2
    start = pl.multiple_of(stage * quarter, 32)
    for i in range(2):
        at = pl.ds(i * rows + start, quarter)
        wide = kv_keep[at, :] + kv_got[at, :].astype(F32)
        near = slice(i * quarter, (i + 1) * quarter)
        short = q_keep[near, :] + q_got[near, :].astype(F32)
        if i == 0:
            low[...] = short
            high[...] = wide
        else:
            send[:, : short.shape[1]] = short.astype(BF16)
            send[:, short.shape[1] :] = wide.astype(BF16)


def query_kernel(ids, low, high, got, gain, *refs):
    sends, scratch = refs[:-1], refs[-1]
    odd = ids[2] % 2 == 1
    cut = low.shape[1]
    got_low, got_high = got[:, :cut].astype(F32), got[:, cut:].astype(F32)
    first = jnp.where(odd, got_low, low[...])
    second = jnp.where(odd, got_high, high[...])
    third = jnp.where(odd, low[...], got_low)
    rows = jnp.concatenate([first, second, third], axis=1)
    inverse = lax.rsqrt(jnp.sum(rows * rows, axis=1, keepdims=True) / QL + norm_eps)
    rows = (rows * inverse * gain[...]).astype(BF16)
    scratch[...] = rows
    width = QL // len(sends)
    lane = 2 * ids[3] + ids[1]
    for k, send in enumerate(sends):
        target = jnp.bitwise_xor(lane, k)
        send[...] = scratch[:, pl.ds(pl.multiple_of(target * width, 128), width)]


def place_kernel(ids, *refs):
    gots, out = refs[:-1], refs[-1]
    rows = gots[0].shape[0]
    lane = 2 * ids[3] + ids[1]
    for k, got in enumerate(gots):
        source = jnp.bitwise_xor(lane, k)
        order = 2 * (source % 2) + source // 2
        out[pl.ds(pl.multiple_of(order * rows, 32), rows), :] = got[...]


def call(kernel, shapes, specs, args, scratch=()):
    return pl.pallas_call(
        kernel,
        scratch_shapes=scratch,
        out_shape=shapes,
        in_specs=specs,
        out_specs=[VMEM] * len(shapes) if isinstance(shapes, list) else VMEM,
        cost_estimate=pl.CostEstimate(flops=20_000_000, bytes_accessed=2_000_000, transcendentals=0),
        compiler_params=pltpu.CompilerParams(vmem_limit_bytes=VMEM_GRANT),
    )(*args)


def shaped(*dims, kind=F32):
    return jax.ShapeDtypeStruct(dims, kind)


def body_pairs(*args):
    return pairs_step(*args)


def pairs_step(
    hidden_x,
    proj_weight,
    q_gain,
    kv_gain,
    old_cache,
    page_plan,
    block_table,
    split_lens,
    dec_query,
    new_key,
):
    n = lax.axis_size("dec")
    group, index = lax.axis_index("grp"), lax.axis_index("dec")
    stage, core = lax.axis_index("stg"), lax.axis_index("tp")
    ids = jnp.stack([group, core, index, stage]).astype(jnp.int32)
    tokens, feats = hidden_x.shape
    cols = proj_weight.shape[1]
    cut = QL - 2 * cols
    half = feats // 2
    pages = page_plan.shape[0]
    requests, heads, _ = dec_query.shape
    queries = requests * heads

    weight = lax.dynamic_slice_in_dim(proj_weight.T, group * half, half, axis=1)
    split = cols // 2 // 128 * 128
    pieces = {"head": weight[:split], "tail": weight[split:]}
    a_pairs = [(0, 2), (3, 1), (1, 0), (2, 3)]
    b_pairs = [(0, 0), (1, 2), (2, 1), (3, 3)]
    a_z, a_y, b_z, b_y = {}, {}, {}, {}
    for name in ("tail", "head"):
        a_z[name] = lax.ppermute(pieces[name], "dec", a_pairs)
    x_far = lax.ppermute(hidden_x, "dec", [(0, 1), (1, 0), (2, 3), (3, 2)])
    packed = jnp.concatenate(
        [page_plan.reshape(-1), block_table.reshape(-1), split_lens.reshape(-1)]
    ).reshape(1, -1)
    tables = [packed]
    for s in range(1, n):
        tables.append(lax.ppermute(packed, "dec", [((i + s) % n, i) for i in range(n)]))
    tables = jnp.pad(
        jnp.concatenate(tables, axis=0), ((0, 8 - n), (0, -packed.shape[1] % 128))
    )
    held, held_tail, held_head = pieces, *lax.optimization_barrier(
        (pieces["tail"], pieces["head"], a_z["head"])
    )[:2]
    held = {"tail": held_tail, "head": held_head}
    for name in ("tail", "head"):
        a_y[name] = swap(a_z[name], "grp")
        b_z[name] = lax.ppermute(held[name], "dec", b_pairs)
    for name in ("tail", "head"):
        b_y[name] = swap(b_z[name], "grp")
    a_weights = (a_z["head"], a_z["tail"], a_y["head"], a_y["tail"])
    b_weights = (b_z["head"], b_z["tail"], b_y["head"], b_y["tail"])

    query = dec_query.reshape(queries, KVW)
    padded_key = jnp.pad(new_key, ((0, 3 * requests), (0, 0)))
    peak, total, out, bias = call(
        functools.partial(old_kernel, n, pages),
        [shaped(queries, 1), shaped(queries, 1), shaped(queries, KVL), shaped(8, 2 * tokens)],
        [SMEM, VMEM, VMEM, VMEM, VMEM],
        (ids, tables, query, old_cache.reshape(-1, KVW), padded_key),
    )

    rows = tokens // 2
    partner = index + 1 - 2 * (index % 2)
    place = core * rows + jnp.arange(rows, dtype=jnp.int32)
    positions = jnp.concatenate([index * tokens + place, partner * tokens + place]).astype(F32)
    pair = jnp.arange(ROPE, dtype=jnp.int32) // 2
    frequency = jnp.power(F32(10000.0), -(2 * pair).astype(F32) / ROPE)
    angles = positions[:, None] * frequency[None, :]
    source = jnp.arange(ROPE, dtype=jnp.int32)[:, None]
    target = jnp.arange(ROPE, dtype=jnp.int32)[None, :]
    turn = jnp.where(
        source == target + 1,
        jnp.where(target % 2 == 0, -1.0, 0.0),
        jnp.where((source + 1 == target) & (target % 2 == 1), 1.0, 0.0),
    )
    early_ids, cos, sin, turn, kv_scale, q_scale = lax.optimization_barrier(
        (ids, jnp.cos(angles), jnp.sin(angles), turn, kv_gain.reshape(1, -1), q_gain.reshape(1, -1))
    )
    a_near = matmul(early_ids, (hidden_x,), a_weights)
    a_far = matmul(ids, (x_far,), a_weights)
    b_both = matmul(ids, (hidden_x, x_far), b_weights)
    sums = []
    for (send, keep) in (a_near, b_both[:2], a_far, b_both[2:]):
        sums += [keep, swap(send, "tp")]
    rows = tokens // 2
    quarter = rows // 2
    kv_send, kv_keep, q_send, q_keep = call(
        middle_kernel,
        [
            shaped(2 * rows, KVW, kind=BF16),
            shaped(2 * rows, KVW),
            shaped(rows, cut, kind=BF16),
            shaped(rows, cut),
        ],
        [SMEM] + [VMEM] * 8,
        (ids, *sums),
    )
    kv_got = swap(kv_send, "stg")
    q_got = swap(q_send, "stg")

    key_rows = call(
        keys_kernel,
        shaped(2 * rows, KVW, kind=BF16),
        [VMEM] * 6,
        (kv_keep, kv_got, cos, sin, turn, kv_scale),
    )
    far_keys = swap(key_rows, "tp")
    part_out = call(
        attend_kernel,
        shaped(queries, KVL + 128, kind=BF16),
        [VMEM] * 7,
        (query, key_rows, far_keys, bias, peak, total, out),
    )
    parts = [part_out]
    for s in range(1, n):
        parts.append(
            lax.ppermute(part_out, "dec", [((i + s) % n, i) for i in range(n)])
        )
    attn = call(combine_kernel, shaped(queries, KVL, kind=BF16), [VMEM] * n, tuple(parts))

    low, high, back = call(
        return_kernel,
        [shaped(quarter, cut), shaped(quarter, KVW), shaped(quarter, cut + KVW, kind=BF16)],
        [SMEM] + [VMEM] * 4,
        (ids, kv_keep, kv_got, q_keep, q_got),
    )
    back = lax.ppermute(back, "dec", [(0, 1), (1, 0), (2, 3), (3, 2)])
    lanes = 4
    width = QL // lanes
    tile = shaped(quarter, width, kind=BF16)
    blocks = call(
        query_kernel,
        [tile] * lanes,
        [SMEM] + [VMEM] * 4,
        (ids, low, high, back, q_scale),
        scratch=[pltpu.VMEM((quarter, QL), BF16)],
    )
    gots = [blocks[0]]
    for k in range(1, lanes):
        gots.append(
            lax.ppermute(blocks[k], ("stg", "tp"), [(i, i ^ k) for i in range(lanes)])
        )
    q_latent = call(
        place_kernel, shaped(tokens, width, kind=BF16), [SMEM] + [VMEM] * lanes, (ids, *gots)
    )
    return (q_latent, attn.reshape(requests, heads, KVL))


def solution(mesh):
    sizes = dict(mesh.shape)
    pairs = sizes["dec"] == 4 and sizes["grp"] == sizes["stg"] == sizes["tp"] == 2
    return jax.shard_map(
        body_pairs if pairs else body_general,
        mesh=mesh,
        in_specs=(
            P(("grp", "dec"), ("stg", "tp")),
            P(("stg", "tp"), "dec"),
            P(),
            P(),
            P(("grp", "dec"), None, None),
            P(("grp", "dec"), None),
            P(("grp", "dec"), None, None),
            P("grp", "dec"),
            P("grp", ("stg", "tp"), None),
            P("grp", None),
        ),
        out_specs=(P(("grp", "dec"), ("stg", "tp")), P("grp", ("stg", "tp"), None)),
        check_vma=False,
    )
```

```python
import functools

import jax
import jax.numpy as jnp
from jax import lax
from jax.experimental import pallas as pl
from jax.experimental.pallas import tpu as pltpu
from jax.sharding import PartitionSpec as P


QL = 1536
KVL = 512
ROPE = 64
PAGE = 32
KVW = KVL + ROPE
MASKED = -1e30

softmax_scale = 192.0 ** (-0.5)
norm_eps = 1e-06


def combined_all(part, axis, combine):
    gathered = jax.tree.map(lambda a: lax.all_gather(a, axis), part)

    def take(source):
        return jax.tree.map(lambda a: lax.dynamic_index_in_dim(a, source, 0, False), gathered)

    return lax.fori_loop(
        1, lax.axis_size(axis), lambda source, state: combine(state, take(source)), take(0)
    )


def rope_rotate(matrix, col_start, positions):
    col_count = matrix.shape[1]
    columns = col_start + jnp.arange(col_count, dtype=jnp.int32)
    is_rope = columns >= KVL
    pair_index = jnp.maximum(columns - KVL, 0) // 2
    frequency = jnp.power(jnp.float32(10000.0), -(2 * pair_index).astype(jnp.float32) / ROPE)
    angles = positions[:, None] * frequency[None, :]
    cosine = jnp.where(is_rope[None, :], jnp.cos(angles), 1.0)
    sine_part = jnp.where(is_rope[None, :], jnp.sin(angles), 0.0)
    paired = matrix.reshape(matrix.shape[0], col_count // 2, 2)
    partner = jnp.stack([-paired[:, :, 1], paired[:, :, 0]], axis=2).reshape(matrix.shape)
    return matrix * cosine + partner * sine_part


def kv_finish(matrix, col_start, latent_sq, kv_gain, positions):
    col_count = matrix.shape[1]
    columns = col_start + jnp.arange(col_count, dtype=jnp.int32)
    gain_full = jnp.concatenate([kv_gain, jnp.ones((ROPE,), jnp.float32)])
    gain_cols = lax.dynamic_slice_in_dim(gain_full, col_start, col_count)
    inverse = lax.rsqrt(latent_sq / KVL + norm_eps)
    row_scale = jnp.where(columns[None, :] < KVL, inverse[:, None] * gain_cols[None, :], 1.0)
    return rope_rotate(matrix * row_scale, col_start, positions).astype(jnp.bfloat16)


def pack_pages(kv_pages, page_table, owner_count, capacity):
    owners = page_table[:, 0]
    slot_ids = page_table[:, 1]
    page_ids = jnp.arange(kv_pages.shape[0], dtype=jnp.int32)
    earlier = (owners[:, None] == owners[None, :]) & (page_ids[None, :] < page_ids[:, None])
    ranking = jnp.sum(earlier.astype(jnp.int32), axis=1)
    targets = owners * capacity + ranking
    places = jnp.arange(owner_count * capacity, dtype=jnp.int32)
    matches = targets[None, :] == places[:, None]
    source_ids = jnp.sum(jnp.where(matches, page_ids[None, :], 0), axis=1)
    filled = jnp.any(matches, axis=1)
    chosen = jnp.where(
        filled[:, None, None], jnp.take(kv_pages, source_ids, axis=0), jnp.zeros((), kv_pages.dtype)
    )
    labels = jnp.where(filled, jnp.take(slot_ids, source_ids), -1).astype(jnp.bfloat16)
    return (
        chosen.reshape(owner_count, capacity, kv_pages.shape[1], kv_pages.shape[2]),
        labels.reshape(owner_count, capacity),
    )


def place_pages(old_cache, got_pages, got_labels):
    flat_pages = got_pages.reshape(-1, old_cache.shape[1], old_cache.shape[2])
    label_ids = got_labels.reshape(-1).astype(jnp.int32)
    slot_ids = jnp.arange(old_cache.shape[0], dtype=jnp.int32)
    arrival_ids = jnp.arange(label_ids.shape[0], dtype=jnp.int32)
    matches = label_ids[None, :] == slot_ids[:, None]
    source_ids = jnp.sum(jnp.where(matches, arrival_ids[None, :], 0), axis=1)
    arrived = jnp.any(matches, axis=1)
    return jnp.where(arrived[:, None, None], jnp.take(flat_pages, source_ids, axis=0), old_cache)


def combine_parts(former, latter):
    overall = jnp.maximum(former[0], latter[0])
    front_scale = jnp.exp(former[0] - overall)
    back_scale = jnp.exp(latter[0] - overall)
    return (
        overall,
        former[1] * front_scale + latter[1] * back_scale,
        former[2] * front_scale[:, :, None] + latter[2] * back_scale[:, :, None],
    )


def body_general(
    hidden_x,
    proj_weight,
    q_gain,
    kv_gain,
    old_cache,
    page_plan,
    block_table,
    split_lens,
    dec_query,
    new_key,
):
    projected = jnp.dot(
        hidden_x,
        lax.all_gather(proj_weight, "dec", axis=1, tiled=True),
        preferred_element_type=jnp.float32,
    )
    query_part = projected[:, :QL]
    kv_part = projected[:, QL:]
    tokens_here = hidden_x.shape[0]
    positions = (
        lax.axis_index("dec") * tokens_here + jnp.arange(tokens_here, dtype=jnp.int32)
    ).astype(jnp.float32)
    lane_count = lax.axis_size(("stg", "tp"))
    lane_index = lax.axis_index(("stg", "tp"))
    owner_count = lax.axis_size("dec")
    page_count = page_plan.shape[0]
    capacity = max(2, -(-page_count // owner_count))
    query_width = QL // lane_count
    query_cols, kv_cols = (
        lax.psum_scatter(query_part, ("stg", "tp"), scatter_dimension=1, tiled=True),
        lax.psum_scatter(kv_part, ("stg", "tp"), scatter_dimension=1, tiled=True),
    )
    kv_width = kv_cols.shape[1]
    col_start = lane_index * kv_width
    columns = col_start + jnp.arange(kv_width, dtype=jnp.int32)
    latent_part_sq = jnp.sum(jnp.where(columns[None, :] < KVL, kv_cols * kv_cols, 0.0), axis=1)
    query_sq, latent_sq = lax.psum(
        (jnp.sum(query_cols * query_cols, axis=1), latent_part_sq), ("stg", "tp")
    )
    kv_rows = kv_finish(kv_cols, col_start, latent_sq, kv_gain, positions)
    kv_pages = kv_rows.reshape(page_count, PAGE, kv_width)
    send_pages, send_labels = pack_pages(kv_pages, page_plan, owner_count, capacity)
    got_slices, got_labels = (
        lax.all_to_all(send_pages, "dec", split_axis=0, concat_axis=0, tiled=True),
        lax.all_to_all(send_labels, "dec", split_axis=0, concat_axis=0, tiled=True),
    )
    got_pages = lax.all_gather(got_slices, ("stg", "tp"), axis=3, tiled=True)
    query_gain = lax.dynamic_slice_in_dim(q_gain, lane_index * query_width, query_width)
    q_latent = (
        query_cols * lax.rsqrt(query_sq / QL + norm_eps)[:, None] * query_gain[None, :]
    ).astype(jnp.bfloat16)
    cache = place_pages(old_cache, got_pages, got_labels)
    slot_table = block_table[0]
    request_count = slot_table.shape[0]
    key_rows = jnp.take(cache, slot_table.reshape(-1), axis=0).reshape(
        request_count, -1, cache.shape[2]
    )
    scores = (
        jnp.einsum("rhc,rlc->rhl", dec_query, key_rows, preferred_element_type=jnp.float32)
        * softmax_scale
    )
    live_mask = jnp.arange(key_rows.shape[1], dtype=jnp.int32)[None, :] < split_lens[:, 0][:, None]
    scores = jnp.where(live_mask[:, None, :], scores, -1e30)
    row_peak = jnp.max(scores, axis=2)
    weights = jnp.where(live_mask[:, None, :], jnp.exp(scores - row_peak[:, :, None]), 0.0)
    row_total = jnp.sum(weights, axis=2)
    rounded = weights.astype(jnp.bfloat16)
    partial_out = jnp.einsum(
        "rhl,rlc->rhc", rounded, key_rows[:, :, :KVL], preferred_element_type=jnp.float32
    )
    peak_all, total_all, output_all = combined_all(
        (row_peak, row_total, partial_out), "dec", combine_parts
    )
    self_score = (
        jnp.einsum("rhc,rc->rh", dec_query, new_key, preferred_element_type=jnp.float32)
        * softmax_scale
    )
    overall = jnp.maximum(peak_all, self_score)
    carried = jnp.exp(peak_all - overall)
    self_weight = jnp.exp(self_score - overall)
    denom = total_all * carried + self_weight
    numer = output_all * carried[:, :, None] + self_weight[:, :, None] * new_key[
        :, None, :KVL
    ].astype(jnp.float32)
    attn_latent = (numer / denom[:, :, None]).astype(jnp.bfloat16)
    return (q_latent, attn_latent)


VMEM = pl.BlockSpec(memory_space=pltpu.VMEM)
SMEM = pl.BlockSpec(memory_space=pltpu.SMEM)
VMEM_GRANT = 16 * 2**20
F32 = jnp.float32
BF16 = jnp.bfloat16


def swap(a, axis):
    return lax.ppermute(a, axis, [(0, 1), (1, 0)])


def dot_t(a, b, **kw):
    return lax.dot_general(a, b, (((1,), (1,)), ((), ())), preferred_element_type=F32, **kw)


def dot_n(a, b, **kw):
    return lax.dot_general(a, b, (((1,), (0,)), ((), ())), preferred_element_type=F32, **kw)


def matmul_kernel(blocks, own, ids, *refs):
    group, core, index = ids[0], ids[1], ids[2]
    xs, refs = refs[:blocks], refs[blocks:]
    (head_z, tail_z, head_y, tail_y), refs = refs[:4], refs[4:]
    weight, outs = (refs[0], refs[1:]) if own else (None, refs)
    half = head_z.shape[1]
    split = head_z.shape[0]
    here = pl.ds(pl.multiple_of(group * half, 128), half)
    there = pl.ds(pl.multiple_of((1 - group) * half, 128), half)
    outer = (index == 0) | (index == 3)
    for z, y, at in ((head_z, head_y, slice(0, split)), (tail_z, tail_y, slice(split, None))):
        w_here, w_there = z[...], y[...]
        if own:
            w_here = jnp.where(outer, weight[at, here], w_here)
            w_there = jnp.where(outer, weight[at, there], w_there)
        for i, x_ref in enumerate(xs):
            send, keep = outs[2 * i], outs[2 * i + 1]
            rows = send.shape[0]
            out = dot_t(x_ref[:, here], w_here) + dot_t(x_ref[:, there], w_there)
            top, bottom = out[:rows], out[rows:]
            send[:, at] = jnp.where(core == 0, bottom, top)
            keep[:, at] = jnp.where(core == 0, top, bottom)


def matmul(ids, xs, weights, own=()):
    rows, feats = xs[0].shape
    cols = weights[0].shape[0] + weights[1].shape[0]
    blocks = len(xs)
    return pl.pallas_call(
        functools.partial(matmul_kernel, blocks, bool(own)),
        in_specs=[SMEM] + [VMEM] * (blocks + 4 + len(own)),
        out_specs=[VMEM] * (2 * blocks),
        out_shape=[jax.ShapeDtypeStruct((rows // 2, cols), F32)] * (2 * blocks),
        cost_estimate=pl.CostEstimate(
            flops=2 * rows * feats * cols * blocks,
            bytes_accessed=8 * rows * cols * blocks,
            transcendentals=0,
        ),
        compiler_params=pltpu.CompilerParams(vmem_limit_bytes=VMEM_GRANT),
        name="project",
    )(ids, *xs, *weights, *own)


def turn_kernel(out):
    source = lax.broadcasted_iota(jnp.int32, out.shape, 0)
    target = lax.broadcasted_iota(jnp.int32, out.shape, 1)
    down = (source == target + 1) & (target % 2 == 0)
    up = (source + 1 == target) & (target % 2 == 1)
    out[...] = jnp.where(down, -1.0, jnp.where(up, 1.0, 0.0))


def old_kernel(n, pages, ids, tab_ref, query_ref, rows_ref, own_ref, peak_ref, total_ref, out_ref, bias_ref):
    index, core = ids[2], ids[1]
    query = query_ref[...]
    keys = rows_ref.shape[0]
    requests = own_ref.shape[0] // 4
    heads = query.shape[0] // requests
    base = 2 * pages
    slots = keys // PAGE
    per = slots // requests

    def iota(rows, cols, axis):
        return lax.broadcasted_iota(jnp.int32, (rows, cols), axis)

    size = tab_ref.shape[1]
    diagonal = iota(size, size, 0) == iota(size, size, 1)
    columns = [
        jnp.sum(jnp.where(diagonal, tab_ref[s : s + 1, :], 0), axis=1, keepdims=True)
        for s in range(n)
    ]
    entry = iota(slots, 1, 0)
    readers = entry // per

    def limits(column):
        lengths = jnp.zeros((slots, 1), jnp.int32)
        for r in range(requests):
            at = base + slots + r
            lengths = jnp.where(readers == r, column[at : at + 1, :], lengths)
        return lengths - PAGE * (entry % per)

    def lookup(hit, values):
        return jnp.sum(jnp.where(hit, values, 0), axis=0, keepdims=True)

    page = iota(1, keys, 1) // PAGE
    hit = columns[0][base : base + slots, :] == page
    limit = lookup(hit, limits(columns[0]))
    reader = lookup(hit, readers)
    is_slot = iota(base, 1, 0) % 2 == 1
    taken = jnp.zeros((1, keys), jnp.int32)
    odd_row = iota(base, base, 0)
    follows = (iota(base, base, 1) == odd_row - 1) & (odd_row % 2 == 1)
    for s in range(n):
        plan = columns[s][:base, :]
        owners = jnp.sum(jnp.where(follows, tab_ref[s : s + 1, :base], 0), axis=1, keepdims=True)
        here = is_slot & (owners == index)
        taken = taken + jnp.sum(jnp.where(here & (plan == page), 1, 0), axis=0, keepdims=True)
    limit = jnp.where(taken > 0, 0, limit)
    live = (iota(1, keys, 1) % PAGE) < limit
    bias = jnp.where(live & (reader == iota(8, keys, 0)), 0.0, MASKED)
    wide = jnp.concatenate(
        [jnp.broadcast_to(bias[r : r + 1], (heads, keys)) for r in range(requests)], axis=0
    )
    scores = dot_t(query, rows_ref[...]) * softmax_scale + wide
    own = dot_t(query, own_ref[...]) * softmax_scale
    mine = iota(*own.shape, 0) // heads == iota(*own.shape, 1)
    own = jnp.sum(jnp.where(mine, own, 0.0), axis=1, keepdims=True)
    own = jnp.where(index == 0, own, MASKED)
    peak = jnp.maximum(jnp.max(scores, axis=1, keepdims=True), own)
    weights = jnp.where(wide < 0.0, 0.0, jnp.exp(scores - peak))
    own_weight = jnp.where(index == 0, jnp.exp(own - peak), 0.0)
    peak_ref[...] = peak
    total_ref[...] = jnp.sum(weights, axis=1, keepdims=True) + own_weight
    out = dot_n(weights.astype(BF16), rows_ref[:, :KVL])
    own_rows = own_ref[:, :KVL].astype(F32)
    latent = jnp.concatenate(
        [jnp.broadcast_to(own_rows[r : r + 1], (heads, KVL)) for r in range(requests)], axis=0
    )
    out_ref[...] = out + own_weight * latent

    width = bias_ref.shape[1]
    half = pages // 2
    spot = iota(1, width, 1) // PAGE
    which = jnp.where(spot // pages == 1, 1 - core, core) * half + spot % half
    partner = (spot % pages) // half == 1
    line = iota(base, width, 0)
    plan = jnp.where(partner, columns[n - 1][:base, :], columns[0][:base, :])
    plan = jnp.where(line % 2 == 1, plan, plan * (2 * slots))
    code = jnp.sum(jnp.where(line // 2 == which, plan, 0), axis=0, keepdims=True)
    limit = jnp.zeros((1, width), jnp.int32)
    reader = jnp.zeros((1, width), jnp.int32)
    for s in range(n):
        owner = (index + s) % n
        hit = columns[s][base : base + slots, :] + owner * (2 * slots) == code
        limit = limit + lookup(hit, limits(columns[s]))
        reader = reader + lookup(hit, readers)
    limit = jnp.where(index % 2 == 1, limit, 0)
    live = (iota(1, width, 1) % PAGE) < limit
    bias_ref[...] = jnp.where(live & (reader == iota(8, width, 0)), 0.0, MASKED)


def middle_kernel(ids, *refs):
    (ak, ar, bk, br, pak, par, pbk, pbr, kv_send, kv_keep, q_send, q_keep) = refs
    first, stage = ids[2] < 2, ids[3]
    rows, cols = ak.shape
    cut = QL - 2 * cols
    quarter = rows // 2
    for i, (a0, a1, b0, b1) in enumerate(((ak, ar, bk, br), (pak, par, pbk, pbr))):
        a = a0[...] + a1[...]
        b = b0[...] + b1[...]
        low, high = jnp.where(first, b, a), jnp.where(first, a, b)
        tail = jnp.concatenate([low[:, cut:], high], axis=1)
        at = slice(i * rows, (i + 1) * rows)
        kv_keep[at, :] = tail
        kv_send[at, :] = tail.astype(BF16)
        top, bottom = low[:quarter, :cut], low[quarter:, :cut]
        at = slice(i * quarter, (i + 1) * quarter)
        q_keep[at, :] = jnp.where(stage == 0, top, bottom)
        q_send[at, :] = jnp.where(stage == 0, bottom, top).astype(BF16)


def keys_kernel(keep, got, cos, sin, turn, gain, out):
    raw = keep[...] + got[...].astype(F32)
    latent = raw[:, :KVL]
    inverse = lax.rsqrt(jnp.sum(latent * latent, axis=1, keepdims=True) / KVL + norm_eps)
    out[:, :KVL] = (latent * inverse * gain[...]).astype(BF16)
    rope = raw[:, KVL:]
    partner = dot_n(rope, turn[...], precision=lax.Precision.HIGHEST)
    out[:, KVL:] = (rope * cos[...] + partner * sin[...]).astype(BF16)


def attend_kernel(query_ref, k0_ref, k1_ref, bias_ref, peak_ref, total_ref, out_ref, packed_ref):
    query = query_ref[...]
    keys = k0_ref.shape[0]
    rows = query.shape[0]
    requests = bias_ref.shape[0] // 2
    heads = rows // requests
    bias = bias_ref[...]
    wide = jnp.concatenate(
        [jnp.broadcast_to(bias[r : r + 1], (heads, 2 * keys)) for r in range(requests)], axis=0
    )
    scores = jnp.concatenate([dot_t(query, k0_ref[...]), dot_t(query, k1_ref[...])], axis=1)
    scores = scores * softmax_scale + wide
    old_peak = peak_ref[...]
    peak = jnp.maximum(old_peak, jnp.max(scores, axis=1, keepdims=True))
    weights = jnp.where(wide < 0.0, 0.0, jnp.exp(scores - peak))
    carried = jnp.exp(old_peak - peak)
    total = jnp.sum(weights, axis=1, keepdims=True) + total_ref[...] * carried
    rounded = weights.astype(BF16)
    out = dot_n(rounded[:, :keys], k0_ref[:, :KVL]) + dot_n(rounded[:, keys:], k1_ref[:, :KVL])
    out = (out + out_ref[...] * carried) / total
    level = peak + jnp.log(total)
    packed_ref[:, :KVL] = out.astype(BF16)
    lead = level.astype(BF16).astype(F32)
    rest = (level - lead).astype(BF16).astype(F32)
    last = level - lead - rest
    lane = lax.broadcasted_iota(jnp.int32, (rows, 128), 1)
    tail = jnp.where(lane == 0, lead, jnp.where(lane == 1, rest, jnp.where(lane == 2, last, 0.0)))
    packed_ref[:, KVL:] = tail.astype(BF16)


def combine_kernel(*refs):
    parts, out = refs[:-1], refs[-1]
    levels = [jnp.sum(p[:, KVL:].astype(F32), axis=1, keepdims=True) for p in parts]
    top = functools.reduce(jnp.maximum, levels)
    shares = [jnp.exp(level - top) for level in levels]
    numer = sum(s * p[:, :KVL].astype(F32) for s, p in zip(shares, parts))
    out[...] = (numer / sum(shares)).astype(BF16)


def return_kernel(ids, kv_keep, kv_got, q_keep, q_got, low, high, send):
    stage = ids[3]
    rows = kv_keep.shape[0] // 2
    quarter = rows // 2
    start = pl.multiple_of(stage * quarter, 32)
    for i in range(2):
        at = pl.ds(i * rows + start, quarter)
        wide = kv_keep[at, :] + kv_got[at, :].astype(F32)
        near = slice(i * quarter, (i + 1) * quarter)
        short = q_keep[near, :] + q_got[near, :].astype(F32)
        if i == 0:
            low[...] = short
            high[...] = wide
        else:
            send[:, : short.shape[1]] = short.astype(BF16)
            send[:, short.shape[1] :] = wide.astype(BF16)


def query_kernel(ids, low, high, got, gain, *refs):
    sends, scratch = refs[:-1], refs[-1]
    odd = ids[2] % 2 == 1
    cut = low.shape[1]
    got_low, got_high = got[:, :cut].astype(F32), got[:, cut:].astype(F32)
    first = jnp.where(odd, got_low, low[...])
    second = jnp.where(odd, got_high, high[...])
    third = jnp.where(odd, low[...], got_low)
    rows = jnp.concatenate([first, second, third], axis=1)
    inverse = lax.rsqrt(jnp.sum(rows * rows, axis=1, keepdims=True) / QL + norm_eps)
    rows = (rows * inverse * gain[...]).astype(BF16)
    scratch[...] = rows
    width = QL // len(sends)
    lane = 2 * ids[3] + ids[1]
    for k, send in enumerate(sends):
        target = jnp.bitwise_xor(lane, k)
        send[...] = scratch[:, pl.ds(pl.multiple_of(target * width, 128), width)]


def place_kernel(ids, *refs):
    gots, out = refs[:-1], refs[-1]
    rows = gots[0].shape[0]
    lane = 2 * ids[3] + ids[1]
    for k, got in enumerate(gots):
        source = jnp.bitwise_xor(lane, k)
        order = 2 * (source % 2) + source // 2
        out[pl.ds(pl.multiple_of(order * rows, 32), rows), :] = got[...]


def call(kernel, shapes, specs, args, scratch=()):
    return pl.pallas_call(
        kernel,
        scratch_shapes=scratch,
        out_shape=shapes,
        in_specs=specs,
        out_specs=[VMEM] * len(shapes) if isinstance(shapes, list) else VMEM,
        cost_estimate=pl.CostEstimate(flops=20_000_000, bytes_accessed=2_000_000, transcendentals=0),
        compiler_params=pltpu.CompilerParams(vmem_limit_bytes=VMEM_GRANT),
    )(*args)


def shaped(*dims, kind=F32):
    return jax.ShapeDtypeStruct(dims, kind)


def body_pairs(*args):
    return pairs_step(*args)


def pairs_step(
    hidden_x,
    proj_weight,
    q_gain,
    kv_gain,
    old_cache,
    page_plan,
    block_table,
    split_lens,
    dec_query,
    new_key,
):
    n = lax.axis_size("dec")
    group, index = lax.axis_index("grp"), lax.axis_index("dec")
    stage, core = lax.axis_index("stg"), lax.axis_index("tp")
    ids = jnp.stack([group, core, index, stage]).astype(jnp.int32)
    tokens, feats = hidden_x.shape
    cols = proj_weight.shape[1]
    cut = QL - 2 * cols
    half = feats // 2
    pages = page_plan.shape[0]
    requests, heads, _ = dec_query.shape
    queries = requests * heads

    weight = proj_weight.T
    split = cols // 2 // 128 * 128
    pieces = {
        "tail": lax.dynamic_slice(weight, (split, group * half), (cols - split, half)),
        "head": lax.dynamic_slice(weight, (0, group * half), (split, half)),
    }
    a_pairs = [(0, 2), (3, 1), (1, 0), (2, 3)]
    b_pairs = [(1, 2), (2, 1)]
    inner = [(g * n + i, (1 - g) * n + i) for g in range(2) for i in (1, 2)]
    a_z, a_y, b_z, b_y = {}, {}, {}, {}
    for name in ("tail", "head"):
        a_z[name] = lax.ppermute(pieces[name], "dec", a_pairs)
    x_far = lax.ppermute(hidden_x, "dec", [(0, 1), (1, 0), (2, 3), (3, 2)])
    packed = jnp.concatenate(
        [page_plan.reshape(-1), block_table.reshape(-1), split_lens.reshape(-1)]
    ).reshape(1, -1)
    tables = [packed]
    for s in range(1, n):
        tables.append(lax.ppermute(packed, "dec", [((i + s) % n, i) for i in range(n)]))
    tables = jnp.pad(
        jnp.concatenate(tables, axis=0), ((0, 8 - n), (0, -packed.shape[1] % 128))
    )
    held, held_tail, held_head = pieces, *lax.optimization_barrier(
        (pieces["tail"], pieces["head"], a_z["head"])
    )[:2]
    held = {"tail": held_tail, "head": held_head}
    for name in ("tail", "head"):
        a_y[name] = swap(a_z[name], "grp")
        b_z[name] = lax.ppermute(held[name], "dec", b_pairs)
    for name in ("tail", "head"):
        b_y[name] = lax.ppermute(b_z[name], ("grp", "dec"), inner)
    a_weights = (a_z["head"], a_z["tail"], a_y["head"], a_y["tail"])
    b_weights = (b_z["head"], b_z["tail"], b_y["head"], b_y["tail"])

    query = dec_query.reshape(queries, KVW)
    padded_key = jnp.pad(new_key, ((0, 3 * requests), (0, 0)))
    peak, total, out, bias = call(
        functools.partial(old_kernel, n, pages),
        [shaped(queries, 1), shaped(queries, 1), shaped(queries, KVL), shaped(8, 2 * tokens)],
        [SMEM, VMEM, VMEM, VMEM, VMEM],
        (ids, tables, query, old_cache.reshape(-1, KVW), padded_key),
    )

    rows = tokens // 2
    partner = index + 1 - 2 * (index % 2)
    place = core * rows + jnp.arange(rows, dtype=jnp.int32)
    positions = jnp.concatenate([index * tokens + place, partner * tokens + place]).astype(F32)
    pair = jnp.arange(ROPE, dtype=jnp.int32) // 2
    frequency = jnp.power(F32(10000.0), -(2 * pair).astype(F32) / ROPE)
    angles = positions[:, None] * frequency[None, :]
    turn = call(turn_kernel, shaped(ROPE, ROPE), [], ())
    early_ids, cos, sin, turn, kv_scale, q_scale = lax.optimization_barrier(
        (ids, jnp.cos(angles), jnp.sin(angles), turn, kv_gain.reshape(1, -1), q_gain.reshape(1, -1))
    )
    a_near = matmul(early_ids, (hidden_x,), a_weights)
    a_far = matmul(ids, (x_far,), a_weights)
    b_both = matmul(ids, (hidden_x, x_far), b_weights, own=(weight,))
    sums = []
    for (send, keep) in (a_near, b_both[:2], a_far, b_both[2:]):
        sums += [keep, swap(send, "tp")]
    rows = tokens // 2
    quarter = rows // 2
    kv_send, kv_keep, q_send, q_keep = call(
        middle_kernel,
        [
            shaped(2 * rows, KVW, kind=BF16),
            shaped(2 * rows, KVW),
            shaped(rows, cut, kind=BF16),
            shaped(rows, cut),
        ],
        [SMEM] + [VMEM] * 8,
        (ids, *sums),
    )
    kv_got = swap(kv_send, "stg")
    q_got = swap(q_send, "stg")

    key_rows = call(
        keys_kernel,
        shaped(2 * rows, KVW, kind=BF16),
        [VMEM] * 6,
        (kv_keep, kv_got, cos, sin, turn, kv_scale),
    )
    far_keys = swap(key_rows, "tp")
    part_out = call(
        attend_kernel,
        shaped(queries, KVL + 128, kind=BF16),
        [VMEM] * 7,
        (query, key_rows, far_keys, bias, peak, total, out),
    )
    parts = [part_out]
    for s in range(1, n):
        parts.append(
            lax.ppermute(part_out, "dec", [((i + s) % n, i) for i in range(n)])
        )
    attn = call(combine_kernel, shaped(queries, KVL, kind=BF16), [VMEM] * n, tuple(parts))

    low, high, back = call(
        return_kernel,
        [shaped(quarter, cut), shaped(quarter, KVW), shaped(quarter, cut + KVW, kind=BF16)],
        [SMEM] + [VMEM] * 4,
        (ids, kv_keep, kv_got, q_keep, q_got),
    )
    back = lax.ppermute(back, "dec", [(0, 1), (1, 0), (2, 3), (3, 2)])
    lanes = 4
    width = QL // lanes
    tile = shaped(quarter, width, kind=BF16)
    blocks = call(
        query_kernel,
        [tile] * lanes,
        [SMEM] + [VMEM] * 4,
        (ids, low, high, back, q_scale),
        scratch=[pltpu.VMEM((quarter, QL), BF16)],
    )
    gots = [blocks[0]]
    for k in range(1, lanes):
        gots.append(
            lax.ppermute(blocks[k], ("stg", "tp"), [(i, i ^ k) for i in range(lanes)])
        )
    q_latent = call(
        place_kernel, shaped(tokens, width, kind=BF16), [SMEM] + [VMEM] * lanes, (ids, *gots)
    )
    return (q_latent, attn.reshape(requests, heads, KVL))


def solution(mesh):
    sizes = dict(mesh.shape)
    pairs = sizes["dec"] == 4 and sizes["grp"] == sizes["stg"] == sizes["tp"] == 2
    return jax.shard_map(
        body_pairs if pairs else body_general,
        mesh=mesh,
        in_specs=(
            P(("grp", "dec"), ("stg", "tp")),
            P(("stg", "tp"), "dec"),
            P(),
            P(),
            P(("grp", "dec"), None, None),
            P(("grp", "dec"), None),
            P(("grp", "dec"), None, None),
            P("grp", "dec"),
            P("grp", ("stg", "tp"), None),
            P("grp", None),
        ),
        out_specs=(P(("grp", "dec"), ("stg", "tp")), P("grp", ("stg", "tp"), None)),
        check_vma=False,
    )
```

```python
import functools

import jax
import jax.numpy as jnp
from jax import lax
from jax.experimental import pallas as pl
from jax.experimental.pallas import tpu as pltpu
from jax.sharding import PartitionSpec as P


QL = 1536
KVL = 512
ROPE = 64
PAGE = 32
KVW = KVL + ROPE
MASKED = -1e30

softmax_scale = 192.0 ** (-0.5)
norm_eps = 1e-06


def combined_all(part, axis, combine):
    gathered = jax.tree.map(lambda a: lax.all_gather(a, axis), part)

    def take(source):
        return jax.tree.map(lambda a: lax.dynamic_index_in_dim(a, source, 0, False), gathered)

    return lax.fori_loop(
        1, lax.axis_size(axis), lambda source, state: combine(state, take(source)), take(0)
    )


def rope_rotate(matrix, col_start, positions):
    col_count = matrix.shape[1]
    columns = col_start + jnp.arange(col_count, dtype=jnp.int32)
    is_rope = columns >= KVL
    pair_index = jnp.maximum(columns - KVL, 0) // 2
    frequency = jnp.power(jnp.float32(10000.0), -(2 * pair_index).astype(jnp.float32) / ROPE)
    angles = positions[:, None] * frequency[None, :]
    cosine = jnp.where(is_rope[None, :], jnp.cos(angles), 1.0)
    sine_part = jnp.where(is_rope[None, :], jnp.sin(angles), 0.0)
    paired = matrix.reshape(matrix.shape[0], col_count // 2, 2)
    partner = jnp.stack([-paired[:, :, 1], paired[:, :, 0]], axis=2).reshape(matrix.shape)
    return matrix * cosine + partner * sine_part


def kv_finish(matrix, col_start, latent_sq, kv_gain, positions):
    col_count = matrix.shape[1]
    columns = col_start + jnp.arange(col_count, dtype=jnp.int32)
    gain_full = jnp.concatenate([kv_gain, jnp.ones((ROPE,), jnp.float32)])
    gain_cols = lax.dynamic_slice_in_dim(gain_full, col_start, col_count)
    inverse = lax.rsqrt(latent_sq / KVL + norm_eps)
    row_scale = jnp.where(columns[None, :] < KVL, inverse[:, None] * gain_cols[None, :], 1.0)
    return rope_rotate(matrix * row_scale, col_start, positions).astype(jnp.bfloat16)


def pack_pages(kv_pages, page_table, owner_count, capacity):
    owners = page_table[:, 0]
    slot_ids = page_table[:, 1]
    page_ids = jnp.arange(kv_pages.shape[0], dtype=jnp.int32)
    earlier = (owners[:, None] == owners[None, :]) & (page_ids[None, :] < page_ids[:, None])
    ranking = jnp.sum(earlier.astype(jnp.int32), axis=1)
    targets = owners * capacity + ranking
    places = jnp.arange(owner_count * capacity, dtype=jnp.int32)
    matches = targets[None, :] == places[:, None]
    source_ids = jnp.sum(jnp.where(matches, page_ids[None, :], 0), axis=1)
    filled = jnp.any(matches, axis=1)
    chosen = jnp.where(
        filled[:, None, None], jnp.take(kv_pages, source_ids, axis=0), jnp.zeros((), kv_pages.dtype)
    )
    labels = jnp.where(filled, jnp.take(slot_ids, source_ids), -1).astype(jnp.bfloat16)
    return (
        chosen.reshape(owner_count, capacity, kv_pages.shape[1], kv_pages.shape[2]),
        labels.reshape(owner_count, capacity),
    )


def place_pages(old_cache, got_pages, got_labels):
    flat_pages = got_pages.reshape(-1, old_cache.shape[1], old_cache.shape[2])
    label_ids = got_labels.reshape(-1).astype(jnp.int32)
    slot_ids = jnp.arange(old_cache.shape[0], dtype=jnp.int32)
    arrival_ids = jnp.arange(label_ids.shape[0], dtype=jnp.int32)
    matches = label_ids[None, :] == slot_ids[:, None]
    source_ids = jnp.sum(jnp.where(matches, arrival_ids[None, :], 0), axis=1)
    arrived = jnp.any(matches, axis=1)
    return jnp.where(arrived[:, None, None], jnp.take(flat_pages, source_ids, axis=0), old_cache)


def combine_parts(former, latter):
    overall = jnp.maximum(former[0], latter[0])
    front_scale = jnp.exp(former[0] - overall)
    back_scale = jnp.exp(latter[0] - overall)
    return (
        overall,
        former[1] * front_scale + latter[1] * back_scale,
        former[2] * front_scale[:, :, None] + latter[2] * back_scale[:, :, None],
    )


def body_general(
    hidden_x,
    proj_weight,
    q_gain,
    kv_gain,
    old_cache,
    page_plan,
    block_table,
    split_lens,
    dec_query,
    new_key,
):
    projected = jnp.dot(
        hidden_x,
        lax.all_gather(proj_weight, "dec", axis=1, tiled=True),
        preferred_element_type=jnp.float32,
    )
    query_part = projected[:, :QL]
    kv_part = projected[:, QL:]
    tokens_here = hidden_x.shape[0]
    positions = (
        lax.axis_index("dec") * tokens_here + jnp.arange(tokens_here, dtype=jnp.int32)
    ).astype(jnp.float32)
    lane_count = lax.axis_size(("stg", "tp"))
    lane_index = lax.axis_index(("stg", "tp"))
    owner_count = lax.axis_size("dec")
    page_count = page_plan.shape[0]
    capacity = max(2, -(-page_count // owner_count))
    query_width = QL // lane_count
    query_cols, kv_cols = (
        lax.psum_scatter(query_part, ("stg", "tp"), scatter_dimension=1, tiled=True),
        lax.psum_scatter(kv_part, ("stg", "tp"), scatter_dimension=1, tiled=True),
    )
    kv_width = kv_cols.shape[1]
    col_start = lane_index * kv_width
    columns = col_start + jnp.arange(kv_width, dtype=jnp.int32)
    latent_part_sq = jnp.sum(jnp.where(columns[None, :] < KVL, kv_cols * kv_cols, 0.0), axis=1)
    query_sq, latent_sq = lax.psum(
        (jnp.sum(query_cols * query_cols, axis=1), latent_part_sq), ("stg", "tp")
    )
    kv_rows = kv_finish(kv_cols, col_start, latent_sq, kv_gain, positions)
    kv_pages = kv_rows.reshape(page_count, PAGE, kv_width)
    send_pages, send_labels = pack_pages(kv_pages, page_plan, owner_count, capacity)
    got_slices, got_labels = (
        lax.all_to_all(send_pages, "dec", split_axis=0, concat_axis=0, tiled=True),
        lax.all_to_all(send_labels, "dec", split_axis=0, concat_axis=0, tiled=True),
    )
    got_pages = lax.all_gather(got_slices, ("stg", "tp"), axis=3, tiled=True)
    query_gain = lax.dynamic_slice_in_dim(q_gain, lane_index * query_width, query_width)
    q_latent = (
        query_cols * lax.rsqrt(query_sq / QL + norm_eps)[:, None] * query_gain[None, :]
    ).astype(jnp.bfloat16)
    cache = place_pages(old_cache, got_pages, got_labels)
    slot_table = block_table[0]
    request_count = slot_table.shape[0]
    key_rows = jnp.take(cache, slot_table.reshape(-1), axis=0).reshape(
        request_count, -1, cache.shape[2]
    )
    scores = (
        jnp.einsum("rhc,rlc->rhl", dec_query, key_rows, preferred_element_type=jnp.float32)
        * softmax_scale
    )
    live_mask = jnp.arange(key_rows.shape[1], dtype=jnp.int32)[None, :] < split_lens[:, 0][:, None]
    scores = jnp.where(live_mask[:, None, :], scores, -1e30)
    row_peak = jnp.max(scores, axis=2)
    weights = jnp.where(live_mask[:, None, :], jnp.exp(scores - row_peak[:, :, None]), 0.0)
    row_total = jnp.sum(weights, axis=2)
    rounded = weights.astype(jnp.bfloat16)
    partial_out = jnp.einsum(
        "rhl,rlc->rhc", rounded, key_rows[:, :, :KVL], preferred_element_type=jnp.float32
    )
    peak_all, total_all, output_all = combined_all(
        (row_peak, row_total, partial_out), "dec", combine_parts
    )
    self_score = (
        jnp.einsum("rhc,rc->rh", dec_query, new_key, preferred_element_type=jnp.float32)
        * softmax_scale
    )
    overall = jnp.maximum(peak_all, self_score)
    carried = jnp.exp(peak_all - overall)
    self_weight = jnp.exp(self_score - overall)
    denom = total_all * carried + self_weight
    numer = output_all * carried[:, :, None] + self_weight[:, :, None] * new_key[
        :, None, :KVL
    ].astype(jnp.float32)
    attn_latent = (numer / denom[:, :, None]).astype(jnp.bfloat16)
    return (q_latent, attn_latent)


VMEM = pl.BlockSpec(memory_space=pltpu.VMEM)
SMEM = pl.BlockSpec(memory_space=pltpu.SMEM)
VMEM_GRANT = 16 * 2**20
GRP, DEC, STG, TP = "grp", "dec", "stg", "tp"
F32 = jnp.float32
BF16 = jnp.bfloat16


def swap(a, axis):
    return lax.ppermute(a, axis, [(0, 1), (1, 0)])


def dot_t(a, b, **kw):
    return lax.dot_general(a, b, (((1,), (1,)), ((), ())), preferred_element_type=F32, **kw)


def dot_n(a, b, **kw):
    return lax.dot_general(a, b, (((1,), (0,)), ((), ())), preferred_element_type=F32, **kw)


def chosen(outer, own, sent):
    return jnp.where(outer, own, sent)


def halves(ids, x_ref):
    half = x_ref.shape[1] // 2
    here = pl.ds(pl.multiple_of(ids[0] * half, 128), half)
    there = pl.ds(pl.multiple_of((1 - ids[0]) * half, 128), half)
    return here, there


def is_outer(ids):
    return (ids[2] == 0) | (ids[2] == 3)


def put(ids, out, send, keep, start):
    rows = send.shape[0]
    top, bottom = out[:rows], out[rows:]
    at = slice(start, start + out.shape[1])
    send[:, at] = jnp.where(ids[1] == 0, bottom, top)
    keep[:, at] = jnp.where(ids[1] == 0, top, bottom)


def primary(ids, x_ref, own_ref, parts, send, keep):
    here, there = halves(ids, x_ref)
    outer = is_outer(ids)
    start = 0
    for z, y in parts:
        at = slice(start, start + z.shape[0])
        w_here = chosen(outer, own_ref[at, here], z[...])
        w_there = chosen(outer, own_ref[at, there], y[...])
        put(ids, dot_t(x_ref[:, here], w_here) + dot_t(x_ref[:, there], w_there), send, keep, start)
        start += z.shape[0]


def secondary(ids, x_refs, a_part, b_part, at, send, keep, starts):
    here, there = halves(ids, x_refs[0])
    outer = is_outer(ids)
    w_here = chosen(outer, a_part[0][at, :], b_part[0][at, :])
    w_there = chosen(outer, a_part[1][at, :], b_part[1][at, :])
    for x_ref, start in zip(x_refs, starts):
        put(ids, dot_t(x_ref[:, here], w_here) + dot_t(x_ref[:, there], w_there), send, keep, start)


def near_kernel(ids, x_ref, own_ref, z0, y0, z1, y1, send, keep):
    primary(ids, x_ref, own_ref, ((z0, y0), (z1, y1)), send, keep)


def far_kernel(keys, ids, x_ref, far_ref, own_ref, z0, y0, z1, y1, bz1, by1, send, keep):
    cols = own_ref.shape[0]
    primary(ids, far_ref, own_ref, ((z0, y0), (z1, y1)), send, keep)
    at = slice(z1.shape[0] - keys, None)
    starts = (cols, cols + keys)
    secondary(ids, (x_ref, far_ref), (z1, y1), (bz1, by1), at, send, keep, starts)


def rest_kernel(keys, ids, x_ref, far_ref, z0, y0, z1, y1, bz0, by0, bz1, by1, send, keep):
    head = z0.shape[0]
    rest = z1.shape[0] - keys
    wide = send.shape[1] // 2
    xs = (x_ref, far_ref)
    secondary(ids, xs, (z0, y0), (bz0, by0), slice(None), send, keep, (0, wide))
    at = slice(0, rest)
    secondary(ids, xs, (z1, y1), (bz1, by1), at, send, keep, (head, wide + head))


def project(kernel, width, args):
    rows, feats = args[1].shape
    shape = jax.ShapeDtypeStruct((rows // 2, width), F32)
    return pl.pallas_call(
        kernel,
        in_specs=[SMEM] + [VMEM] * (len(args) - 1),
        out_specs=[VMEM] * 2,
        out_shape=[shape] * 2,
        cost_estimate=pl.CostEstimate(
            flops=2 * rows * feats * width, bytes_accessed=8 * rows * width, transcendentals=0
        ),
        compiler_params=pltpu.CompilerParams(vmem_limit_bytes=VMEM_GRANT),
    )(*args)


def turn_kernel(out):
    source = lax.broadcasted_iota(jnp.int32, out.shape, 0)
    target = lax.broadcasted_iota(jnp.int32, out.shape, 1)
    down = (source == target + 1) & (target % 2 == 0)
    up = (source + 1 == target) & (target % 2 == 1)
    out[...] = jnp.where(down, -1.0, jnp.where(up, 1.0, 0.0))


def old_kernel(n, pages, ids, tab_ref, query_ref, rows_ref, own_ref, packed_ref, bias_ref):
    index, core = ids[2], ids[1]
    query = query_ref[...]
    keys = rows_ref.shape[0]
    requests = own_ref.shape[0] // 4
    heads = query.shape[0] // requests
    base = 2 * pages
    slots = keys // PAGE
    per = slots // requests

    def iota(rows, cols, axis):
        return lax.broadcasted_iota(jnp.int32, (rows, cols), axis)

    size = tab_ref.shape[1]
    diagonal = iota(size, size, 0) == iota(size, size, 1)
    columns = [
        jnp.sum(jnp.where(diagonal, tab_ref[s : s + 1, :], 0), axis=1, keepdims=True)
        for s in range(n)
    ]
    entry = iota(slots, 1, 0)
    readers = entry // per

    def limits(column):
        lengths = jnp.zeros((slots, 1), jnp.int32)
        for r in range(requests):
            at = base + slots + r
            lengths = jnp.where(readers == r, column[at : at + 1, :], lengths)
        return lengths - PAGE * (entry % per)

    def lookup(hit, values):
        return jnp.sum(jnp.where(hit, values, 0), axis=0, keepdims=True)

    page = iota(1, keys, 1) // PAGE
    hit = columns[0][base : base + slots, :] == page
    limit = lookup(hit, limits(columns[0]))
    reader = lookup(hit, readers)
    is_slot = iota(base, 1, 0) % 2 == 1
    taken = jnp.zeros((1, keys), jnp.int32)
    odd_row = iota(base, base, 0)
    follows = (iota(base, base, 1) == odd_row - 1) & (odd_row % 2 == 1)
    for s in range(n):
        plan = columns[s][:base, :]
        owners = jnp.sum(jnp.where(follows, tab_ref[s : s + 1, :base], 0), axis=1, keepdims=True)
        here = is_slot & (owners == index)
        taken = taken + jnp.sum(jnp.where(here & (plan == page), 1, 0), axis=0, keepdims=True)
    limit = jnp.where(taken > 0, 0, limit)
    live = (iota(1, keys, 1) % PAGE) < limit
    bias = jnp.where(live & (reader == iota(8, keys, 0)), 0.0, MASKED)
    wide = jnp.concatenate(
        [jnp.broadcast_to(bias[r : r + 1], (heads, keys)) for r in range(requests)], axis=0
    )
    scores = dot_t(query, rows_ref[...]) * softmax_scale + wide
    own = dot_t(query, own_ref[...]) * softmax_scale
    mine = iota(*own.shape, 0) // heads == iota(*own.shape, 1)
    own = jnp.sum(jnp.where(mine, own, 0.0), axis=1, keepdims=True)
    own = jnp.where(index == 0, own, MASKED)
    peak = jnp.maximum(jnp.max(scores, axis=1, keepdims=True), own)
    weights = jnp.where(wide < 0.0, 0.0, jnp.exp(scores - peak))
    own_weight = jnp.where(index == 0, jnp.exp(own - peak), 0.0)
    total = jnp.sum(weights, axis=1, keepdims=True) + own_weight
    out = dot_n(weights.astype(BF16), rows_ref[:, :KVL])
    own_rows = own_ref[:, :KVL].astype(F32)
    latent = jnp.concatenate(
        [jnp.broadcast_to(own_rows[r : r + 1], (heads, KVL)) for r in range(requests)], axis=0
    )
    pack((out + own_weight * latent) / total, peak + jnp.log(total), packed_ref)

    width = bias_ref.shape[1]
    half = pages // 2
    spot = iota(1, width, 1) // PAGE
    which = jnp.where(spot // pages == 1, 1 - core, core) * half + spot % half
    partner = (spot % pages) // half == 1
    line = iota(base, width, 0)
    plan = jnp.where(partner, columns[n - 1][:base, :], columns[0][:base, :])
    plan = jnp.where(line % 2 == 1, plan, plan * (2 * slots))
    code = jnp.sum(jnp.where(line // 2 == which, plan, 0), axis=0, keepdims=True)
    limit = jnp.zeros((1, width), jnp.int32)
    reader = jnp.zeros((1, width), jnp.int32)
    for s in range(n):
        owner = (index + s) % n
        hit = columns[s][base : base + slots, :] + owner * (2 * slots) == code
        limit = limit + lookup(hit, limits(columns[s]))
        reader = reader + lookup(hit, readers)
    limit = jnp.where(index % 2 == 1, limit, 0)
    live = (iota(1, width, 1) % PAGE) < limit
    bias_ref[...] = jnp.where(live & (reader == iota(8, width, 0)), 0.0, MASKED)


def parted(ids, block):
    half = block.shape[0] // 2
    odd, stage = ids[2] % 2 == 1, ids[3]
    top, bottom = block[:half], block[half:]
    mine = jnp.where(stage == 0, top, bottom)
    away = jnp.where(stage == 0, bottom, top)
    twice = lambda part: jnp.concatenate([part, part], axis=0)
    return jnp.where(odd, block, twice(mine)), jnp.where(odd, block, twice(away))


def cross_near_kernel(ids, kept, got, send, keep):
    mine, away = parted(ids, kept[...] + got[...])
    keep[...] = mine
    send[...] = away.astype(BF16)


def cross_far_kernel(cols, ids, kept, got, send, keep):
    both = kept[...] + got[...]
    mine, away = parted(ids, both[:, :cols])
    keep[:, :cols] = mine
    keep[:, cols:] = both[:, cols:]
    send[:, :cols] = away.astype(BF16)
    send[:, cols:] = both[:, cols:].astype(BF16)


def cross_rest_kernel(cut, keys, ids, kept, got, kept_far, got_far, send, keep):
    wide = kept.shape[1] // 2
    cols = send.shape[1]
    stage = ids[3]
    for i in range(2):
        at = slice(i * wide, i * wide + cut)
        last = slice(cols + i * keys, cols + (i + 1) * keys)
        block = jnp.concatenate(
            [kept[:, at] + got[:, at], kept_far[:, last] + got_far[:, last]], axis=1
        )
        half = block.shape[0] // 2
        top, bottom = block[:half], block[half:]
        at = slice(i * half, (i + 1) * half)
        keep[at, :] = jnp.where(stage == 0, top, bottom)
        send[at, :] = jnp.where(stage == 0, bottom, top).astype(BF16)


def keys_kernel(keys, keep0, got0, keep1, got1, cos, sin, turn, gain, out):
    rows, cols = keep0.shape
    for i in range(2):
        last = slice(cols + i * keys, cols + (i + 1) * keys)
        tail = keep1[:, last] + got1[:, last].astype(F32)
        if i == 0:
            block = keep0[...] + got0[...].astype(F32)
        else:
            block = keep1[:, :cols] + got1[:, :cols].astype(F32)
        raw = jnp.concatenate([tail, block], axis=1)
        at = slice(i * rows, (i + 1) * rows)
        latent = raw[:, :KVL]
        inverse = lax.rsqrt(jnp.sum(latent * latent, axis=1, keepdims=True) / KVL + norm_eps)
        out[at, :KVL] = (latent * inverse * gain[...]).astype(BF16)
        rope = raw[:, KVL:]
        partner = dot_n(rope, turn[...], precision=lax.Precision.HIGHEST)
        out[at, KVL:] = (rope * cos[at, :] + partner * sin[at, :]).astype(BF16)


def pack(out, level, packed_ref):
    packed_ref[:, :KVL] = out.astype(BF16)
    lead = level.astype(BF16).astype(F32)
    rest = (level - lead).astype(BF16).astype(F32)
    last = level - lead - rest
    lane = lax.broadcasted_iota(jnp.int32, (out.shape[0], 128), 1)
    tail = jnp.where(lane == 0, lead, jnp.where(lane == 1, rest, jnp.where(lane == 2, last, 0.0)))
    packed_ref[:, KVL:] = tail.astype(BF16)


def unpack(packed):
    level = jnp.sum(packed[:, KVL:].astype(F32), axis=1, keepdims=True)
    return packed[:, :KVL].astype(F32), level


def attend_kernel(query_ref, k0_ref, k1_ref, bias_ref, old_ref, far_ref, packed_ref):
    query = query_ref[...]
    keys = k0_ref.shape[0]
    requests = bias_ref.shape[0] // 2
    heads = query.shape[0] // requests
    bias = bias_ref[...]
    wide = jnp.concatenate(
        [jnp.broadcast_to(bias[r : r + 1], (heads, 2 * keys)) for r in range(requests)], axis=0
    )
    scores = jnp.concatenate([dot_t(query, k0_ref[...]), dot_t(query, k1_ref[...])], axis=1)
    scores = scores * softmax_scale + wide
    old, old_level = unpack(old_ref[...])
    far, far_level = unpack(far_ref[...])
    peak = jnp.maximum(old_level, far_level)
    peak = jnp.maximum(peak, jnp.max(scores, axis=1, keepdims=True))
    weights = jnp.where(wide < 0.0, 0.0, jnp.exp(scores - peak))
    old_share, far_share = jnp.exp(old_level - peak), jnp.exp(far_level - peak)
    total = jnp.sum(weights, axis=1, keepdims=True) + old_share + far_share
    rounded = weights.astype(BF16)
    out = dot_n(rounded[:, :keys], k0_ref[:, :KVL]) + dot_n(rounded[:, keys:], k1_ref[:, :KVL])
    out = out + old * old_share + far * far_share
    pack(out / total, peak + jnp.log(total), packed_ref)


def combine_kernel(ids, own, across, partner, other, out):
    odd = ids[2] % 2 == 1
    first, level = unpack(jnp.where(odd, own[...], partner[...]))
    second, other_level = unpack(jnp.where(odd, across[...], other[...]))
    top = jnp.maximum(level, other_level)
    share, other_share = jnp.exp(level - top), jnp.exp(other_level - top)
    out[...] = ((first * share + second * other_share) / (share + other_share)).astype(BF16)


def return_kernel(keep0, got0, keep1, got1, keep2, got2, low, high, send):
    rows, cols = low.shape
    for i in range(2):
        near = slice(i * rows, (i + 1) * rows)
        keep, got = (keep0, got0) if i == 0 else (keep1, got1)
        first = keep[:rows, :cols] + got[:rows, :cols].astype(F32)
        second = keep2[near, :] + got2[near, :].astype(F32)
        if i == 0:
            low[...] = first
            high[...] = second
        else:
            send[:, :cols] = first.astype(BF16)
            send[:, cols:] = second.astype(BF16)


def query_kernel(ids, low, high, got, gain, *refs):
    sends, scratch = refs[:-1], refs[-1]
    odd = ids[2] % 2 == 1
    cols = low.shape[1]
    cut = QL - 2 * cols
    got_low, got_high = got[:, :cols].astype(F32), got[:, cols:].astype(F32)
    first = jnp.where(odd, got_low, low[...])
    second = jnp.where(odd, got_high, high[...])
    third = jnp.where(odd, high[:, :cut], got_high[:, :cut])
    rows = jnp.concatenate([first, second, third], axis=1)
    inverse = lax.rsqrt(jnp.sum(rows * rows, axis=1, keepdims=True) / QL + norm_eps)
    rows = (rows * inverse * gain[...]).astype(BF16)
    scratch[...] = rows
    width = QL // len(sends)
    lane = 2 * ids[3] + ids[1]
    for k, send in enumerate(sends):
        target = jnp.bitwise_xor(lane, k)
        send[...] = scratch[:, pl.ds(pl.multiple_of(target * width, 128), width)]


def place_kernel(ids, *refs):
    gots, out = refs[:-1], refs[-1]
    rows = gots[0].shape[0]
    lane = 2 * ids[3] + ids[1]
    for k, got in enumerate(gots):
        source = jnp.bitwise_xor(lane, k)
        order = 2 * (source % 2) + source // 2
        out[pl.ds(pl.multiple_of(order * rows, 32), rows), :] = got[...]


def call(kernel, shapes, specs, args, scratch=()):
    return pl.pallas_call(
        kernel,
        scratch_shapes=scratch,
        out_shape=shapes,
        in_specs=specs,
        out_specs=[VMEM] * len(shapes) if isinstance(shapes, list) else VMEM,
        cost_estimate=pl.CostEstimate(flops=20_000_000, bytes_accessed=2_000_000, transcendentals=0),
        compiler_params=pltpu.CompilerParams(vmem_limit_bytes=VMEM_GRANT),
    )(*args)


def shaped(*dims, kind=F32):
    return jax.ShapeDtypeStruct(dims, kind)


def body_pairs(*args):
    return pairs_step(*args)


def pairs_step(
    hidden_x,
    proj_weight,
    q_gain,
    kv_gain,
    old_cache,
    page_plan,
    block_table,
    split_lens,
    dec_query,
    new_key,
):
    n = lax.axis_size(DEC)
    group, index = lax.axis_index(GRP), lax.axis_index(DEC)
    stage, core = lax.axis_index(STG), lax.axis_index(TP)
    ids = jnp.stack([group, core, index, stage]).astype(jnp.int32)
    tokens, feats = hidden_x.shape
    cols = proj_weight.shape[1]
    cut = QL - 2 * cols
    half = feats // 2
    pages = page_plan.shape[0]
    requests, heads, _ = dec_query.shape
    queries = requests * heads
    rows = tokens // 2
    quarter = rows // 2

    weight = proj_weight.T
    split = cols // 2 // 128 * 128
    pieces = [
        lax.dynamic_slice(weight, (0, group * half), (split, half)),
        lax.dynamic_slice(weight, (split, group * half), (cols - split, half)),
    ]
    partners = [(0, 1), (1, 0), (2, 3), (3, 2)]
    inner = [(g * n + i, (1 - g) * n + i) for g in range(2) for i in (1, 2)]
    a_z, a_y, b_z, b_y = [None] * 2, [None] * 2, [None] * 2, [None] * 2
    for p in (1, 0):
        a_z[p] = lax.ppermute(pieces[p], DEC, [(0, 2), (3, 1), (1, 0), (2, 3)])
    packed = jnp.concatenate(
        [page_plan.reshape(-1), block_table.reshape(-1), split_lens.reshape(-1)]
    ).reshape(1, -1)
    tables = [packed]
    for s in range(1, n):
        tables.append(lax.ppermute(packed, DEC, [((i + s) % n, i) for i in range(n)]))
    tables = jnp.pad(
        jnp.concatenate(tables, axis=0), ((0, 8 - n), (0, -packed.shape[1] % 128))
    )
    x_far = lax.ppermute(hidden_x, DEC, partners)
    held = lax.optimization_barrier((pieces[0], pieces[1], a_z[0]))
    for p in (1, 0):
        a_y[p] = swap(a_z[p], GRP)
        b_z[p] = lax.ppermute(held[p], DEC, [(1, 2), (2, 1)])
    for p in (1, 0):
        b_y[p] = lax.ppermute(b_z[p], (GRP, DEC), inner)
    query = dec_query.reshape(queries, KVW)
    padded_key = jnp.pad(new_key, ((0, 3 * requests), (0, 0)))
    old, bias = call(
        functools.partial(old_kernel, n, pages),
        [shaped(queries, KVL + 128, kind=BF16), shaped(8, 2 * tokens)],
        [SMEM, VMEM, VMEM, VMEM, VMEM],
        (ids, tables, query, old_cache.reshape(-1, KVW), padded_key),
    )

    old_far = lax.ppermute(old, DEC, partners)

    partner = index + 1 - 2 * (index % 2)
    place = core * rows + jnp.arange(rows, dtype=jnp.int32)
    positions = jnp.concatenate([index * tokens + place, partner * tokens + place]).astype(F32)
    pair = jnp.arange(ROPE, dtype=jnp.int32) // 2
    frequency = jnp.power(F32(10000.0), -(2 * pair).astype(F32) / ROPE)
    angles = positions[:, None] * frequency[None, :]
    turn = call(turn_kernel, shaped(ROPE, ROPE), [], ())
    early_ids, cos, sin, turn, kv_scale, q_scale = lax.optimization_barrier(
        (ids, jnp.cos(angles), jnp.sin(angles), turn, kv_gain.reshape(1, -1), q_gain.reshape(1, -1))
    )

    a_refs = (a_z[0], a_y[0], a_z[1], a_y[1])
    keys = cols - cut
    wide = -(-cut // 128) * 128
    send, kept0 = project(near_kernel, cols, (early_ids, hidden_x, weight, *a_refs))
    other0 = swap(send, TP)
    send0, keep0 = call(
        cross_near_kernel,
        [shaped(rows, cols, kind=BF16), shaped(rows, cols)],
        [SMEM, VMEM, VMEM],
        (ids, kept0, other0),
    )
    got0 = swap(send0, STG)
    send, kept1 = project(
        functools.partial(far_kernel, keys),
        cols + 2 * keys,
        (ids, hidden_x, x_far, weight, *a_refs, b_z[1], b_y[1]),
    )
    other1 = swap(send, TP)
    send1, keep1 = call(
        functools.partial(cross_far_kernel, cols),
        [shaped(rows, cols + 2 * keys, kind=BF16), shaped(rows, cols + 2 * keys)],
        [SMEM, VMEM, VMEM],
        (ids, kept1, other1),
    )
    got1 = swap(send1, STG)
    send, kept2 = project(
        functools.partial(rest_kernel, keys),
        2 * wide,
        (ids, hidden_x, x_far, *a_refs, b_z[0], b_y[0], b_z[1], b_y[1]),
    )
    other2 = swap(send, TP)
    send2, keep2 = call(
        functools.partial(cross_rest_kernel, cut, keys),
        [shaped(rows, cols, kind=BF16), shaped(rows, cols)],
        [SMEM] + [VMEM] * 4,
        (ids, kept2, other2, kept1, other1),
    )
    got2 = swap(send2, STG)

    key_rows = call(
        functools.partial(keys_kernel, keys),
        shaped(tokens, KVW, kind=BF16),
        [VMEM] * 8,
        (keep0, got0, keep1, got1, cos, sin, turn, kv_scale),
    )
    far_keys = swap(key_rows, TP)
    part_out = call(
        attend_kernel,
        shaped(queries, KVL + 128, kind=BF16),
        [VMEM] * 6,
        (query, key_rows, far_keys, bias, old, old_far),
    )
    spread = []
    for pairs in ([(1, 3), (3, 1)], [(1, 0), (3, 2)], [(1, 2), (3, 0)]):
        spread.append(lax.ppermute(part_out, DEC, pairs))
    attn = call(
        combine_kernel,
        shaped(queries, KVL, kind=BF16),
        [SMEM] + [VMEM] * 4,
        (ids, part_out, *spread),
    )

    low, high, back = call(
        return_kernel,
        [shaped(quarter, cols), shaped(quarter, cols), shaped(quarter, 2 * cols, kind=BF16)],
        [VMEM] * 6,
        (keep0, got0, keep1, got1, keep2, got2),
    )
    back = lax.ppermute(back, DEC, partners)
    lanes = 4
    width = QL // lanes
    tile = shaped(quarter, width, kind=BF16)
    blocks = call(
        query_kernel,
        [tile] * lanes,
        [SMEM] + [VMEM] * 4,
        (ids, low, high, back, q_scale),
        scratch=[pltpu.VMEM((quarter, QL), BF16)],
    )
    gots = [blocks[0]]
    for k in range(1, lanes):
        gots.append(lax.ppermute(blocks[k], (STG, TP), [(i, i ^ k) for i in range(lanes)]))
    q_latent = call(
        place_kernel, shaped(tokens, width, kind=BF16), [SMEM] + [VMEM] * lanes, (ids, *gots)
    )
    return (q_latent, attn.reshape(requests, heads, KVL))


def solution(mesh):
    sizes = dict(mesh.shape)
    pairs = sizes["dec"] == 4 and sizes["grp"] == sizes["stg"] == sizes["tp"] == 2
    return jax.shard_map(
        body_pairs if pairs else body_general,
        mesh=mesh,
        in_specs=(
            P(("grp", "dec"), ("stg", "tp")),
            P(("stg", "tp"), "dec"),
            P(),
            P(),
            P(("grp", "dec"), None, None),
            P(("grp", "dec"), None),
            P(("grp", "dec"), None, None),
            P("grp", "dec"),
            P("grp", ("stg", "tp"), None),
            P("grp", None),
        ),
        out_specs=(P(("grp", "dec"), ("stg", "tp")), P("grp", ("stg", "tp"), None)),
        check_vma=False,
    )
```

```python
import functools

import jax
import jax.numpy as jnp
from jax import lax
from jax.experimental import pallas as pl
from jax.experimental.pallas import tpu as pltpu
from jax.sharding import PartitionSpec as P


QL = 1536
KVL = 512
ROPE = 64
PAGE = 32
KVW = KVL + ROPE
MASKED = -1e30

softmax_scale = 192.0 ** (-0.5)
norm_eps = 1e-06


def combined_all(part, axis, combine):
    gathered = jax.tree.map(lambda a: lax.all_gather(a, axis), part)

    def take(source):
        return jax.tree.map(lambda a: lax.dynamic_index_in_dim(a, source, 0, False), gathered)

    return lax.fori_loop(
        1, lax.axis_size(axis), lambda source, state: combine(state, take(source)), take(0)
    )


def rope_rotate(matrix, col_start, positions):
    col_count = matrix.shape[1]
    columns = col_start + jnp.arange(col_count, dtype=jnp.int32)
    is_rope = columns >= KVL
    pair_index = jnp.maximum(columns - KVL, 0) // 2
    frequency = jnp.power(jnp.float32(10000.0), -(2 * pair_index).astype(jnp.float32) / ROPE)
    angles = positions[:, None] * frequency[None, :]
    cosine = jnp.where(is_rope[None, :], jnp.cos(angles), 1.0)
    sine_part = jnp.where(is_rope[None, :], jnp.sin(angles), 0.0)
    paired = matrix.reshape(matrix.shape[0], col_count // 2, 2)
    partner = jnp.stack([-paired[:, :, 1], paired[:, :, 0]], axis=2).reshape(matrix.shape)
    return matrix * cosine + partner * sine_part


def kv_finish(matrix, col_start, latent_sq, kv_gain, positions):
    col_count = matrix.shape[1]
    columns = col_start + jnp.arange(col_count, dtype=jnp.int32)
    gain_full = jnp.concatenate([kv_gain, jnp.ones((ROPE,), jnp.float32)])
    gain_cols = lax.dynamic_slice_in_dim(gain_full, col_start, col_count)
    inverse = lax.rsqrt(latent_sq / KVL + norm_eps)
    row_scale = jnp.where(columns[None, :] < KVL, inverse[:, None] * gain_cols[None, :], 1.0)
    return rope_rotate(matrix * row_scale, col_start, positions).astype(jnp.bfloat16)


def pack_pages(kv_pages, page_table, owner_count, capacity):
    owners = page_table[:, 0]
    slot_ids = page_table[:, 1]
    page_ids = jnp.arange(kv_pages.shape[0], dtype=jnp.int32)
    earlier = (owners[:, None] == owners[None, :]) & (page_ids[None, :] < page_ids[:, None])
    ranking = jnp.sum(earlier.astype(jnp.int32), axis=1)
    targets = owners * capacity + ranking
    places = jnp.arange(owner_count * capacity, dtype=jnp.int32)
    matches = targets[None, :] == places[:, None]
    source_ids = jnp.sum(jnp.where(matches, page_ids[None, :], 0), axis=1)
    filled = jnp.any(matches, axis=1)
    chosen = jnp.where(
        filled[:, None, None], jnp.take(kv_pages, source_ids, axis=0), jnp.zeros((), kv_pages.dtype)
    )
    labels = jnp.where(filled, jnp.take(slot_ids, source_ids), -1).astype(jnp.bfloat16)
    return (
        chosen.reshape(owner_count, capacity, kv_pages.shape[1], kv_pages.shape[2]),
        labels.reshape(owner_count, capacity),
    )


def place_pages(old_cache, got_pages, got_labels):
    flat_pages = got_pages.reshape(-1, old_cache.shape[1], old_cache.shape[2])
    label_ids = got_labels.reshape(-1).astype(jnp.int32)
    slot_ids = jnp.arange(old_cache.shape[0], dtype=jnp.int32)
    arrival_ids = jnp.arange(label_ids.shape[0], dtype=jnp.int32)
    matches = label_ids[None, :] == slot_ids[:, None]
    source_ids = jnp.sum(jnp.where(matches, arrival_ids[None, :], 0), axis=1)
    arrived = jnp.any(matches, axis=1)
    return jnp.where(arrived[:, None, None], jnp.take(flat_pages, source_ids, axis=0), old_cache)


def combine_parts(former, latter):
    overall = jnp.maximum(former[0], latter[0])
    front_scale = jnp.exp(former[0] - overall)
    back_scale = jnp.exp(latter[0] - overall)
    return (
        overall,
        former[1] * front_scale + latter[1] * back_scale,
        former[2] * front_scale[:, :, None] + latter[2] * back_scale[:, :, None],
    )


def body_general(
    hidden_x,
    proj_weight,
    q_gain,
    kv_gain,
    old_cache,
    page_plan,
    block_table,
    split_lens,
    dec_query,
    new_key,
):
    projected = jnp.dot(
        hidden_x,
        lax.all_gather(proj_weight, "dec", axis=1, tiled=True),
        preferred_element_type=jnp.float32,
    )
    query_part = projected[:, :QL]
    kv_part = projected[:, QL:]
    tokens_here = hidden_x.shape[0]
    positions = (
        lax.axis_index("dec") * tokens_here + jnp.arange(tokens_here, dtype=jnp.int32)
    ).astype(jnp.float32)
    lane_count = lax.axis_size(("stg", "tp"))
    lane_index = lax.axis_index(("stg", "tp"))
    owner_count = lax.axis_size("dec")
    page_count = page_plan.shape[0]
    capacity = max(2, -(-page_count // owner_count))
    query_width = QL // lane_count
    query_cols, kv_cols = (
        lax.psum_scatter(query_part, ("stg", "tp"), scatter_dimension=1, tiled=True),
        lax.psum_scatter(kv_part, ("stg", "tp"), scatter_dimension=1, tiled=True),
    )
    kv_width = kv_cols.shape[1]
    col_start = lane_index * kv_width
    columns = col_start + jnp.arange(kv_width, dtype=jnp.int32)
    latent_part_sq = jnp.sum(jnp.where(columns[None, :] < KVL, kv_cols * kv_cols, 0.0), axis=1)
    query_sq, latent_sq = lax.psum(
        (jnp.sum(query_cols * query_cols, axis=1), latent_part_sq), ("stg", "tp")
    )
    kv_rows = kv_finish(kv_cols, col_start, latent_sq, kv_gain, positions)
    kv_pages = kv_rows.reshape(page_count, PAGE, kv_width)
    send_pages, send_labels = pack_pages(kv_pages, page_plan, owner_count, capacity)
    got_slices, got_labels = (
        lax.all_to_all(send_pages, "dec", split_axis=0, concat_axis=0, tiled=True),
        lax.all_to_all(send_labels, "dec", split_axis=0, concat_axis=0, tiled=True),
    )
    got_pages = lax.all_gather(got_slices, ("stg", "tp"), axis=3, tiled=True)
    query_gain = lax.dynamic_slice_in_dim(q_gain, lane_index * query_width, query_width)
    q_latent = (
        query_cols * lax.rsqrt(query_sq / QL + norm_eps)[:, None] * query_gain[None, :]
    ).astype(jnp.bfloat16)
    cache = place_pages(old_cache, got_pages, got_labels)
    slot_table = block_table[0]
    request_count = slot_table.shape[0]
    key_rows = jnp.take(cache, slot_table.reshape(-1), axis=0).reshape(
        request_count, -1, cache.shape[2]
    )
    scores = (
        jnp.einsum("rhc,rlc->rhl", dec_query, key_rows, preferred_element_type=jnp.float32)
        * softmax_scale
    )
    live_mask = jnp.arange(key_rows.shape[1], dtype=jnp.int32)[None, :] < split_lens[:, 0][:, None]
    scores = jnp.where(live_mask[:, None, :], scores, -1e30)
    row_peak = jnp.max(scores, axis=2)
    weights = jnp.where(live_mask[:, None, :], jnp.exp(scores - row_peak[:, :, None]), 0.0)
    row_total = jnp.sum(weights, axis=2)
    rounded = weights.astype(jnp.bfloat16)
    partial_out = jnp.einsum(
        "rhl,rlc->rhc", rounded, key_rows[:, :, :KVL], preferred_element_type=jnp.float32
    )
    peak_all, total_all, output_all = combined_all(
        (row_peak, row_total, partial_out), "dec", combine_parts
    )
    self_score = (
        jnp.einsum("rhc,rc->rh", dec_query, new_key, preferred_element_type=jnp.float32)
        * softmax_scale
    )
    overall = jnp.maximum(peak_all, self_score)
    carried = jnp.exp(peak_all - overall)
    self_weight = jnp.exp(self_score - overall)
    denom = total_all * carried + self_weight
    numer = output_all * carried[:, :, None] + self_weight[:, :, None] * new_key[
        :, None, :KVL
    ].astype(jnp.float32)
    attn_latent = (numer / denom[:, :, None]).astype(jnp.bfloat16)
    return (q_latent, attn_latent)


VMEM = pl.BlockSpec(memory_space=pltpu.VMEM)
SMEM = pl.BlockSpec(memory_space=pltpu.SMEM)
VMEM_GRANT = 16 * 2**20
GRP, DEC, STG, TP = "grp", "dec", "stg", "tp"
F32 = jnp.float32
BF16 = jnp.bfloat16


def swap(a, axis):
    return lax.ppermute(a, axis, [(0, 1), (1, 0)])


def dot_t(a, b, **kw):
    return lax.dot_general(a, b, (((1,), (1,)), ((), ())), preferred_element_type=F32, **kw)


def dot_n(a, b, **kw):
    return lax.dot_general(a, b, (((1,), (0,)), ((), ())), preferred_element_type=F32, **kw)


def chosen(outer, own, sent):
    return jnp.where(outer, own, sent)


def halves(ids, x_ref):
    half = x_ref.shape[1] // 2
    here = pl.ds(pl.multiple_of(ids[0] * half, 128), half)
    there = pl.ds(pl.multiple_of((1 - ids[0]) * half, 128), half)
    return here, there


def is_outer(ids):
    return (ids[2] == 0) | (ids[2] == 3)


def put(ids, out, send, keep, chunk, column, row=0):
    part = chunk // 2
    columns = slice(column, column + out.shape[1])
    for c in range(out.shape[0] // chunk):
        top, bottom = out[c * chunk : c * chunk + part], out[c * chunk + part : (c + 1) * chunk]
        at = slice(row + c * part, row + (c + 1) * part)
        send[at, columns] = jnp.where(ids[1] == 0, bottom, top)
        keep[at, columns] = jnp.where(ids[1] == 0, top, bottom)


def primary(ids, x_ref, own_ref, parts, send, keep, chunk):
    here, there = halves(ids, x_ref)
    outer = is_outer(ids)
    start = 0
    for z, y in parts:
        at = slice(start, start + z.shape[0])
        w_here = chosen(outer, own_ref[at, here], z[...])
        w_there = chosen(outer, own_ref[at, there], y[...])
        out = dot_t(x_ref[:, here], w_here) + dot_t(x_ref[:, there], w_there)
        put(ids, out, send, keep, chunk, start)
        start += z.shape[0]


def secondary(ids, x_refs, w_here, w_there, outs, chunk, places):
    here, there = halves(ids, x_refs[0])
    for x_ref, (column, step, row) in zip(x_refs, places):
        out = dot_t(x_ref[:, here], w_here) + dot_t(x_ref[:, there], w_there)
        for c in range(out.shape[0] // chunk):
            piece = out[c * chunk : (c + 1) * chunk]
            put(ids, piece, *outs, chunk, column + c * step, row + (0 if step else c * chunk // 2))


def near_kernel(chunk, ids, x_ref, own_ref, z0, y0, z1, y1, send, keep):
    primary(ids, x_ref, own_ref, ((z0, y0), (z1, y1)), send, keep, chunk)


def far_kernel(chunk, ids, far_ref, own_ref, z0, y0, z1, y1, send, keep):
    primary(ids, far_ref, own_ref, ((z0, y0), (z1, y1)), send, keep, chunk)


def last_kernel(chunk, keys, ids, x_ref, far0, far1, own_ref, z0, y0, z1, y1, bz1, by1, send, keep):
    cols = own_ref.shape[0]
    primary(ids, far1, own_ref, ((z0, y0), (z1, y1)), send, keep, chunk)
    outer = is_outer(ids)
    at = slice(z1.shape[0] - keys, None)
    w_here = chosen(outer, z1[at, :], bz1[at, :])
    w_there = chosen(outer, y1[at, :], by1[at, :])
    places = [(cols, keys, 0), (cols + 2 * keys, keys, 0), (cols + 3 * keys, keys, 0)]
    secondary(ids, (x_ref, far0, far1), w_here, w_there, (send, keep), chunk, places)


def rest_kernel(
    chunk, keys, ids, x_ref, far0, far1, z0, y0, z1, y1, whole, bz0, by0, bz1, by1, send, keep
):
    outer = is_outer(ids)
    head, direct = z0.shape[0], whole.shape[0]
    wide = send.shape[1] // 2
    here, there = halves(ids, x_ref)
    xs = (x_ref, far0, far1)
    rest = slice(0, z1.shape[0] - keys)
    late = slice(direct, None)
    for column, w_here, w_there in (
        (
            0,
            jnp.concatenate(
                [
                    chosen(outer, z0[:direct, :], whole[:, here]),
                    chosen(outer, z0[late, :], bz0[...]),
                ],
                axis=0,
            ),
            jnp.concatenate(
                [
                    chosen(outer, y0[:direct, :], whole[:, there]),
                    chosen(outer, y0[late, :], by0[...]),
                ],
                axis=0,
            ),
        ),
        (
            head,
            chosen(outer, z1[rest, :], bz1[rest, :]),
            chosen(outer, y1[rest, :], by1[rest, :]),
        ),
    ):
        places = [(column, 0, 0), (wide + column, 0, 0), (wide + column, 0, chunk // 2)]
        secondary(ids, xs, w_here, w_there, (send, keep), chunk, places)


def project(kernel, rows, width, args):
    feats = args[1].shape[1]
    shape = jax.ShapeDtypeStruct((rows, width), F32)
    return pl.pallas_call(
        kernel,
        in_specs=[SMEM] + [VMEM] * (len(args) - 1),
        out_specs=[VMEM] * 2,
        out_shape=[shape] * 2,
        cost_estimate=pl.CostEstimate(
            flops=4 * rows * feats * width, bytes_accessed=8 * rows * width, transcendentals=0
        ),
        compiler_params=pltpu.CompilerParams(vmem_limit_bytes=VMEM_GRANT),
    )(*args)


def turn_kernel(out):
    source = lax.broadcasted_iota(jnp.int32, out.shape, 0)
    target = lax.broadcasted_iota(jnp.int32, out.shape, 1)
    down = (source == target + 1) & (target % 2 == 0)
    up = (source + 1 == target) & (target % 2 == 1)
    out[...] = jnp.where(down, -1.0, jnp.where(up, 1.0, 0.0))


def old_kernel(n, pages, ids, tab_ref, query_ref, rows_ref, own_ref, packed_ref, bias_ref):
    index, core = ids[2], ids[1]
    query = query_ref[...]
    keys = rows_ref.shape[0]
    requests = own_ref.shape[0] // 4
    heads = query.shape[0] // requests
    base = 2 * pages
    slots = keys // PAGE
    per = slots // requests

    def iota(rows, cols, axis):
        return lax.broadcasted_iota(jnp.int32, (rows, cols), axis)

    size = tab_ref.shape[1]
    diagonal = iota(size, size, 0) == iota(size, size, 1)
    columns = [
        jnp.sum(jnp.where(diagonal, tab_ref[s : s + 1, :], 0), axis=1, keepdims=True)
        for s in range(n)
    ]
    entry = iota(slots, 1, 0)
    readers = entry // per

    def limits(column):
        lengths = jnp.zeros((slots, 1), jnp.int32)
        for r in range(requests):
            at = base + slots + r
            lengths = jnp.where(readers == r, column[at : at + 1, :], lengths)
        return lengths - PAGE * (entry % per)

    def lookup(hit, values):
        return jnp.sum(jnp.where(hit, values, 0), axis=0, keepdims=True)

    page = iota(1, keys, 1) // PAGE
    hit = columns[0][base : base + slots, :] == page
    limit = lookup(hit, limits(columns[0]))
    reader = lookup(hit, readers)
    is_slot = iota(base, 1, 0) % 2 == 1
    taken = jnp.zeros((1, keys), jnp.int32)
    odd_row = iota(base, base, 0)
    follows = (iota(base, base, 1) == odd_row - 1) & (odd_row % 2 == 1)
    for s in range(n):
        plan = columns[s][:base, :]
        owners = jnp.sum(jnp.where(follows, tab_ref[s : s + 1, :base], 0), axis=1, keepdims=True)
        here = is_slot & (owners == index)
        taken = taken + jnp.sum(jnp.where(here & (plan == page), 1, 0), axis=0, keepdims=True)
    limit = jnp.where(taken > 0, 0, limit)
    live = (iota(1, keys, 1) % PAGE) < limit
    bias = jnp.where(live & (reader == iota(8, keys, 0)), 0.0, MASKED)
    wide = jnp.concatenate(
        [jnp.broadcast_to(bias[r : r + 1], (heads, keys)) for r in range(requests)], axis=0
    )
    scores = dot_t(query, rows_ref[...]) * softmax_scale + wide
    own = dot_t(query, own_ref[...]) * softmax_scale
    mine = iota(*own.shape, 0) // heads == iota(*own.shape, 1)
    own = jnp.sum(jnp.where(mine, own, 0.0), axis=1, keepdims=True)
    own = jnp.where(index == 0, own, MASKED)
    peak = jnp.maximum(jnp.max(scores, axis=1, keepdims=True), own)
    weights = jnp.where(wide < 0.0, 0.0, jnp.exp(scores - peak))
    own_weight = jnp.where(index == 0, jnp.exp(own - peak), 0.0)
    total = jnp.sum(weights, axis=1, keepdims=True) + own_weight
    out = dot_n(weights.astype(BF16), rows_ref[:, :KVL])
    own_rows = own_ref[:, :KVL].astype(F32)
    latent = jnp.concatenate(
        [jnp.broadcast_to(own_rows[r : r + 1], (heads, KVL)) for r in range(requests)], axis=0
    )
    pack((out + own_weight * latent) / total, peak + jnp.log(total), packed_ref)

    width = bias_ref.shape[1]
    half = pages // 2
    spot = iota(1, width, 1) // PAGE
    place = spot % half
    taker = jnp.where(spot // pages == 1, 1 - core, core)
    which = (place // (half // 2)) * half + taker * (half // 2) + place % (half // 2)
    partner = (spot % pages) // half == 1
    line = iota(base, width, 0)
    plan = jnp.where(partner, columns[n - 1][:base, :], columns[0][:base, :])
    plan = jnp.where(line % 2 == 1, plan, plan * (2 * slots))
    code = jnp.sum(jnp.where(line // 2 == which, plan, 0), axis=0, keepdims=True)
    limit = jnp.zeros((1, width), jnp.int32)
    reader = jnp.zeros((1, width), jnp.int32)
    for s in range(n):
        owner = (index + s) % n
        hit = columns[s][base : base + slots, :] + owner * (2 * slots) == code
        limit = limit + lookup(hit, limits(columns[s]))
        reader = reader + lookup(hit, readers)
    limit = jnp.where(index % 2 == 1, limit, 0)
    live = (iota(1, width, 1) % PAGE) < limit
    bias_ref[...] = jnp.where(live & (reader == iota(8, width, 0)), 0.0, MASKED)


def lane_rows(ids, block):
    half = block.shape[0] // 2
    top, bottom = block[:half], block[half:]
    stage = ids[3]
    return jnp.where(stage == 0, top, bottom), jnp.where(stage == 0, bottom, top)


def cross_kernel(cols, part, ids, kept, got, send, keep):
    odd = ids[2] % 2 == 1
    both = kept[...] + got[...]
    for c in range(both.shape[0] // part):
        at = slice(c * part, (c + 1) * part)
        block = both[at, :cols]
        mine, away = lane_rows(ids, block)
        keep[at, :cols] = jnp.where(odd, block, jnp.concatenate([mine, mine], axis=0))
        send[at, :cols] = jnp.where(odd, block, jnp.concatenate([away, away], axis=0)).astype(BF16)
    if both.shape[1] > cols:
        keep[:, cols:] = both[:, cols:]
        send[:, cols:] = both[:, cols:].astype(BF16)


def cross_rest_kernel(cut, keys, ids, kept, got, kept_last, got_last, send, keep):
    wide = kept.shape[1] // 2
    cols = send.shape[1]
    part = kept.shape[0] // 2
    half = part // 2
    for i in range(4):
        side, c = divmod(i, 2)
        rows, at = slice(c * part, (c + 1) * part), slice(side * wide, side * wide + cut)
        last = slice(cols + i * keys, cols + (i + 1) * keys)
        block = jnp.concatenate(
            [kept[rows, at] + got[rows, at], kept_last[:, last] + got_last[:, last]], axis=1
        )
        mine, away = lane_rows(ids, block)
        at = slice(i * half, (i + 1) * half)
        keep[at, :] = mine
        send[at, :] = away.astype(BF16)


def keys_kernel(keys, keep0, got0, keep1, got1, keep2, got2, cos, sin, turn, gain, out):
    cols = keep0.shape[1]
    part = keep1.shape[0]
    for i in range(4):
        last = slice(cols + i * keys, cols + (i + 1) * keys)
        tail = keep2[:, last] + got2[:, last].astype(F32)
        keep, got = ((keep0, got0), (keep0, got0), (keep1, got1), (keep2, got2))[i]
        rows = slice(part, 2 * part) if i == 1 else slice(0, part)
        block = keep[rows, :cols] + got[rows, :cols].astype(F32)
        raw = jnp.concatenate([tail, block], axis=1)
        at = slice(i * part, (i + 1) * part)
        latent = raw[:, :KVL]
        inverse = lax.rsqrt(jnp.sum(latent * latent, axis=1, keepdims=True) / KVL + norm_eps)
        out[at, :KVL] = (latent * inverse * gain[...]).astype(BF16)
        rope = raw[:, KVL:]
        partner = dot_n(rope, turn[...], precision=lax.Precision.HIGHEST)
        out[at, KVL:] = (rope * cos[at, :] + partner * sin[at, :]).astype(BF16)


def pack(out, level, packed_ref):
    packed_ref[:, :KVL] = out.astype(BF16)
    lead = level.astype(BF16).astype(F32)
    rest = (level - lead).astype(BF16).astype(F32)
    last = level - lead - rest
    lane = lax.broadcasted_iota(jnp.int32, (out.shape[0], 128), 1)
    tail = jnp.where(lane == 0, lead, jnp.where(lane == 1, rest, jnp.where(lane == 2, last, 0.0)))
    packed_ref[:, KVL:] = tail.astype(BF16)


def unpack(packed):
    level = jnp.sum(packed[:, KVL:].astype(F32), axis=1, keepdims=True)
    return packed[:, :KVL].astype(F32), level


def attend_kernel(query_ref, k0_ref, k1_ref, bias_ref, old_ref, far_ref, packed_ref):
    query = query_ref[...]
    keys = k0_ref.shape[0]
    requests = bias_ref.shape[0] // 2
    heads = query.shape[0] // requests
    bias = bias_ref[...]
    wide = jnp.concatenate(
        [jnp.broadcast_to(bias[r : r + 1], (heads, 2 * keys)) for r in range(requests)], axis=0
    )
    scores = jnp.concatenate([dot_t(query, k0_ref[...]), dot_t(query, k1_ref[...])], axis=1)
    scores = scores * softmax_scale + wide
    old, old_level = unpack(old_ref[...])
    far, far_level = unpack(far_ref[...])
    peak = jnp.maximum(old_level, far_level)
    peak = jnp.maximum(peak, jnp.max(scores, axis=1, keepdims=True))
    weights = jnp.where(wide < 0.0, 0.0, jnp.exp(scores - peak))
    old_share, far_share = jnp.exp(old_level - peak), jnp.exp(far_level - peak)
    total = jnp.sum(weights, axis=1, keepdims=True) + old_share + far_share
    rounded = weights.astype(BF16)
    out = dot_n(rounded[:, :keys], k0_ref[:, :KVL]) + dot_n(rounded[:, keys:], k1_ref[:, :KVL])
    out = out + old * old_share + far * far_share
    pack(out / total, peak + jnp.log(total), packed_ref)


def combine_kernel(ids, own, across, partner, other, out):
    odd = ids[2] % 2 == 1
    first, level = unpack(jnp.where(odd, own[...], partner[...]))
    second, other_level = unpack(jnp.where(odd, across[...], other[...]))
    top = jnp.maximum(level, other_level)
    share, other_share = jnp.exp(level - top), jnp.exp(other_level - top)
    out[...] = ((first * share + second * other_share) / (share + other_share)).astype(BF16)


def return_kernel(keep0, got0, keep1, got1, keep2, got2, keep3, got3, low, high, send):
    rows, cols = low.shape
    half = rows // 2
    part = keep1.shape[0]
    for i in range(4):
        keep, got = ((keep0, got0), (keep0, got0), (keep1, got1), (keep2, got2))[i]
        start = part if i == 1 else 0
        from_rows, at = slice(start, start + half), slice(i * half, (i + 1) * half)
        first = keep[from_rows, :cols] + got[from_rows, :cols].astype(F32)
        second = keep3[at, :] + got3[at, :].astype(F32)
        if i < 2:
            low[at, :] = first
            high[at, :] = second
        else:
            at = slice((i - 2) * half, (i - 1) * half)
            send[at, :cols] = first.astype(BF16)
            send[at, cols:] = second.astype(BF16)


def query_kernel(ids, low, high, got, gain, *refs):
    sends, scratch = refs[:-1], refs[-1]
    odd = ids[2] % 2 == 1
    cols = low.shape[1]
    cut = QL - 2 * cols
    got_low, got_high = got[:, :cols].astype(F32), got[:, cols:].astype(F32)
    first = jnp.where(odd, got_low, low[...])
    second = jnp.where(odd, got_high, high[...])
    third = jnp.where(odd, high[:, :cut], got_high[:, :cut])
    rows = jnp.concatenate([first, second, third], axis=1)
    inverse = lax.rsqrt(jnp.sum(rows * rows, axis=1, keepdims=True) / QL + norm_eps)
    rows = (rows * inverse * gain[...]).astype(BF16)
    scratch[...] = rows
    width = QL // len(sends)
    lane = 2 * ids[3] + ids[1]
    for k, send in enumerate(sends):
        target = jnp.bitwise_xor(lane, k)
        send[...] = scratch[:, pl.ds(pl.multiple_of(target * width, 128), width)]


def place_kernel(ids, *refs):
    gots, out = refs[:-1], refs[-1]
    half = gots[0].shape[0] // 2
    chunk = out.shape[0] // 2
    lane = 2 * ids[3] + ids[1]
    for k, got in enumerate(gots):
        source = jnp.bitwise_xor(lane, k)
        start = (source % 2) * (2 * half) + (source // 2) * half
        for c in range(2):
            at = pl.ds(pl.multiple_of(c * chunk + start, 16), half)
            out[at, :] = got[c * half : (c + 1) * half, :]


def call(kernel, shapes, specs, args, scratch=()):
    return pl.pallas_call(
        kernel,
        scratch_shapes=scratch,
        out_shape=shapes,
        in_specs=specs,
        out_specs=[VMEM] * len(shapes) if isinstance(shapes, list) else VMEM,
        cost_estimate=pl.CostEstimate(flops=20_000_000, bytes_accessed=2_000_000, transcendentals=0),
        compiler_params=pltpu.CompilerParams(vmem_limit_bytes=VMEM_GRANT),
    )(*args)


def shaped(*dims, kind=F32):
    return jax.ShapeDtypeStruct(dims, kind)


def body_pairs(*args):
    return pairs_step(*args)


def pairs_step(
    hidden_x,
    proj_weight,
    q_gain,
    kv_gain,
    old_cache,
    page_plan,
    block_table,
    split_lens,
    dec_query,
    new_key,
):
    n = lax.axis_size(DEC)
    group, index = lax.axis_index(GRP), lax.axis_index(DEC)
    stage, core = lax.axis_index(STG), lax.axis_index(TP)
    ids = jnp.stack([group, core, index, stage]).astype(jnp.int32)
    tokens, feats = hidden_x.shape
    cols = proj_weight.shape[1]
    cut = QL - 2 * cols
    half = feats // 2
    pages = page_plan.shape[0]
    requests, heads, _ = dec_query.shape
    queries = requests * heads
    rows = tokens // 2
    quarter = rows // 2

    weight = proj_weight.T
    split = cols // 2 // 128 * 128
    pieces = [
        lax.dynamic_slice(weight, (0, group * half), (split, half)),
        lax.dynamic_slice(weight, (split, group * half), (cols - split, half)),
    ]
    partners = [(0, 1), (1, 0), (2, 3), (3, 2)]
    inner = [(g * n + i, (1 - g) * n + i) for g in range(2) for i in (1, 2)]
    a_z, a_y, b_z, b_y = [None] * 2, [None] * 2, [None] * 2, [None] * 2
    for p in (1, 0):
        a_z[p] = lax.ppermute(pieces[p], DEC, [(0, 2), (3, 1), (1, 0), (2, 3)])
    packed = jnp.concatenate(
        [page_plan.reshape(-1), block_table.reshape(-1), split_lens.reshape(-1)]
    ).reshape(1, -1)
    tables = [packed]
    for s in range(1, n):
        tables.append(lax.ppermute(packed, DEC, [((i + s) % n, i) for i in range(n)]))
    tables = jnp.pad(
        jnp.concatenate(tables, axis=0), ((0, 8 - n), (0, -packed.shape[1] % 128))
    )
    x_far = []
    for c in range(2):
        x_far.append(lax.ppermute(hidden_x[c * rows : (c + 1) * rows], DEC, partners))
    direct = split // 2
    held = lax.optimization_barrier(
        (pieces[0][direct:], pieces[1], weight[:direct], a_z[0])
    )
    for p in (1, 0):
        a_y[p] = swap(a_z[p], GRP)
        b_z[p] = lax.ppermute(held[p], DEC, [(1, 2), (2, 1)])
    b_whole = lax.ppermute(held[2], DEC, [(1, 2), (2, 1)])
    for p in (1, 0):
        b_y[p] = lax.ppermute(b_z[p], (GRP, DEC), inner)
    query = dec_query.reshape(queries, KVW)
    padded_key = jnp.pad(new_key, ((0, 3 * requests), (0, 0)))
    old, bias = call(
        functools.partial(old_kernel, n, pages),
        [shaped(queries, KVL + 128, kind=BF16), shaped(8, 2 * tokens)],
        [SMEM, VMEM, VMEM, VMEM, VMEM],
        (ids, tables, query, old_cache.reshape(-1, KVW), padded_key),
    )

    old_far = lax.ppermute(old, DEC, partners)

    partner = index + 1 - 2 * (index % 2)
    place = jnp.arange(rows, dtype=jnp.int32)
    place = place + core * quarter + (place // quarter) * quarter
    positions = jnp.concatenate([index * tokens + place, partner * tokens + place]).astype(F32)
    pair = jnp.arange(ROPE, dtype=jnp.int32) // 2
    frequency = jnp.power(F32(10000.0), -(2 * pair).astype(F32) / ROPE)
    angles = positions[:, None] * frequency[None, :]
    turn = call(turn_kernel, shaped(ROPE, ROPE), [], ())
    early_ids, cos, sin, turn, kv_scale, q_scale = lax.optimization_barrier(
        (ids, jnp.cos(angles), jnp.sin(angles), turn, kv_gain.reshape(1, -1), q_gain.reshape(1, -1))
    )

    a_refs = (a_z[0], a_y[0], a_z[1], a_y[1])
    keys = cols - cut
    wide = -(-cut // 128) * 128
    last = cols + 4 * keys

    def crossed(kernel, rows, width, args):
        send, kept = project(kernel, rows, width, args)
        other = swap(send, TP)
        send, keep = call(
            functools.partial(cross_kernel, cols, quarter),
            [shaped(rows, width, kind=BF16), shaped(rows, width)],
            [SMEM, VMEM, VMEM],
            (ids, kept, other),
        )
        return (keep, swap(send, STG)), (kept, other)

    near, _ = crossed(
        functools.partial(near_kernel, rows), rows, cols, (early_ids, hidden_x, weight, *a_refs)
    )
    far, _ = crossed(
        functools.partial(far_kernel, rows), quarter, cols, (ids, x_far[0], weight, *a_refs)
    )
    final, final_sums = crossed(
        functools.partial(last_kernel, rows, keys),
        quarter,
        last,
        (ids, hidden_x, *x_far, weight, *a_refs, b_z[1], b_y[1]),
    )
    send, kept = project(
        functools.partial(rest_kernel, rows, keys),
        rows,
        2 * wide,
        (ids, hidden_x, *x_far, *a_refs, b_whole, b_z[0], b_y[0], b_z[1], b_y[1]),
    )
    other = swap(send, TP)
    send, kept = call(
        functools.partial(cross_rest_kernel, cut, keys),
        [shaped(rows, cols, kind=BF16), shaped(rows, cols)],
        [SMEM] + [VMEM] * 4,
        (ids, kept, other, *final_sums),
    )
    rest = (kept, swap(send, STG))

    key_rows = call(
        functools.partial(keys_kernel, keys),
        shaped(tokens, KVW, kind=BF16),
        [VMEM] * 10,
        (*near, *far, *final, cos, sin, turn, kv_scale),
    )
    far_keys = swap(key_rows, TP)
    part_out = call(
        attend_kernel,
        shaped(queries, KVL + 128, kind=BF16),
        [VMEM] * 6,
        (query, key_rows, far_keys, bias, old, old_far),
    )
    spread = []
    for pairs in ([(1, 3), (3, 1)], [(1, 0), (3, 2)], [(1, 2), (3, 0)]):
        spread.append(lax.ppermute(part_out, DEC, pairs))
    attn = call(
        combine_kernel,
        shaped(queries, KVL, kind=BF16),
        [SMEM] + [VMEM] * 4,
        (ids, part_out, *spread),
    )

    low, high, back = call(
        return_kernel,
        [shaped(quarter, cols), shaped(quarter, cols), shaped(quarter, 2 * cols, kind=BF16)],
        [VMEM] * 8,
        (*near, *far, *final, *rest),
    )
    back = lax.ppermute(back, DEC, partners)
    lanes = 4
    width = QL // lanes
    tile = shaped(quarter, width, kind=BF16)
    blocks = call(
        query_kernel,
        [tile] * lanes,
        [SMEM] + [VMEM] * 4,
        (ids, low, high, back, q_scale),
        scratch=[pltpu.VMEM((quarter, QL), BF16)],
    )
    gots = [blocks[0]]
    for k in range(1, lanes):
        gots.append(lax.ppermute(blocks[k], (STG, TP), [(i, i ^ k) for i in range(lanes)]))
    q_latent = call(
        place_kernel, shaped(tokens, width, kind=BF16), [SMEM] + [VMEM] * lanes, (ids, *gots)
    )
    return (q_latent, attn.reshape(requests, heads, KVL))


def solution(mesh):
    sizes = dict(mesh.shape)
    pairs = sizes["dec"] == 4 and sizes["grp"] == sizes["stg"] == sizes["tp"] == 2
    return jax.shard_map(
        body_pairs if pairs else body_general,
        mesh=mesh,
        in_specs=(
            P(("grp", "dec"), ("stg", "tp")),
            P(("stg", "tp"), "dec"),
            P(),
            P(),
            P(("grp", "dec"), None, None),
            P(("grp", "dec"), None),
            P(("grp", "dec"), None, None),
            P("grp", "dec"),
            P("grp", ("stg", "tp"), None),
            P("grp", None),
        ),
        out_specs=(P(("grp", "dec"), ("stg", "tp")), P("grp", ("stg", "tp"), None)),
        check_vma=False,
    )
```

```python
import functools

import jax
import jax.numpy as jnp
from jax import lax
from jax.experimental import pallas as pl
from jax.experimental.pallas import tpu as pltpu
from jax.sharding import PartitionSpec as P


QL = 1536
KVL = 512
ROPE = 64
PAGE = 32
KVW = KVL + ROPE
MASKED = -1e30

softmax_scale = 192.0 ** (-0.5)
norm_eps = 1e-06


def combined_all(part, axis, combine):
    gathered = jax.tree.map(lambda a: lax.all_gather(a, axis), part)

    def take(source):
        return jax.tree.map(lambda a: lax.dynamic_index_in_dim(a, source, 0, False), gathered)

    return lax.fori_loop(
        1, lax.axis_size(axis), lambda source, state: combine(state, take(source)), take(0)
    )


def rope_rotate(matrix, col_start, positions):
    col_count = matrix.shape[1]
    columns = col_start + jnp.arange(col_count, dtype=jnp.int32)
    is_rope = columns >= KVL
    pair_index = jnp.maximum(columns - KVL, 0) // 2
    frequency = jnp.power(jnp.float32(10000.0), -(2 * pair_index).astype(jnp.float32) / ROPE)
    angles = positions[:, None] * frequency[None, :]
    cosine = jnp.where(is_rope[None, :], jnp.cos(angles), 1.0)
    sine_part = jnp.where(is_rope[None, :], jnp.sin(angles), 0.0)
    paired = matrix.reshape(matrix.shape[0], col_count // 2, 2)
    partner = jnp.stack([-paired[:, :, 1], paired[:, :, 0]], axis=2).reshape(matrix.shape)
    return matrix * cosine + partner * sine_part


def kv_finish(matrix, col_start, latent_sq, kv_gain, positions):
    col_count = matrix.shape[1]
    columns = col_start + jnp.arange(col_count, dtype=jnp.int32)
    gain_full = jnp.concatenate([kv_gain, jnp.ones((ROPE,), jnp.float32)])
    gain_cols = lax.dynamic_slice_in_dim(gain_full, col_start, col_count)
    inverse = lax.rsqrt(latent_sq / KVL + norm_eps)
    row_scale = jnp.where(columns[None, :] < KVL, inverse[:, None] * gain_cols[None, :], 1.0)
    return rope_rotate(matrix * row_scale, col_start, positions).astype(jnp.bfloat16)


def pack_pages(kv_pages, page_table, owner_count, capacity):
    owners = page_table[:, 0]
    slot_ids = page_table[:, 1]
    page_ids = jnp.arange(kv_pages.shape[0], dtype=jnp.int32)
    earlier = (owners[:, None] == owners[None, :]) & (page_ids[None, :] < page_ids[:, None])
    ranking = jnp.sum(earlier.astype(jnp.int32), axis=1)
    targets = owners * capacity + ranking
    places = jnp.arange(owner_count * capacity, dtype=jnp.int32)
    matches = targets[None, :] == places[:, None]
    source_ids = jnp.sum(jnp.where(matches, page_ids[None, :], 0), axis=1)
    filled = jnp.any(matches, axis=1)
    chosen = jnp.where(
        filled[:, None, None], jnp.take(kv_pages, source_ids, axis=0), jnp.zeros((), kv_pages.dtype)
    )
    labels = jnp.where(filled, jnp.take(slot_ids, source_ids), -1).astype(jnp.bfloat16)
    return (
        chosen.reshape(owner_count, capacity, kv_pages.shape[1], kv_pages.shape[2]),
        labels.reshape(owner_count, capacity),
    )


def place_pages(old_cache, got_pages, got_labels):
    flat_pages = got_pages.reshape(-1, old_cache.shape[1], old_cache.shape[2])
    label_ids = got_labels.reshape(-1).astype(jnp.int32)
    slot_ids = jnp.arange(old_cache.shape[0], dtype=jnp.int32)
    arrival_ids = jnp.arange(label_ids.shape[0], dtype=jnp.int32)
    matches = label_ids[None, :] == slot_ids[:, None]
    source_ids = jnp.sum(jnp.where(matches, arrival_ids[None, :], 0), axis=1)
    arrived = jnp.any(matches, axis=1)
    return jnp.where(arrived[:, None, None], jnp.take(flat_pages, source_ids, axis=0), old_cache)


def combine_parts(former, latter):
    overall = jnp.maximum(former[0], latter[0])
    front_scale = jnp.exp(former[0] - overall)
    back_scale = jnp.exp(latter[0] - overall)
    return (
        overall,
        former[1] * front_scale + latter[1] * back_scale,
        former[2] * front_scale[:, :, None] + latter[2] * back_scale[:, :, None],
    )


def body_general(
    hidden_x,
    proj_weight,
    q_gain,
    kv_gain,
    old_cache,
    page_plan,
    block_table,
    split_lens,
    dec_query,
    new_key,
):
    projected = jnp.dot(
        hidden_x,
        lax.all_gather(proj_weight, "dec", axis=1, tiled=True),
        preferred_element_type=jnp.float32,
    )
    query_part = projected[:, :QL]
    kv_part = projected[:, QL:]
    tokens_here = hidden_x.shape[0]
    positions = (
        lax.axis_index("dec") * tokens_here + jnp.arange(tokens_here, dtype=jnp.int32)
    ).astype(jnp.float32)
    lane_count = lax.axis_size(("stg", "tp"))
    lane_index = lax.axis_index(("stg", "tp"))
    owner_count = lax.axis_size("dec")
    page_count = page_plan.shape[0]
    capacity = max(2, -(-page_count // owner_count))
    query_width = QL // lane_count
    query_cols, kv_cols = (
        lax.psum_scatter(query_part, ("stg", "tp"), scatter_dimension=1, tiled=True),
        lax.psum_scatter(kv_part, ("stg", "tp"), scatter_dimension=1, tiled=True),
    )
    kv_width = kv_cols.shape[1]
    col_start = lane_index * kv_width
    columns = col_start + jnp.arange(kv_width, dtype=jnp.int32)
    latent_part_sq = jnp.sum(jnp.where(columns[None, :] < KVL, kv_cols * kv_cols, 0.0), axis=1)
    query_sq, latent_sq = lax.psum(
        (jnp.sum(query_cols * query_cols, axis=1), latent_part_sq), ("stg", "tp")
    )
    kv_rows = kv_finish(kv_cols, col_start, latent_sq, kv_gain, positions)
    kv_pages = kv_rows.reshape(page_count, PAGE, kv_width)
    send_pages, send_labels = pack_pages(kv_pages, page_plan, owner_count, capacity)
    got_slices, got_labels = (
        lax.all_to_all(send_pages, "dec", split_axis=0, concat_axis=0, tiled=True),
        lax.all_to_all(send_labels, "dec", split_axis=0, concat_axis=0, tiled=True),
    )
    got_pages = lax.all_gather(got_slices, ("stg", "tp"), axis=3, tiled=True)
    query_gain = lax.dynamic_slice_in_dim(q_gain, lane_index * query_width, query_width)
    q_latent = (
        query_cols * lax.rsqrt(query_sq / QL + norm_eps)[:, None] * query_gain[None, :]
    ).astype(jnp.bfloat16)
    cache = place_pages(old_cache, got_pages, got_labels)
    slot_table = block_table[0]
    request_count = slot_table.shape[0]
    key_rows = jnp.take(cache, slot_table.reshape(-1), axis=0).reshape(
        request_count, -1, cache.shape[2]
    )
    scores = (
        jnp.einsum("rhc,rlc->rhl", dec_query, key_rows, preferred_element_type=jnp.float32)
        * softmax_scale
    )
    live_mask = jnp.arange(key_rows.shape[1], dtype=jnp.int32)[None, :] < split_lens[:, 0][:, None]
    scores = jnp.where(live_mask[:, None, :], scores, -1e30)
    row_peak = jnp.max(scores, axis=2)
    weights = jnp.where(live_mask[:, None, :], jnp.exp(scores - row_peak[:, :, None]), 0.0)
    row_total = jnp.sum(weights, axis=2)
    rounded = weights.astype(jnp.bfloat16)
    partial_out = jnp.einsum(
        "rhl,rlc->rhc", rounded, key_rows[:, :, :KVL], preferred_element_type=jnp.float32
    )
    peak_all, total_all, output_all = combined_all(
        (row_peak, row_total, partial_out), "dec", combine_parts
    )
    self_score = (
        jnp.einsum("rhc,rc->rh", dec_query, new_key, preferred_element_type=jnp.float32)
        * softmax_scale
    )
    overall = jnp.maximum(peak_all, self_score)
    carried = jnp.exp(peak_all - overall)
    self_weight = jnp.exp(self_score - overall)
    denom = total_all * carried + self_weight
    numer = output_all * carried[:, :, None] + self_weight[:, :, None] * new_key[
        :, None, :KVL
    ].astype(jnp.float32)
    attn_latent = (numer / denom[:, :, None]).astype(jnp.bfloat16)
    return (q_latent, attn_latent)


VMEM = pl.BlockSpec(memory_space=pltpu.VMEM)
SMEM = pl.BlockSpec(memory_space=pltpu.SMEM)
VMEM_GRANT = 16 * 2**20
GRP, DEC, STG, TP = "grp", "dec", "stg", "tp"
TILE = 256
F32 = jnp.float32
BF16 = jnp.bfloat16


def swap(a, axis):
    return lax.ppermute(a, axis, [(0, 1), (1, 0)])


def dot_t(a, b, **kw):
    return lax.dot_general(a, b, (((1,), (1,)), ((), ())), preferred_element_type=F32, **kw)


def dot_n(a, b, **kw):
    return lax.dot_general(a, b, (((1,), (0,)), ((), ())), preferred_element_type=F32, **kw)


def chosen(outer, own, sent):
    return jnp.where(outer, own, sent)


def halves(ids, x_ref):
    half = x_ref.shape[1] // 2
    here = pl.ds(pl.multiple_of(ids[0] * half, 128), half)
    there = pl.ds(pl.multiple_of((1 - ids[0]) * half, 128), half)
    return here, there


def is_outer(ids):
    return (ids[2] == 0) | (ids[2] == 3)


def put(ids, out, send, keep, start):
    rows = send.shape[0]
    top, bottom = out[:rows], out[rows:]
    at = slice(start, start + out.shape[1])
    send[:, at] = jnp.where(ids[1] == 0, bottom, top)
    keep[:, at] = jnp.where(ids[1] == 0, top, bottom)


def primary(ids, x_ref, own_ref, parts, send, keep):
    here, there = halves(ids, x_ref)
    outer = is_outer(ids)
    start = 0
    for z, y in parts:
        at = slice(start, start + z.shape[0])
        w_here = chosen(outer, own_ref[at, here], z[...])
        w_there = chosen(outer, own_ref[at, there], y[...])
        put(ids, dot_t(x_ref[:, here], w_here) + dot_t(x_ref[:, there], w_there), send, keep, start)
        start += z.shape[0]


def projected(ids, x_ref, w_here, w_there):
    here, there = halves(ids, x_ref)
    return dot_t(x_ref[:, here], w_here) + dot_t(x_ref[:, there], w_there)


def near_kernel(ids, x_ref, own_ref, z0, y0, z1, y1, send, keep):
    primary(ids, x_ref, own_ref, ((z0, y0), (z1, y1)), send, keep)


def far_kernel(keys, ids, x_ref, far_ref, own_ref, z0, y0, z1, y1, bz1, by1, send, keep):
    cols, head = own_ref.shape[0], z0.shape[0]
    full = z1.shape[0] // TILE * TILE
    outer = is_outer(ids)
    here, there = halves(ids, x_ref)
    primary(
        ids, far_ref, own_ref, ((z0, y0), (z1.at[:full, :], y1.at[:full, :])), send, keep
    )
    at, left, own = slice(z1.shape[0] - keys, None), slice(full, None), slice(head + full, None)
    k_here = chosen(outer, z1[at, :], bz1[at, :])
    k_there = chosen(outer, y1[at, :], by1[at, :])
    w_here = jnp.concatenate([chosen(outer, own_ref[own, here], z1[left, :]), k_here], axis=0)
    w_there = jnp.concatenate([chosen(outer, own_ref[own, there], y1[left, :]), k_there], axis=0)
    out = projected(ids, far_ref, w_here, w_there)
    put(ids, out[:, : cols - head - full], send, keep, head + full)
    put(ids, out[:, cols - head - full :], send, keep, cols + keys)
    put(ids, projected(ids, x_ref, k_here, k_there), send, keep, cols)


def rest_kernel(used, ids, x_ref, far_ref, z, y, bz, by, send, keep):
    outer = is_outer(ids)
    w_here = chosen(outer, z[:used, :], bz[:used, :])
    w_there = chosen(outer, y[:used, :], by[:used, :])
    put(ids, projected(ids, x_ref, w_here, w_there), send, keep, 0)
    put(ids, projected(ids, far_ref, w_here, w_there), send, keep, send.shape[1] - used)


def project(kernel, width, args):
    rows, feats = args[1].shape
    shape = jax.ShapeDtypeStruct((rows // 2, width), F32)
    return pl.pallas_call(
        kernel,
        in_specs=[SMEM] + [VMEM] * (len(args) - 1),
        out_specs=[VMEM] * 2,
        out_shape=[shape] * 2,
        cost_estimate=pl.CostEstimate(
            flops=2 * rows * feats * width, bytes_accessed=8 * rows * width, transcendentals=0
        ),
        compiler_params=pltpu.CompilerParams(vmem_limit_bytes=VMEM_GRANT),
    )(*args)


def share_kernel(ids, weight, out):
    out[...] = weight[...]


def share(ids, weight):
    rows, feats = weight.shape
    return pl.pallas_call(
        share_kernel,
        grid_spec=pltpu.PrefetchScalarGridSpec(
            num_scalar_prefetch=1,
            grid=(1,),
            in_specs=[pl.BlockSpec((rows, feats // 2), lambda i, ids: (0, ids[0]))],
            out_specs=pl.BlockSpec((rows, feats // 2), lambda i, ids: (0, 0)),
        ),
        out_shape=jax.ShapeDtypeStruct((rows, feats // 2), weight.dtype),
        compiler_params=pltpu.CompilerParams(vmem_limit_bytes=VMEM_GRANT),
    )(ids, weight)


def turn_kernel(out):
    source = lax.broadcasted_iota(jnp.int32, out.shape, 0)
    target = lax.broadcasted_iota(jnp.int32, out.shape, 1)
    down = (source == target + 1) & (target % 2 == 0)
    up = (source + 1 == target) & (target % 2 == 1)
    out[...] = jnp.where(down, -1.0, jnp.where(up, 1.0, 0.0))


def old_kernel(n, pages, ids, tab_ref, query_ref, rows_ref, own_ref, packed_ref, bias_ref):
    index, core = ids[2], ids[1]
    query = query_ref[...]
    keys = rows_ref.shape[0]
    requests = own_ref.shape[0] // 4
    heads = query.shape[0] // requests
    base = 2 * pages
    slots = keys // PAGE
    per = slots // requests

    def iota(rows, cols, axis):
        return lax.broadcasted_iota(jnp.int32, (rows, cols), axis)

    size = tab_ref.shape[1]
    diagonal = iota(size, size, 0) == iota(size, size, 1)
    columns = [
        jnp.sum(jnp.where(diagonal, tab_ref[s : s + 1, :], 0), axis=1, keepdims=True)
        for s in range(n)
    ]
    entry = iota(slots, 1, 0)
    readers = entry // per

    def limits(column):
        lengths = jnp.zeros((slots, 1), jnp.int32)
        for r in range(requests):
            at = base + slots + r
            lengths = jnp.where(readers == r, column[at : at + 1, :], lengths)
        return lengths - PAGE * (entry % per)

    def lookup(hit, values):
        return jnp.sum(jnp.where(hit, values, 0), axis=0, keepdims=True)

    page = iota(1, keys, 1) // PAGE
    hit = columns[0][base : base + slots, :] == page
    limit = lookup(hit, limits(columns[0]))
    reader = lookup(hit, readers)
    is_slot = iota(base, 1, 0) % 2 == 1
    taken = jnp.zeros((1, keys), jnp.int32)
    odd_row = iota(base, base, 0)
    follows = (iota(base, base, 1) == odd_row - 1) & (odd_row % 2 == 1)
    for s in range(n):
        plan = columns[s][:base, :]
        owners = jnp.sum(jnp.where(follows, tab_ref[s : s + 1, :base], 0), axis=1, keepdims=True)
        here = is_slot & (owners == index)
        taken = taken + jnp.sum(jnp.where(here & (plan == page), 1, 0), axis=0, keepdims=True)
    limit = jnp.where(taken > 0, 0, limit)
    live = (iota(1, keys, 1) % PAGE) < limit
    bias = jnp.where(live & (reader == iota(8, keys, 0)), 0.0, MASKED)
    wide = jnp.concatenate(
        [jnp.broadcast_to(bias[r : r + 1], (heads, keys)) for r in range(requests)], axis=0
    )
    scores = dot_t(query, rows_ref[...]) * softmax_scale + wide
    own = dot_t(query, own_ref[...]) * softmax_scale
    mine = iota(*own.shape, 0) // heads == iota(*own.shape, 1)
    own = jnp.sum(jnp.where(mine, own, 0.0), axis=1, keepdims=True)
    own = jnp.where(index == 0, own, MASKED)
    peak = jnp.maximum(jnp.max(scores, axis=1, keepdims=True), own)
    weights = jnp.where(wide < 0.0, 0.0, jnp.exp(scores - peak))
    own_weight = jnp.where(index == 0, jnp.exp(own - peak), 0.0)
    total = jnp.sum(weights, axis=1, keepdims=True) + own_weight
    out = dot_n(weights.astype(BF16), rows_ref[:, :KVL])
    own_rows = own_ref[:, :KVL].astype(F32)
    latent = jnp.concatenate(
        [jnp.broadcast_to(own_rows[r : r + 1], (heads, KVL)) for r in range(requests)], axis=0
    )
    pack((out + own_weight * latent) / total, peak + jnp.log(total), packed_ref)

    width = bias_ref.shape[1]
    half = pages // 2
    spot = iota(1, width, 1) // PAGE
    which = jnp.where(spot // pages == 1, 1 - core, core) * half + spot % half
    partner = (spot % pages) // half == 1
    line = iota(base, width, 0)
    plan = jnp.where(partner, columns[n - 1][:base, :], columns[0][:base, :])
    plan = jnp.where(line % 2 == 1, plan, plan * (2 * slots))
    code = jnp.sum(jnp.where(line // 2 == which, plan, 0), axis=0, keepdims=True)
    limit = jnp.zeros((1, width), jnp.int32)
    reader = jnp.zeros((1, width), jnp.int32)
    for s in range(n):
        owner = (index + s) % n
        hit = columns[s][base : base + slots, :] + owner * (2 * slots) == code
        limit = limit + lookup(hit, limits(columns[s]))
        reader = reader + lookup(hit, readers)
    limit = jnp.where(index % 2 == 1, limit, 0)
    live = (iota(1, width, 1) % PAGE) < limit
    bias_ref[...] = jnp.where(live & (reader == iota(8, width, 0)), 0.0, MASKED)


def parted(ids, block):
    half = block.shape[0] // 2
    odd, stage = ids[2] % 2 == 1, ids[3]
    top, bottom = block[:half], block[half:]
    mine = jnp.where(stage == 0, top, bottom)
    away = jnp.where(stage == 0, bottom, top)
    twice = lambda part: jnp.concatenate([part, part], axis=0)
    return jnp.where(odd, block, twice(mine)), jnp.where(odd, block, twice(away))


def cross_near_kernel(ids, kept, got, send, keep):
    mine, away = parted(ids, kept[...] + got[...])
    keep[...] = mine
    send[...] = away.astype(BF16)


def cross_far_kernel(cols, ids, kept, got, send, keep):
    both = kept[...] + got[...]
    mine, away = parted(ids, both[:, :cols])
    keep[:, :cols] = mine
    keep[:, cols:] = both[:, cols:]
    send[:, :cols] = away.astype(BF16)
    send[:, cols:] = both[:, cols:].astype(BF16)


def cross_rest_kernel(
    head, rest, keys, ids, kept_tail, got_tail, kept_head, got_head, kept_far, got_far, send, keep
):
    cols = send.shape[1]
    stage = ids[3]
    for i in range(2):
        start = i * (kept_head.shape[1] - head)
        at = slice(start, start + head)
        first = kept_head[:, at] + got_head[:, at]
        start = i * (kept_tail.shape[1] - rest)
        at = slice(start, start + rest)
        second = kept_tail[:, at] + got_tail[:, at]
        at = slice(cols + i * keys, cols + (i + 1) * keys)
        block = jnp.concatenate([first, second, kept_far[:, at] + got_far[:, at]], axis=1)
        half = block.shape[0] // 2
        top, bottom = block[:half], block[half:]
        at = slice(i * half, (i + 1) * half)
        keep[at, :] = jnp.where(stage == 0, top, bottom)
        send[at, :] = jnp.where(stage == 0, bottom, top).astype(BF16)


def keys_kernel(keys, keep0, got0, keep1, got1, cos, sin, turn, gain, out):
    rows, cols = keep0.shape
    for i in range(2):
        last = slice(cols + i * keys, cols + (i + 1) * keys)
        tail = keep1[:, last] + got1[:, last].astype(F32)
        if i == 0:
            block = keep0[...] + got0[...].astype(F32)
        else:
            block = keep1[:, :cols] + got1[:, :cols].astype(F32)
        raw = jnp.concatenate([tail, block], axis=1)
        at = slice(i * rows, (i + 1) * rows)
        latent = raw[:, :KVL]
        inverse = lax.rsqrt(jnp.sum(latent * latent, axis=1, keepdims=True) / KVL + norm_eps)
        out[at, :KVL] = (latent * inverse * gain[...]).astype(BF16)
        rope = raw[:, KVL:]
        partner = dot_n(rope, turn[...], precision=lax.Precision.HIGHEST)
        out[at, KVL:] = (rope * cos[at, :] + partner * sin[at, :]).astype(BF16)


def pack(out, level, packed_ref):
    packed_ref[:, :KVL] = out.astype(BF16)
    lead = level.astype(BF16).astype(F32)
    rest = (level - lead).astype(BF16).astype(F32)
    last = level - lead - rest
    lane = lax.broadcasted_iota(jnp.int32, (out.shape[0], 128), 1)
    tail = jnp.where(lane == 0, lead, jnp.where(lane == 1, rest, jnp.where(lane == 2, last, 0.0)))
    packed_ref[:, KVL:] = tail.astype(BF16)


def unpack(packed):
    level = jnp.sum(packed[:, KVL:].astype(F32), axis=1, keepdims=True)
    return packed[:, :KVL].astype(F32), level


def attend_kernel(query_ref, k0_ref, k1_ref, bias_ref, old_ref, far_ref, packed_ref):
    query = query_ref[...]
    keys = k0_ref.shape[0]
    requests = bias_ref.shape[0] // 2
    heads = query.shape[0] // requests
    bias = bias_ref[...]
    wide = jnp.concatenate(
        [jnp.broadcast_to(bias[r : r + 1], (heads, 2 * keys)) for r in range(requests)], axis=0
    )
    scores = jnp.concatenate([dot_t(query, k0_ref[...]), dot_t(query, k1_ref[...])], axis=1)
    scores = scores * softmax_scale + wide
    old, old_level = unpack(old_ref[...])
    far, far_level = unpack(far_ref[...])
    peak = jnp.maximum(old_level, far_level)
    peak = jnp.maximum(peak, jnp.max(scores, axis=1, keepdims=True))
    weights = jnp.where(wide < 0.0, 0.0, jnp.exp(scores - peak))
    old_share, far_share = jnp.exp(old_level - peak), jnp.exp(far_level - peak)
    total = jnp.sum(weights, axis=1, keepdims=True) + old_share + far_share
    rounded = weights.astype(BF16)
    out = dot_n(rounded[:, :keys], k0_ref[:, :KVL]) + dot_n(rounded[:, keys:], k1_ref[:, :KVL])
    out = out + old * old_share + far * far_share
    pack(out / total, peak + jnp.log(total), packed_ref)


def combine_kernel(ids, own, across, partner, other, out):
    odd = ids[2] % 2 == 1
    first, level = unpack(jnp.where(odd, own[...], partner[...]))
    second, other_level = unpack(jnp.where(odd, across[...], other[...]))
    top = jnp.maximum(level, other_level)
    share, other_share = jnp.exp(level - top), jnp.exp(other_level - top)
    out[...] = ((first * share + second * other_share) / (share + other_share)).astype(BF16)


def return_first_kernel(keep0, got0, keep1, got1, low, send):
    rows, cols = low.shape
    low[...] = keep0[:rows, :] + got0[:rows, :].astype(F32)
    send[...] = (keep1[:rows, :cols] + got1[:rows, :cols].astype(F32)).astype(BF16)


def return_second_kernel(keep, got, high, send):
    rows = high.shape[0]
    both = keep[...] + got[...].astype(F32)
    high[...] = both[:rows]
    send[...] = both[rows:].astype(BF16)


def query_kernel(ids, low, high, got_first, got_second, gain, *refs):
    sends, scratch = refs[:-1], refs[-1]
    odd = ids[2] % 2 == 1
    cols = low.shape[1]
    cut = QL - 2 * cols
    got_low, got_high = got_first[...].astype(F32), got_second[...].astype(F32)
    first = jnp.where(odd, got_low, low[...])
    second = jnp.where(odd, got_high, high[...])
    third = jnp.where(odd, high[:, :cut], got_high[:, :cut])
    rows = jnp.concatenate([first, second, third], axis=1)
    inverse = lax.rsqrt(jnp.sum(rows * rows, axis=1, keepdims=True) / QL + norm_eps)
    rows = (rows * inverse * gain[...]).astype(BF16)
    scratch[...] = rows
    width = QL // len(sends)
    lane = 2 * ids[3] + ids[1]
    for k, send in enumerate(sends):
        target = jnp.bitwise_xor(lane, k)
        send[...] = scratch[:, pl.ds(pl.multiple_of(target * width, 128), width)]


def place_kernel(ids, *refs):
    gots, out = refs[:-1], refs[-1]
    rows = gots[0].shape[0]
    lane = 2 * ids[3] + ids[1]
    for k, got in enumerate(gots):
        source = jnp.bitwise_xor(lane, k)
        order = 2 * (source % 2) + source // 2
        out[pl.ds(pl.multiple_of(order * rows, 32), rows), :] = got[...]


def call(kernel, shapes, specs, args, scratch=()):
    return pl.pallas_call(
        kernel,
        scratch_shapes=scratch,
        out_shape=shapes,
        in_specs=specs,
        out_specs=[VMEM] * len(shapes) if isinstance(shapes, list) else VMEM,
        cost_estimate=pl.CostEstimate(flops=20_000_000, bytes_accessed=2_000_000, transcendentals=0),
        compiler_params=pltpu.CompilerParams(vmem_limit_bytes=VMEM_GRANT),
    )(*args)


def shaped(*dims, kind=F32):
    return jax.ShapeDtypeStruct(dims, kind)


def body_pairs(*args):
    return pairs_step(*args)


def pairs_step(
    hidden_x,
    proj_weight,
    q_gain,
    kv_gain,
    old_cache,
    page_plan,
    block_table,
    split_lens,
    dec_query,
    new_key,
):
    n = lax.axis_size(DEC)
    group, index = lax.axis_index(GRP), lax.axis_index(DEC)
    stage, core = lax.axis_index(STG), lax.axis_index(TP)
    ids = jnp.stack([group, core, index, stage]).astype(jnp.int32)
    tokens, _ = hidden_x.shape
    cols = proj_weight.shape[1]
    cut = QL - 2 * cols
    pages = page_plan.shape[0]
    requests, heads, _ = dec_query.shape
    queries = requests * heads
    rows = tokens // 2
    quarter = rows // 2

    weight = proj_weight.T
    split = cols // 2 // 128 * 128
    pieces = [share(ids, weight[:split]), share(ids, weight[split:])]
    partners = [(0, 1), (1, 0), (2, 3), (3, 2)]
    a_z, a_y, b_z, b_y = [None] * 2, [None] * 2, [None] * 2, [None] * 2
    for p in (1, 0):
        a_z[p] = lax.ppermute(pieces[p], DEC, [(0, 2), (3, 1), (1, 0), (2, 3)])
    packed = jnp.concatenate(
        [page_plan.reshape(-1), block_table.reshape(-1), split_lens.reshape(-1)]
    ).reshape(1, -1)
    tables = [packed]
    for s in range(1, n):
        tables.append(lax.ppermute(packed, DEC, [((i + s) % n, i) for i in range(n)]))
    tables = jnp.pad(
        jnp.concatenate(tables, axis=0), ((0, 8 - n), (0, -packed.shape[1] % 128))
    )
    x_far = lax.ppermute(hidden_x, DEC, partners)
    held = lax.optimization_barrier((pieces[0], pieces[1], a_z[0]))
    for p in (1, 0):
        a_y[p] = swap(a_z[p], GRP)
        b_z[p] = lax.ppermute(held[p], DEC, [(1, 2), (2, 1)])
    for p in (1, 0):
        b_y[p] = swap(b_z[p], GRP)
    query = dec_query.reshape(queries, KVW)
    padded_key = jnp.pad(new_key, ((0, 3 * requests), (0, 0)))
    old, bias = call(
        functools.partial(old_kernel, n, pages),
        [shaped(queries, KVL + 128, kind=BF16), shaped(8, 2 * tokens)],
        [SMEM, VMEM, VMEM, VMEM, VMEM],
        (ids, tables, query, old_cache.reshape(-1, KVW), padded_key),
    )

    old_far = lax.ppermute(old, DEC, partners)

    partner = index + 1 - 2 * (index % 2)
    place = core * rows + jnp.arange(rows, dtype=jnp.int32)
    positions = jnp.concatenate([index * tokens + place, partner * tokens + place]).astype(F32)
    pair = jnp.arange(ROPE, dtype=jnp.int32) // 2
    frequency = jnp.power(F32(10000.0), -(2 * pair).astype(F32) / ROPE)
    angles = positions[:, None] * frequency[None, :]
    turn = call(turn_kernel, shaped(ROPE, ROPE), [], ())
    early_ids, cos, sin, turn, kv_scale, q_scale = lax.optimization_barrier(
        (ids, jnp.cos(angles), jnp.sin(angles), turn, kv_gain.reshape(1, -1), q_gain.reshape(1, -1))
    )

    a_refs = (a_z[0], a_y[0], a_z[1], a_y[1])
    keys = cols - cut
    send, kept0 = project(near_kernel, cols, (early_ids, hidden_x, weight, *a_refs))
    other0 = swap(send, TP)
    send0, keep0 = call(
        cross_near_kernel,
        [shaped(rows, cols, kind=BF16), shaped(rows, cols)],
        [SMEM, VMEM, VMEM],
        (ids, kept0, other0),
    )
    got0 = swap(send0, STG)
    send, kept1 = project(
        functools.partial(far_kernel, keys),
        cols + 2 * keys,
        (ids, hidden_x, x_far, weight, *a_refs, b_z[1], b_y[1]),
    )
    other1 = swap(send, TP)
    send1, keep1 = call(
        functools.partial(cross_far_kernel, cols),
        [shaped(rows, cols + 2 * keys, kind=BF16), shaped(rows, cols + 2 * keys)],
        [SMEM, VMEM, VMEM],
        (ids, kept1, other1),
    )
    got1 = swap(send1, STG)
    used = (cols - split - keys, split)
    rest = []
    for k, p in enumerate((1, 0)):
        send, kept = project(
            functools.partial(rest_kernel, used[k]),
            -(-used[k] // 128) * 128 + used[k],
            (ids, hidden_x, x_far, a_z[p], a_y[p], b_z[p], b_y[p]),
        )
        rest += [kept, swap(send, TP)]
    send2, keep2 = call(
        functools.partial(cross_rest_kernel, split, used[0], keys),
        [shaped(rows, cols, kind=BF16), shaped(rows, cols)],
        [SMEM] + [VMEM] * 6,
        (ids, *rest, kept1, other1),
    )
    got2 = swap(send2, STG)

    key_rows = call(
        functools.partial(keys_kernel, keys),
        shaped(tokens, KVW, kind=BF16),
        [VMEM] * 8,
        (keep0, got0, keep1, got1, cos, sin, turn, kv_scale),
    )
    far_keys = swap(key_rows, TP)
    part_out = call(
        attend_kernel,
        shaped(queries, KVL + 128, kind=BF16),
        [VMEM] * 6,
        (query, key_rows, far_keys, bias, old, old_far),
    )
    spread = []
    for pairs in ([(1, 3), (3, 1)], [(1, 0), (3, 2)], [(1, 2), (3, 0)]):
        spread.append(lax.ppermute(part_out, DEC, pairs))
    attn = call(
        combine_kernel,
        shaped(queries, KVL, kind=BF16),
        [SMEM] + [VMEM] * 4,
        (ids, part_out, *spread),
    )

    low, back0 = call(
        return_first_kernel,
        [shaped(quarter, cols), shaped(quarter, cols, kind=BF16)],
        [VMEM] * 4,
        (keep0, got0, keep1, got1),
    )
    back0 = lax.ppermute(back0, DEC, partners)
    high, back1 = call(
        return_second_kernel,
        [shaped(quarter, cols), shaped(quarter, cols, kind=BF16)],
        [VMEM] * 2,
        (keep2, got2),
    )
    back1 = lax.ppermute(back1, DEC, partners)
    lanes = 4
    width = QL // lanes
    tile = shaped(quarter, width, kind=BF16)
    blocks = call(
        query_kernel,
        [tile] * lanes,
        [SMEM] + [VMEM] * 5,
        (ids, low, high, back0, back1, q_scale),
        scratch=[pltpu.VMEM((quarter, QL), BF16)],
    )
    gots = [blocks[0]]
    for k in range(1, lanes):
        gots.append(lax.ppermute(blocks[k], (STG, TP), [(i, i ^ k) for i in range(lanes)]))
    q_latent = call(
        place_kernel, shaped(tokens, width, kind=BF16), [SMEM] + [VMEM] * lanes, (ids, *gots)
    )
    return (q_latent, attn.reshape(requests, heads, KVL))


def solution(mesh):
    sizes = dict(mesh.shape)
    pairs = sizes["dec"] == 4 and sizes["grp"] == sizes["stg"] == sizes["tp"] == 2
    return jax.shard_map(
        body_pairs if pairs else body_general,
        mesh=mesh,
        in_specs=(
            P(("grp", "dec"), ("stg", "tp")),
            P(("stg", "tp"), "dec"),
            P(),
            P(),
            P(("grp", "dec"), None, None),
            P(("grp", "dec"), None),
            P(("grp", "dec"), None, None),
            P("grp", "dec"),
            P("grp", ("stg", "tp"), None),
            P("grp", None),
        ),
        out_specs=(P(("grp", "dec"), ("stg", "tp")), P("grp", ("stg", "tp"), None)),
        check_vma=False,
    )
```

```python
import functools

import jax
import jax.numpy as jnp
from jax import lax
from jax.experimental import pallas as pl
from jax.experimental.pallas import tpu as pltpu
from jax.sharding import PartitionSpec as P


QL = 1536
KVL = 512
ROPE = 64
PAGE = 32
KVW = KVL + ROPE
MASKED = -1e30

softmax_scale = 192.0 ** (-0.5)
norm_eps = 1e-06


def combined_all(part, axis, combine):
    gathered = jax.tree.map(lambda a: lax.all_gather(a, axis), part)

    def take(source):
        return jax.tree.map(lambda a: lax.dynamic_index_in_dim(a, source, 0, False), gathered)

    return lax.fori_loop(
        1, lax.axis_size(axis), lambda source, state: combine(state, take(source)), take(0)
    )


def rope_rotate(matrix, col_start, positions):
    col_count = matrix.shape[1]
    columns = col_start + jnp.arange(col_count, dtype=jnp.int32)
    is_rope = columns >= KVL
    pair_index = jnp.maximum(columns - KVL, 0) // 2
    frequency = jnp.power(jnp.float32(10000.0), -(2 * pair_index).astype(jnp.float32) / ROPE)
    angles = positions[:, None] * frequency[None, :]
    cosine = jnp.where(is_rope[None, :], jnp.cos(angles), 1.0)
    sine_part = jnp.where(is_rope[None, :], jnp.sin(angles), 0.0)
    paired = matrix.reshape(matrix.shape[0], col_count // 2, 2)
    partner = jnp.stack([-paired[:, :, 1], paired[:, :, 0]], axis=2).reshape(matrix.shape)
    return matrix * cosine + partner * sine_part


def kv_finish(matrix, col_start, latent_sq, kv_gain, positions):
    col_count = matrix.shape[1]
    columns = col_start + jnp.arange(col_count, dtype=jnp.int32)
    gain_full = jnp.concatenate([kv_gain, jnp.ones((ROPE,), jnp.float32)])
    gain_cols = lax.dynamic_slice_in_dim(gain_full, col_start, col_count)
    inverse = lax.rsqrt(latent_sq / KVL + norm_eps)
    row_scale = jnp.where(columns[None, :] < KVL, inverse[:, None] * gain_cols[None, :], 1.0)
    return rope_rotate(matrix * row_scale, col_start, positions).astype(jnp.bfloat16)


def pack_pages(kv_pages, page_table, owner_count, capacity):
    owners = page_table[:, 0]
    slot_ids = page_table[:, 1]
    page_ids = jnp.arange(kv_pages.shape[0], dtype=jnp.int32)
    earlier = (owners[:, None] == owners[None, :]) & (page_ids[None, :] < page_ids[:, None])
    ranking = jnp.sum(earlier.astype(jnp.int32), axis=1)
    targets = owners * capacity + ranking
    places = jnp.arange(owner_count * capacity, dtype=jnp.int32)
    matches = targets[None, :] == places[:, None]
    source_ids = jnp.sum(jnp.where(matches, page_ids[None, :], 0), axis=1)
    filled = jnp.any(matches, axis=1)
    chosen = jnp.where(
        filled[:, None, None], jnp.take(kv_pages, source_ids, axis=0), jnp.zeros((), kv_pages.dtype)
    )
    labels = jnp.where(filled, jnp.take(slot_ids, source_ids), -1).astype(jnp.bfloat16)
    return (
        chosen.reshape(owner_count, capacity, kv_pages.shape[1], kv_pages.shape[2]),
        labels.reshape(owner_count, capacity),
    )


def place_pages(old_cache, got_pages, got_labels):
    flat_pages = got_pages.reshape(-1, old_cache.shape[1], old_cache.shape[2])
    label_ids = got_labels.reshape(-1).astype(jnp.int32)
    slot_ids = jnp.arange(old_cache.shape[0], dtype=jnp.int32)
    arrival_ids = jnp.arange(label_ids.shape[0], dtype=jnp.int32)
    matches = label_ids[None, :] == slot_ids[:, None]
    source_ids = jnp.sum(jnp.where(matches, arrival_ids[None, :], 0), axis=1)
    arrived = jnp.any(matches, axis=1)
    return jnp.where(arrived[:, None, None], jnp.take(flat_pages, source_ids, axis=0), old_cache)


def combine_parts(former, latter):
    overall = jnp.maximum(former[0], latter[0])
    front_scale = jnp.exp(former[0] - overall)
    back_scale = jnp.exp(latter[0] - overall)
    return (
        overall,
        former[1] * front_scale + latter[1] * back_scale,
        former[2] * front_scale[:, :, None] + latter[2] * back_scale[:, :, None],
    )


def body_general(
    hidden_x,
    proj_weight,
    q_gain,
    kv_gain,
    old_cache,
    page_plan,
    block_table,
    split_lens,
    dec_query,
    new_key,
):
    projected = jnp.dot(
        hidden_x,
        lax.all_gather(proj_weight, "dec", axis=1, tiled=True),
        preferred_element_type=jnp.float32,
    )
    query_part = projected[:, :QL]
    kv_part = projected[:, QL:]
    tokens_here = hidden_x.shape[0]
    positions = (
        lax.axis_index("dec") * tokens_here + jnp.arange(tokens_here, dtype=jnp.int32)
    ).astype(jnp.float32)
    lane_count = lax.axis_size(("stg", "tp"))
    lane_index = lax.axis_index(("stg", "tp"))
    owner_count = lax.axis_size("dec")
    page_count = page_plan.shape[0]
    capacity = max(2, -(-page_count // owner_count))
    query_width = QL // lane_count
    query_cols, kv_cols = (
        lax.psum_scatter(query_part, ("stg", "tp"), scatter_dimension=1, tiled=True),
        lax.psum_scatter(kv_part, ("stg", "tp"), scatter_dimension=1, tiled=True),
    )
    kv_width = kv_cols.shape[1]
    col_start = lane_index * kv_width
    columns = col_start + jnp.arange(kv_width, dtype=jnp.int32)
    latent_part_sq = jnp.sum(jnp.where(columns[None, :] < KVL, kv_cols * kv_cols, 0.0), axis=1)
    query_sq, latent_sq = lax.psum(
        (jnp.sum(query_cols * query_cols, axis=1), latent_part_sq), ("stg", "tp")
    )
    kv_rows = kv_finish(kv_cols, col_start, latent_sq, kv_gain, positions)
    kv_pages = kv_rows.reshape(page_count, PAGE, kv_width)
    send_pages, send_labels = pack_pages(kv_pages, page_plan, owner_count, capacity)
    got_slices, got_labels = (
        lax.all_to_all(send_pages, "dec", split_axis=0, concat_axis=0, tiled=True),
        lax.all_to_all(send_labels, "dec", split_axis=0, concat_axis=0, tiled=True),
    )
    got_pages = lax.all_gather(got_slices, ("stg", "tp"), axis=3, tiled=True)
    query_gain = lax.dynamic_slice_in_dim(q_gain, lane_index * query_width, query_width)
    q_latent = (
        query_cols * lax.rsqrt(query_sq / QL + norm_eps)[:, None] * query_gain[None, :]
    ).astype(jnp.bfloat16)
    cache = place_pages(old_cache, got_pages, got_labels)
    slot_table = block_table[0]
    request_count = slot_table.shape[0]
    key_rows = jnp.take(cache, slot_table.reshape(-1), axis=0).reshape(
        request_count, -1, cache.shape[2]
    )
    scores = (
        jnp.einsum("rhc,rlc->rhl", dec_query, key_rows, preferred_element_type=jnp.float32)
        * softmax_scale
    )
    live_mask = jnp.arange(key_rows.shape[1], dtype=jnp.int32)[None, :] < split_lens[:, 0][:, None]
    scores = jnp.where(live_mask[:, None, :], scores, -1e30)
    row_peak = jnp.max(scores, axis=2)
    weights = jnp.where(live_mask[:, None, :], jnp.exp(scores - row_peak[:, :, None]), 0.0)
    row_total = jnp.sum(weights, axis=2)
    rounded = weights.astype(jnp.bfloat16)
    partial_out = jnp.einsum(
        "rhl,rlc->rhc", rounded, key_rows[:, :, :KVL], preferred_element_type=jnp.float32
    )
    peak_all, total_all, output_all = combined_all(
        (row_peak, row_total, partial_out), "dec", combine_parts
    )
    self_score = (
        jnp.einsum("rhc,rc->rh", dec_query, new_key, preferred_element_type=jnp.float32)
        * softmax_scale
    )
    overall = jnp.maximum(peak_all, self_score)
    carried = jnp.exp(peak_all - overall)
    self_weight = jnp.exp(self_score - overall)
    denom = total_all * carried + self_weight
    numer = output_all * carried[:, :, None] + self_weight[:, :, None] * new_key[
        :, None, :KVL
    ].astype(jnp.float32)
    attn_latent = (numer / denom[:, :, None]).astype(jnp.bfloat16)
    return (q_latent, attn_latent)


VMEM = pl.BlockSpec(memory_space=pltpu.VMEM)
SMEM = pl.BlockSpec(memory_space=pltpu.SMEM)
VMEM_GRANT = 16 * 2**20
VMEM_ALL = 62 * 2**20
GRP, DEC, STG, TP = "grp", "dec", "stg", "tp"
TILE = 256
F32 = jnp.float32
BF16 = jnp.bfloat16


def swap(a, axis):
    return lax.ppermute(a, axis, [(0, 1), (1, 0)])


def dot_t(a, b, **kw):
    return lax.dot_general(a, b, (((1,), (1,)), ((), ())), preferred_element_type=F32, **kw)


def dot_n(a, b, **kw):
    return lax.dot_general(a, b, (((1,), (0,)), ((), ())), preferred_element_type=F32, **kw)


def chosen(outer, own, sent):
    return jnp.where(outer, own, sent)


def halves(ids, x_ref):
    half = x_ref.shape[1] // 2
    here = pl.ds(pl.multiple_of(ids[0] * half, 128), half)
    there = pl.ds(pl.multiple_of((1 - ids[0]) * half, 128), half)
    return here, there


def is_outer(ids):
    return (ids[2] == 0) | (ids[2] == 3)


def put(ids, out, send, keep, start):
    rows = send.shape[0]
    top, bottom = out[:rows], out[rows:]
    at = slice(start, start + out.shape[1])
    send[:, at] = jnp.where(ids[1] == 0, bottom, top)
    keep[:, at] = jnp.where(ids[1] == 0, top, bottom)


def primary(ids, x_ref, own_ref, parts, send, keep):
    here, there = halves(ids, x_ref)
    outer = is_outer(ids)
    start = 0
    for z, y in parts:
        at = slice(start, start + z.shape[0])
        w_here = chosen(outer, own_ref[at, here], z[...])
        w_there = chosen(outer, own_ref[at, there], y[...])
        put(ids, dot_t(x_ref[:, here], w_here) + dot_t(x_ref[:, there], w_there), send, keep, start)
        start += z.shape[0]


def projected(ids, x_ref, w_here, w_there):
    here, there = halves(ids, x_ref)
    return dot_t(x_ref[:, here], w_here) + dot_t(x_ref[:, there], w_there)


def near_kernel(ids, x_ref, own_ref, z0, y0, z1, y1, send, keep):
    primary(ids, x_ref, own_ref, ((z0, y0), (z1, y1)), send, keep)


def far_kernel(keys, ids, x_ref, far_ref, own_ref, z0, y0, z1, y1, bz1, by1, send, keep):
    cols, head = own_ref.shape[0], z0.shape[0]
    full = z1.shape[0] // TILE * TILE
    outer = is_outer(ids)
    here, there = halves(ids, x_ref)
    primary(
        ids, far_ref, own_ref, ((z0, y0), (z1.at[:full, :], y1.at[:full, :])), send, keep
    )
    at, left, own = slice(z1.shape[0] - keys, None), slice(full, None), slice(head + full, None)
    k_here = chosen(outer, z1[at, :], bz1[at, :])
    k_there = chosen(outer, y1[at, :], by1[at, :])
    w_here = jnp.concatenate([chosen(outer, own_ref[own, here], z1[left, :]), k_here], axis=0)
    w_there = jnp.concatenate([chosen(outer, own_ref[own, there], y1[left, :]), k_there], axis=0)
    out = projected(ids, far_ref, w_here, w_there)
    put(ids, out[:, : cols - head - full], send, keep, head + full)
    put(ids, out[:, cols - head - full :], send, keep, cols + keys)
    put(ids, projected(ids, x_ref, k_here, k_there), send, keep, cols)


def rest_kernel(used, ids, x_ref, far_ref, z, y, bz, by, send, keep):
    outer = is_outer(ids)
    w_here = chosen(outer, z[:used, :], bz[:used, :])
    w_there = chosen(outer, y[:used, :], by[:used, :])
    put(ids, projected(ids, x_ref, w_here, w_there), send, keep, 0)
    put(ids, projected(ids, far_ref, w_here, w_there), send, keep, send.shape[1] - used)


def project(kernel, width, args):
    rows, feats = args[1].shape
    shape = jax.ShapeDtypeStruct((rows // 2, width), F32)
    return pl.pallas_call(
        kernel,
        in_specs=[SMEM] + [VMEM] * (len(args) - 1),
        out_specs=[VMEM] * 2,
        out_shape=[shape] * 2,
        cost_estimate=pl.CostEstimate(
            flops=2 * rows * feats * width, bytes_accessed=8 * rows * width, transcendentals=0
        ),
        compiler_params=pltpu.CompilerParams(vmem_limit_bytes=VMEM_GRANT),
    )(*args)


def share_kernel(ids, weight, head, tail, sems):
    split, half = head.shape
    columns = pl.ds(pl.multiple_of(ids[0] * half, 128), half)
    first = pltpu.make_async_copy(weight.at[split:, columns], tail, sems.at[0])
    second = pltpu.make_async_copy(weight.at[:split, columns], head, sems.at[1])
    first.start()
    second.start()
    first.wait()
    second.wait()


def share(ids, weight, split):
    rows, feats = weight.shape
    sizes = (split, rows - split)
    return pl.pallas_call(
        share_kernel,
        in_specs=[SMEM, pl.BlockSpec(memory_space=pltpu.HBM)],
        out_specs=[VMEM] * 2,
        out_shape=[jax.ShapeDtypeStruct((size, feats // 2), weight.dtype) for size in sizes],
        scratch_shapes=[pltpu.SemaphoreType.DMA((2,))],
        compiler_params=pltpu.CompilerParams(vmem_limit_bytes=VMEM_ALL),
    )(ids, weight)


def turn_kernel(out):
    source = lax.broadcasted_iota(jnp.int32, out.shape, 0)
    target = lax.broadcasted_iota(jnp.int32, out.shape, 1)
    down = (source == target + 1) & (target % 2 == 0)
    up = (source + 1 == target) & (target % 2 == 1)
    out[...] = jnp.where(down, -1.0, jnp.where(up, 1.0, 0.0))


def old_kernel(n, pages, ids, tab_ref, query_ref, rows_ref, own_ref, packed_ref, bias_ref):
    index, core = ids[2], ids[1]
    query = query_ref[...]
    keys = rows_ref.shape[0]
    requests = own_ref.shape[0] // 4
    heads = query.shape[0] // requests
    base = 2 * pages
    slots = keys // PAGE
    per = slots // requests

    def iota(rows, cols, axis):
        return lax.broadcasted_iota(jnp.int32, (rows, cols), axis)

    size = tab_ref.shape[1]
    diagonal = iota(size, size, 0) == iota(size, size, 1)
    columns = [
        jnp.sum(jnp.where(diagonal, tab_ref[s : s + 1, :], 0), axis=1, keepdims=True)
        for s in range(n)
    ]
    entry = iota(slots, 1, 0)
    readers = entry // per

    def limits(column):
        lengths = jnp.zeros((slots, 1), jnp.int32)
        for r in range(requests):
            at = base + slots + r
            lengths = jnp.where(readers == r, column[at : at + 1, :], lengths)
        return lengths - PAGE * (entry % per)

    def lookup(hit, values):
        return jnp.sum(jnp.where(hit, values, 0), axis=0, keepdims=True)

    page = iota(1, keys, 1) // PAGE
    hit = columns[0][base : base + slots, :] == page
    limit = lookup(hit, limits(columns[0]))
    reader = lookup(hit, readers)
    is_slot = iota(base, 1, 0) % 2 == 1
    taken = jnp.zeros((1, keys), jnp.int32)
    odd_row = iota(base, base, 0)
    follows = (iota(base, base, 1) == odd_row - 1) & (odd_row % 2 == 1)
    for s in range(n):
        plan = columns[s][:base, :]
        owners = jnp.sum(jnp.where(follows, tab_ref[s : s + 1, :base], 0), axis=1, keepdims=True)
        here = is_slot & (owners == index)
        taken = taken + jnp.sum(jnp.where(here & (plan == page), 1, 0), axis=0, keepdims=True)
    limit = jnp.where(taken > 0, 0, limit)
    live = (iota(1, keys, 1) % PAGE) < limit
    bias = jnp.where(live & (reader == iota(8, keys, 0)), 0.0, MASKED)
    wide = jnp.concatenate(
        [jnp.broadcast_to(bias[r : r + 1], (heads, keys)) for r in range(requests)], axis=0
    )
    scores = dot_t(query, rows_ref[...]) * softmax_scale + wide
    own = dot_t(query, own_ref[...]) * softmax_scale
    mine = iota(*own.shape, 0) // heads == iota(*own.shape, 1)
    own = jnp.sum(jnp.where(mine, own, 0.0), axis=1, keepdims=True)
    own = jnp.where(index == 0, own, MASKED)
    peak = jnp.maximum(jnp.max(scores, axis=1, keepdims=True), own)
    weights = jnp.where(wide < 0.0, 0.0, jnp.exp(scores - peak))
    own_weight = jnp.where(index == 0, jnp.exp(own - peak), 0.0)
    total = jnp.sum(weights, axis=1, keepdims=True) + own_weight
    out = dot_n(weights.astype(BF16), rows_ref[:, :KVL])
    own_rows = own_ref[:, :KVL].astype(F32)
    latent = jnp.concatenate(
        [jnp.broadcast_to(own_rows[r : r + 1], (heads, KVL)) for r in range(requests)], axis=0
    )
    pack((out + own_weight * latent) / total, peak + jnp.log(total), packed_ref)

    width = bias_ref.shape[1]
    half = pages // 2
    spot = iota(1, width, 1) // PAGE
    which = jnp.where(spot // pages == 1, 1 - core, core) * half + spot % half
    partner = (spot % pages) // half == 1
    line = iota(base, width, 0)
    plan = jnp.where(partner, columns[n - 1][:base, :], columns[0][:base, :])
    plan = jnp.where(line % 2 == 1, plan, plan * (2 * slots))
    code = jnp.sum(jnp.where(line // 2 == which, plan, 0), axis=0, keepdims=True)
    limit = jnp.zeros((1, width), jnp.int32)
    reader = jnp.zeros((1, width), jnp.int32)
    for s in range(n):
        owner = (index + s) % n
        hit = columns[s][base : base + slots, :] + owner * (2 * slots) == code
        limit = limit + lookup(hit, limits(columns[s]))
        reader = reader + lookup(hit, readers)
    limit = jnp.where(index % 2 == 1, limit, 0)
    live = (iota(1, width, 1) % PAGE) < limit
    bias_ref[...] = jnp.where(live & (reader == iota(8, width, 0)), 0.0, MASKED)


def parted(ids, block):
    half = block.shape[0] // 2
    odd, stage = ids[2] % 2 == 1, ids[3]
    top, bottom = block[:half], block[half:]
    mine = jnp.where(stage == 0, top, bottom)
    away = jnp.where(stage == 0, bottom, top)
    twice = lambda part: jnp.concatenate([part, part], axis=0)
    return jnp.where(odd, block, twice(mine)), jnp.where(odd, block, twice(away))


def cross_near_kernel(ids, kept, got, send, keep):
    mine, away = parted(ids, kept[...] + got[...])
    keep[...] = mine
    send[...] = away.astype(BF16)


def cross_far_kernel(cols, ids, kept, got, send, keep):
    both = kept[...] + got[...]
    mine, away = parted(ids, both[:, :cols])
    keep[:, :cols] = mine
    keep[:, cols:] = both[:, cols:]
    send[:, :cols] = away.astype(BF16)
    send[:, cols:] = both[:, cols:].astype(BF16)


def cross_rest_kernel(
    head, rest, keys, ids, kept_tail, got_tail, kept_head, got_head, kept_far, got_far, send, keep
):
    cols = send.shape[1]
    stage = ids[3]
    for i in range(2):
        start = i * (kept_head.shape[1] - head)
        at = slice(start, start + head)
        first = kept_head[:, at] + got_head[:, at]
        start = i * (kept_tail.shape[1] - rest)
        at = slice(start, start + rest)
        second = kept_tail[:, at] + got_tail[:, at]
        at = slice(cols + i * keys, cols + (i + 1) * keys)
        block = jnp.concatenate([first, second, kept_far[:, at] + got_far[:, at]], axis=1)
        half = block.shape[0] // 2
        top, bottom = block[:half], block[half:]
        at = slice(i * half, (i + 1) * half)
        keep[at, :] = jnp.where(stage == 0, top, bottom)
        send[at, :] = jnp.where(stage == 0, bottom, top).astype(BF16)


def keys_kernel(keys, keep0, got0, keep1, got1, cos, sin, turn, gain, out):
    rows, cols = keep0.shape
    for i in range(2):
        last = slice(cols + i * keys, cols + (i + 1) * keys)
        tail = keep1[:, last] + got1[:, last].astype(F32)
        if i == 0:
            block = keep0[...] + got0[...].astype(F32)
        else:
            block = keep1[:, :cols] + got1[:, :cols].astype(F32)
        raw = jnp.concatenate([tail, block], axis=1)
        at = slice(i * rows, (i + 1) * rows)
        latent = raw[:, :KVL]
        inverse = lax.rsqrt(jnp.sum(latent * latent, axis=1, keepdims=True) / KVL + norm_eps)
        out[at, :KVL] = (latent * inverse * gain[...]).astype(BF16)
        rope = raw[:, KVL:]
        partner = dot_n(rope, turn[...], precision=lax.Precision.HIGHEST)
        out[at, KVL:] = (rope * cos[at, :] + partner * sin[at, :]).astype(BF16)


def pack(out, level, packed_ref):
    packed_ref[:, :KVL] = out.astype(BF16)
    lead = level.astype(BF16).astype(F32)
    rest = (level - lead).astype(BF16).astype(F32)
    last = level - lead - rest
    lane = lax.broadcasted_iota(jnp.int32, (out.shape[0], 128), 1)
    tail = jnp.where(lane == 0, lead, jnp.where(lane == 1, rest, jnp.where(lane == 2, last, 0.0)))
    packed_ref[:, KVL:] = tail.astype(BF16)


def unpack(packed):
    level = jnp.sum(packed[:, KVL:].astype(F32), axis=1, keepdims=True)
    return packed[:, :KVL].astype(F32), level


def attend_kernel(query_ref, k0_ref, k1_ref, bias_ref, old_ref, far_ref, packed_ref):
    query = query_ref[...]
    keys = k0_ref.shape[0]
    requests = bias_ref.shape[0] // 2
    heads = query.shape[0] // requests
    bias = bias_ref[...]
    wide = jnp.concatenate(
        [jnp.broadcast_to(bias[r : r + 1], (heads, 2 * keys)) for r in range(requests)], axis=0
    )
    scores = jnp.concatenate([dot_t(query, k0_ref[...]), dot_t(query, k1_ref[...])], axis=1)
    scores = scores * softmax_scale + wide
    old, old_level = unpack(old_ref[...])
    far, far_level = unpack(far_ref[...])
    peak = jnp.maximum(old_level, far_level)
    peak = jnp.maximum(peak, jnp.max(scores, axis=1, keepdims=True))
    weights = jnp.where(wide < 0.0, 0.0, jnp.exp(scores - peak))
    old_share, far_share = jnp.exp(old_level - peak), jnp.exp(far_level - peak)
    total = jnp.sum(weights, axis=1, keepdims=True) + old_share + far_share
    rounded = weights.astype(BF16)
    out = dot_n(rounded[:, :keys], k0_ref[:, :KVL]) + dot_n(rounded[:, keys:], k1_ref[:, :KVL])
    out = out + old * old_share + far * far_share
    pack(out / total, peak + jnp.log(total), packed_ref)


def combine_kernel(own, across, out):
    first, level = unpack(own[...])
    second, other_level = unpack(across[...])
    top = jnp.maximum(level, other_level)
    share, other_share = jnp.exp(level - top), jnp.exp(other_level - top)
    out[...] = ((first * share + second * other_share) / (share + other_share)).astype(BF16)


def final_kernel(ids, own, partner, out):
    out[...] = jnp.where(ids[2] % 2 == 1, own[...], partner[...])


def return_first_kernel(keep0, got0, keep1, got1, low, send):
    rows, cols = low.shape
    low[...] = keep0[:rows, :] + got0[:rows, :].astype(F32)
    send[...] = (keep1[:rows, :cols] + got1[:rows, :cols].astype(F32)).astype(BF16)


def return_second_kernel(keep, got, high, send):
    rows = high.shape[0]
    both = keep[...] + got[...].astype(F32)
    high[...] = both[:rows]
    send[...] = both[rows:].astype(BF16)


def query_kernel(ids, low, high, got_first, got_second, gain, *refs):
    sends, scratch = refs[:-1], refs[-1]
    odd = ids[2] % 2 == 1
    cols = low.shape[1]
    cut = QL - 2 * cols
    got_low, got_high = got_first[...].astype(F32), got_second[...].astype(F32)
    first = jnp.where(odd, got_low, low[...])
    second = jnp.where(odd, got_high, high[...])
    third = jnp.where(odd, high[:, :cut], got_high[:, :cut])
    rows = jnp.concatenate([first, second, third], axis=1)
    inverse = lax.rsqrt(jnp.sum(rows * rows, axis=1, keepdims=True) / QL + norm_eps)
    rows = (rows * inverse * gain[...]).astype(BF16)
    scratch[...] = rows
    width = QL // len(sends)
    lane = 2 * ids[3] + ids[1]
    for k, send in enumerate(sends):
        target = jnp.bitwise_xor(lane, k)
        send[...] = scratch[:, pl.ds(pl.multiple_of(target * width, 128), width)]


def place_kernel(ids, *refs):
    gots, out = refs[:-1], refs[-1]
    rows = gots[0].shape[0]
    lane = 2 * ids[3] + ids[1]
    for k, got in enumerate(gots):
        source = jnp.bitwise_xor(lane, k)
        order = 2 * (source % 2) + source // 2
        out[pl.ds(pl.multiple_of(order * rows, 32), rows), :] = got[...]


def call(kernel, shapes, specs, args, scratch=()):
    return pl.pallas_call(
        kernel,
        scratch_shapes=scratch,
        out_shape=shapes,
        in_specs=specs,
        out_specs=[VMEM] * len(shapes) if isinstance(shapes, list) else VMEM,
        cost_estimate=pl.CostEstimate(flops=20_000_000, bytes_accessed=2_000_000, transcendentals=0),
        compiler_params=pltpu.CompilerParams(vmem_limit_bytes=VMEM_GRANT),
    )(*args)


def shaped(*dims, kind=F32):
    return jax.ShapeDtypeStruct(dims, kind)


def body_pairs(*args):
    return pairs_step(*args)


def pairs_step(
    hidden_x,
    proj_weight,
    q_gain,
    kv_gain,
    old_cache,
    page_plan,
    block_table,
    split_lens,
    dec_query,
    new_key,
):
    n = lax.axis_size(DEC)
    group, index = lax.axis_index(GRP), lax.axis_index(DEC)
    stage, core = lax.axis_index(STG), lax.axis_index(TP)
    ids = jnp.stack([group, core, index, stage]).astype(jnp.int32)
    tokens, _ = hidden_x.shape
    cols = proj_weight.shape[1]
    cut = QL - 2 * cols
    pages = page_plan.shape[0]
    requests, heads, _ = dec_query.shape
    queries = requests * heads
    rows = tokens // 2
    quarter = rows // 2

    weight = proj_weight.T
    split = cols // 2 // 128 * 128
    pieces = share(ids, weight, split)
    partners = [(0, 1), (1, 0), (2, 3), (3, 2)]
    a_z, a_y, b_z, b_y = [None] * 2, [None] * 2, [None] * 2, [None] * 2
    for p in (1, 0):
        a_z[p] = lax.ppermute(pieces[p], DEC, [(0, 2), (3, 1), (1, 0), (2, 3)])
    packed = jnp.concatenate(
        [page_plan.reshape(-1), block_table.reshape(-1), split_lens.reshape(-1)]
    ).reshape(1, -1)
    tables = [packed]
    for s in range(1, n):
        tables.append(lax.ppermute(packed, DEC, [((i + s) % n, i) for i in range(n)]))
    tables = jnp.pad(
        jnp.concatenate(tables, axis=0), ((0, 8 - n), (0, -packed.shape[1] % 128))
    )
    x_far = lax.ppermute(hidden_x, DEC, partners)
    held = lax.optimization_barrier((pieces[0], pieces[1], a_z[0]))
    for p in (1, 0):
        a_y[p] = swap(a_z[p], GRP)
        b_z[p] = lax.ppermute(held[p], DEC, [(1, 2), (2, 1)])
    for p in (1, 0):
        b_y[p] = swap(b_z[p], GRP)
    query = dec_query.reshape(queries, KVW)
    padded_key = jnp.pad(new_key, ((0, 3 * requests), (0, 0)))
    old, bias = call(
        functools.partial(old_kernel, n, pages),
        [shaped(queries, KVL + 128, kind=BF16), shaped(8, 2 * tokens)],
        [SMEM, VMEM, VMEM, VMEM, VMEM],
        (ids, tables, query, old_cache.reshape(-1, KVW), padded_key),
    )

    old_far = lax.ppermute(old, DEC, partners)

    partner = index + 1 - 2 * (index % 2)
    place = core * rows + jnp.arange(rows, dtype=jnp.int32)
    positions = jnp.concatenate([index * tokens + place, partner * tokens + place]).astype(F32)
    pair = jnp.arange(ROPE, dtype=jnp.int32) // 2
    frequency = jnp.power(F32(10000.0), -(2 * pair).astype(F32) / ROPE)
    angles = positions[:, None] * frequency[None, :]
    turn = call(turn_kernel, shaped(ROPE, ROPE), [], ())
    early_ids, cos, sin, turn, kv_scale, q_scale = lax.optimization_barrier(
        (ids, jnp.cos(angles), jnp.sin(angles), turn, kv_gain.reshape(1, -1), q_gain.reshape(1, -1))
    )

    a_refs = (a_z[0], a_y[0], a_z[1], a_y[1])
    keys = cols - cut
    send, kept0 = project(near_kernel, cols, (early_ids, hidden_x, weight, *a_refs))
    other0 = swap(send, TP)
    send0, keep0 = call(
        cross_near_kernel,
        [shaped(rows, cols, kind=BF16), shaped(rows, cols)],
        [SMEM, VMEM, VMEM],
        (ids, kept0, other0),
    )
    got0 = swap(send0, STG)
    send, kept1 = project(
        functools.partial(far_kernel, keys),
        cols + 2 * keys,
        (ids, hidden_x, x_far, weight, *a_refs, b_z[1], b_y[1]),
    )
    other1 = swap(send, TP)
    send1, keep1 = call(
        functools.partial(cross_far_kernel, cols),
        [shaped(rows, cols + 2 * keys, kind=BF16), shaped(rows, cols + 2 * keys)],
        [SMEM, VMEM, VMEM],
        (ids, kept1, other1),
    )
    got1 = swap(send1, STG)
    used = (cols - split - keys, split)
    rest = []
    for k, p in enumerate((1, 0)):
        send, kept = project(
            functools.partial(rest_kernel, used[k]),
            -(-used[k] // 128) * 128 + used[k],
            (ids, hidden_x, x_far, a_z[p], a_y[p], b_z[p], b_y[p]),
        )
        rest += [kept, swap(send, TP)]
    send2, keep2 = call(
        functools.partial(cross_rest_kernel, split, used[0], keys),
        [shaped(rows, cols, kind=BF16), shaped(rows, cols)],
        [SMEM] + [VMEM] * 6,
        (ids, *rest, kept1, other1),
    )
    got2 = swap(send2, STG)

    key_rows = call(
        functools.partial(keys_kernel, keys),
        shaped(tokens, KVW, kind=BF16),
        [VMEM] * 8,
        (keep0, got0, keep1, got1, cos, sin, turn, kv_scale),
    )
    far_keys = swap(key_rows, TP)
    part_out = call(
        attend_kernel,
        shaped(queries, KVL + 128, kind=BF16),
        [VMEM] * 6,
        (query, key_rows, far_keys, bias, old, old_far),
    )
    across = lax.ppermute(part_out, DEC, [(1, 3), (3, 1)])
    merged = call(combine_kernel, shaped(queries, KVL, kind=BF16), [VMEM] * 2, (part_out, across))
    given = lax.ppermute(merged, DEC, partners)
    attn = call(
        final_kernel,
        shaped(queries, KVL, kind=BF16),
        [SMEM] + [VMEM] * 2,
        (ids, merged, given),
    )

    low, back0 = call(
        return_first_kernel,
        [shaped(quarter, cols), shaped(quarter, cols, kind=BF16)],
        [VMEM] * 4,
        (keep0, got0, keep1, got1),
    )
    back0 = lax.ppermute(back0, DEC, partners)
    high, back1 = call(
        return_second_kernel,
        [shaped(quarter, cols), shaped(quarter, cols, kind=BF16)],
        [VMEM] * 2,
        (keep2, got2),
    )
    back1 = lax.ppermute(back1, DEC, partners)
    lanes = 4
    width = QL // lanes
    tile = shaped(quarter, width, kind=BF16)
    blocks = call(
        query_kernel,
        [tile] * lanes,
        [SMEM] + [VMEM] * 5,
        (ids, low, high, back0, back1, q_scale),
        scratch=[pltpu.VMEM((quarter, QL), BF16)],
    )
    gots = [blocks[0]]
    for k in range(1, lanes):
        gots.append(lax.ppermute(blocks[k], (STG, TP), [(i, i ^ k) for i in range(lanes)]))
    q_latent = call(
        place_kernel, shaped(tokens, width, kind=BF16), [SMEM] + [VMEM] * lanes, (ids, *gots)
    )
    return (q_latent, attn.reshape(requests, heads, KVL))


def solution(mesh):
    sizes = dict(mesh.shape)
    pairs = sizes["dec"] == 4 and sizes["grp"] == sizes["stg"] == sizes["tp"] == 2
    return jax.shard_map(
        body_pairs if pairs else body_general,
        mesh=mesh,
        in_specs=(
            P(("grp", "dec"), ("stg", "tp")),
            P(("stg", "tp"), "dec"),
            P(),
            P(),
            P(("grp", "dec"), None, None),
            P(("grp", "dec"), None),
            P(("grp", "dec"), None, None),
            P("grp", "dec"),
            P("grp", ("stg", "tp"), None),
            P("grp", None),
        ),
        out_specs=(P(("grp", "dec"), ("stg", "tp")), P("grp", ("stg", "tp"), None)),
        check_vma=False,
    )
```

```python
import functools

import jax
import jax.numpy as jnp
from jax import lax
from jax.experimental import pallas as pl
from jax.experimental.pallas import tpu as pltpu
from jax.sharding import PartitionSpec as P


QL = 1536
KVL = 512
ROPE = 64
PAGE = 32
KVW = KVL + ROPE
MASKED = -1e30

softmax_scale = 192.0 ** (-0.5)
norm_eps = 1e-06


def combined_all(part, axis, combine):
    gathered = jax.tree.map(lambda a: lax.all_gather(a, axis), part)

    def take(source):
        return jax.tree.map(lambda a: lax.dynamic_index_in_dim(a, source, 0, False), gathered)

    return lax.fori_loop(
        1, lax.axis_size(axis), lambda source, state: combine(state, take(source)), take(0)
    )


def rope_rotate(matrix, col_start, positions):
    col_count = matrix.shape[1]
    columns = col_start + jnp.arange(col_count, dtype=jnp.int32)
    is_rope = columns >= KVL
    pair_index = jnp.maximum(columns - KVL, 0) // 2
    frequency = jnp.power(jnp.float32(10000.0), -(2 * pair_index).astype(jnp.float32) / ROPE)
    angles = positions[:, None] * frequency[None, :]
    cosine = jnp.where(is_rope[None, :], jnp.cos(angles), 1.0)
    sine_part = jnp.where(is_rope[None, :], jnp.sin(angles), 0.0)
    paired = matrix.reshape(matrix.shape[0], col_count // 2, 2)
    partner = jnp.stack([-paired[:, :, 1], paired[:, :, 0]], axis=2).reshape(matrix.shape)
    return matrix * cosine + partner * sine_part


def kv_finish(matrix, col_start, latent_sq, kv_gain, positions):
    col_count = matrix.shape[1]
    columns = col_start + jnp.arange(col_count, dtype=jnp.int32)
    gain_full = jnp.concatenate([kv_gain, jnp.ones((ROPE,), jnp.float32)])
    gain_cols = lax.dynamic_slice_in_dim(gain_full, col_start, col_count)
    inverse = lax.rsqrt(latent_sq / KVL + norm_eps)
    row_scale = jnp.where(columns[None, :] < KVL, inverse[:, None] * gain_cols[None, :], 1.0)
    return rope_rotate(matrix * row_scale, col_start, positions).astype(jnp.bfloat16)


def pack_pages(kv_pages, page_table, owner_count, capacity):
    owners = page_table[:, 0]
    slot_ids = page_table[:, 1]
    page_ids = jnp.arange(kv_pages.shape[0], dtype=jnp.int32)
    earlier = (owners[:, None] == owners[None, :]) & (page_ids[None, :] < page_ids[:, None])
    ranking = jnp.sum(earlier.astype(jnp.int32), axis=1)
    targets = owners * capacity + ranking
    places = jnp.arange(owner_count * capacity, dtype=jnp.int32)
    matches = targets[None, :] == places[:, None]
    source_ids = jnp.sum(jnp.where(matches, page_ids[None, :], 0), axis=1)
    filled = jnp.any(matches, axis=1)
    chosen = jnp.where(
        filled[:, None, None], jnp.take(kv_pages, source_ids, axis=0), jnp.zeros((), kv_pages.dtype)
    )
    labels = jnp.where(filled, jnp.take(slot_ids, source_ids), -1).astype(jnp.bfloat16)
    return (
        chosen.reshape(owner_count, capacity, kv_pages.shape[1], kv_pages.shape[2]),
        labels.reshape(owner_count, capacity),
    )


def place_pages(old_cache, got_pages, got_labels):
    flat_pages = got_pages.reshape(-1, old_cache.shape[1], old_cache.shape[2])
    label_ids = got_labels.reshape(-1).astype(jnp.int32)
    slot_ids = jnp.arange(old_cache.shape[0], dtype=jnp.int32)
    arrival_ids = jnp.arange(label_ids.shape[0], dtype=jnp.int32)
    matches = label_ids[None, :] == slot_ids[:, None]
    source_ids = jnp.sum(jnp.where(matches, arrival_ids[None, :], 0), axis=1)
    arrived = jnp.any(matches, axis=1)
    return jnp.where(arrived[:, None, None], jnp.take(flat_pages, source_ids, axis=0), old_cache)


def combine_parts(former, latter):
    overall = jnp.maximum(former[0], latter[0])
    front_scale = jnp.exp(former[0] - overall)
    back_scale = jnp.exp(latter[0] - overall)
    return (
        overall,
        former[1] * front_scale + latter[1] * back_scale,
        former[2] * front_scale[:, :, None] + latter[2] * back_scale[:, :, None],
    )


def body_general(
    hidden_x,
    proj_weight,
    q_gain,
    kv_gain,
    old_cache,
    page_plan,
    block_table,
    split_lens,
    dec_query,
    new_key,
):
    projected = jnp.dot(
        hidden_x,
        lax.all_gather(proj_weight, "dec", axis=1, tiled=True),
        preferred_element_type=jnp.float32,
    )
    query_part = projected[:, :QL]
    kv_part = projected[:, QL:]
    tokens_here = hidden_x.shape[0]
    positions = (
        lax.axis_index("dec") * tokens_here + jnp.arange(tokens_here, dtype=jnp.int32)
    ).astype(jnp.float32)
    lane_count = lax.axis_size(("stg", "tp"))
    lane_index = lax.axis_index(("stg", "tp"))
    owner_count = lax.axis_size("dec")
    page_count = page_plan.shape[0]
    capacity = max(2, -(-page_count // owner_count))
    query_width = QL // lane_count
    query_cols, kv_cols = (
        lax.psum_scatter(query_part, ("stg", "tp"), scatter_dimension=1, tiled=True),
        lax.psum_scatter(kv_part, ("stg", "tp"), scatter_dimension=1, tiled=True),
    )
    kv_width = kv_cols.shape[1]
    col_start = lane_index * kv_width
    columns = col_start + jnp.arange(kv_width, dtype=jnp.int32)
    latent_part_sq = jnp.sum(jnp.where(columns[None, :] < KVL, kv_cols * kv_cols, 0.0), axis=1)
    query_sq, latent_sq = lax.psum(
        (jnp.sum(query_cols * query_cols, axis=1), latent_part_sq), ("stg", "tp")
    )
    kv_rows = kv_finish(kv_cols, col_start, latent_sq, kv_gain, positions)
    kv_pages = kv_rows.reshape(page_count, PAGE, kv_width)
    send_pages, send_labels = pack_pages(kv_pages, page_plan, owner_count, capacity)
    got_slices, got_labels = (
        lax.all_to_all(send_pages, "dec", split_axis=0, concat_axis=0, tiled=True),
        lax.all_to_all(send_labels, "dec", split_axis=0, concat_axis=0, tiled=True),
    )
    got_pages = lax.all_gather(got_slices, ("stg", "tp"), axis=3, tiled=True)
    query_gain = lax.dynamic_slice_in_dim(q_gain, lane_index * query_width, query_width)
    q_latent = (
        query_cols * lax.rsqrt(query_sq / QL + norm_eps)[:, None] * query_gain[None, :]
    ).astype(jnp.bfloat16)
    cache = place_pages(old_cache, got_pages, got_labels)
    slot_table = block_table[0]
    request_count = slot_table.shape[0]
    key_rows = jnp.take(cache, slot_table.reshape(-1), axis=0).reshape(
        request_count, -1, cache.shape[2]
    )
    scores = (
        jnp.einsum("rhc,rlc->rhl", dec_query, key_rows, preferred_element_type=jnp.float32)
        * softmax_scale
    )
    live_mask = jnp.arange(key_rows.shape[1], dtype=jnp.int32)[None, :] < split_lens[:, 0][:, None]
    scores = jnp.where(live_mask[:, None, :], scores, -1e30)
    row_peak = jnp.max(scores, axis=2)
    weights = jnp.where(live_mask[:, None, :], jnp.exp(scores - row_peak[:, :, None]), 0.0)
    row_total = jnp.sum(weights, axis=2)
    rounded = weights.astype(jnp.bfloat16)
    partial_out = jnp.einsum(
        "rhl,rlc->rhc", rounded, key_rows[:, :, :KVL], preferred_element_type=jnp.float32
    )
    peak_all, total_all, output_all = combined_all(
        (row_peak, row_total, partial_out), "dec", combine_parts
    )
    self_score = (
        jnp.einsum("rhc,rc->rh", dec_query, new_key, preferred_element_type=jnp.float32)
        * softmax_scale
    )
    overall = jnp.maximum(peak_all, self_score)
    carried = jnp.exp(peak_all - overall)
    self_weight = jnp.exp(self_score - overall)
    denom = total_all * carried + self_weight
    numer = output_all * carried[:, :, None] + self_weight[:, :, None] * new_key[
        :, None, :KVL
    ].astype(jnp.float32)
    attn_latent = (numer / denom[:, :, None]).astype(jnp.bfloat16)
    return (q_latent, attn_latent)


VMEM = pl.BlockSpec(memory_space=pltpu.VMEM)
SMEM = pl.BlockSpec(memory_space=pltpu.SMEM)
VMEM_GRANT = 16 * 2**20
GRP, DEC, STG, TP = "grp", "dec", "stg", "tp"
TILE = 256
F32 = jnp.float32
BF16 = jnp.bfloat16


def swap(a, axis):
    return lax.ppermute(a, axis, [(0, 1), (1, 0)])


def dot_t(a, b, **kw):
    return lax.dot_general(a, b, (((1,), (1,)), ((), ())), preferred_element_type=F32, **kw)


def dot_n(a, b, **kw):
    return lax.dot_general(a, b, (((1,), (0,)), ((), ())), preferred_element_type=F32, **kw)


def chosen(outer, own, sent):
    return jnp.where(outer, own, sent)


def halves(ids, x_ref):
    half = x_ref.shape[1] // 2
    here = pl.ds(pl.multiple_of(ids[0] * half, 128), half)
    there = pl.ds(pl.multiple_of((1 - ids[0]) * half, 128), half)
    return here, there


def is_outer(ids):
    return (ids[2] == 0) | (ids[2] == 3)


def put(ids, out, send, keep, start):
    rows = send.shape[0]
    top, bottom = out[:rows], out[rows:]
    at = slice(start, start + out.shape[1])
    send[:, at] = jnp.where(ids[1] == 0, bottom, top)
    keep[:, at] = jnp.where(ids[1] == 0, top, bottom)


def primary(ids, x_ref, own_ref, parts, send, keep):
    here, there = halves(ids, x_ref)
    outer = is_outer(ids)
    start = 0
    for z, y in parts:
        at = slice(start, start + z.shape[0])
        w_here = chosen(outer, own_ref[at, here], z[...])
        w_there = chosen(outer, own_ref[at, there], y[...])
        put(ids, dot_t(x_ref[:, here], w_here) + dot_t(x_ref[:, there], w_there), send, keep, start)
        start += z.shape[0]


def projected(ids, x_ref, w_here, w_there):
    here, there = halves(ids, x_ref)
    return dot_t(x_ref[:, here], w_here) + dot_t(x_ref[:, there], w_there)


def near_kernel(ids, x_ref, own_ref, z0, y0, z1, y1, send, keep):
    primary(ids, x_ref, own_ref, ((z0, y0), (z1, y1)), send, keep)


def far_kernel(keys, ids, x_ref, far_ref, own_ref, z0, y0, z1, y1, bz1, by1, send, keep):
    cols, head = own_ref.shape[0], z0.shape[0]
    full = z1.shape[0] // TILE * TILE
    outer = is_outer(ids)
    here, there = halves(ids, x_ref)
    primary(
        ids, far_ref, own_ref, ((z0, y0), (z1.at[:full, :], y1.at[:full, :])), send, keep
    )
    at, left, own = slice(z1.shape[0] - keys, None), slice(full, None), slice(head + full, None)
    k_here = chosen(outer, z1[at, :], bz1[at, :])
    k_there = chosen(outer, y1[at, :], by1[at, :])
    w_here = jnp.concatenate([chosen(outer, own_ref[own, here], z1[left, :]), k_here], axis=0)
    w_there = jnp.concatenate([chosen(outer, own_ref[own, there], y1[left, :]), k_there], axis=0)
    out = projected(ids, far_ref, w_here, w_there)
    put(ids, out[:, : cols - head - full], send, keep, head + full)
    put(ids, out[:, cols - head - full :], send, keep, cols + keys)
    put(ids, projected(ids, x_ref, k_here, k_there), send, keep, cols)


def rest_kernel(used, ids, x_ref, far_ref, z, y, bz, by, send, keep):
    outer = is_outer(ids)
    w_here = chosen(outer, z[:used, :], bz[:used, :])
    w_there = chosen(outer, y[:used, :], by[:used, :])
    put(ids, projected(ids, x_ref, w_here, w_there), send, keep, 0)
    put(ids, projected(ids, far_ref, w_here, w_there), send, keep, send.shape[1] - used)


def project(kernel, width, args):
    rows, feats = args[1].shape
    shape = jax.ShapeDtypeStruct((rows // 2, width), F32)
    return pl.pallas_call(
        kernel,
        in_specs=[SMEM] + [VMEM] * (len(args) - 1),
        out_specs=[VMEM] * 2,
        out_shape=[shape] * 2,
        cost_estimate=pl.CostEstimate(
            flops=2 * rows * feats * width, bytes_accessed=8 * rows * width, transcendentals=0
        ),
        compiler_params=pltpu.CompilerParams(vmem_limit_bytes=VMEM_GRANT),
    )(*args)


def turn_kernel(out):
    source = lax.broadcasted_iota(jnp.int32, out.shape, 0)
    target = lax.broadcasted_iota(jnp.int32, out.shape, 1)
    down = (source == target + 1) & (target % 2 == 0)
    up = (source + 1 == target) & (target % 2 == 1)
    out[...] = jnp.where(down, -1.0, jnp.where(up, 1.0, 0.0))


def old_kernel(n, pages, ids, tab_ref, query_ref, rows_ref, own_ref, packed_ref, bias_ref):
    index, core = ids[2], ids[1]
    query = query_ref[...]
    keys = rows_ref.shape[0]
    requests = own_ref.shape[0] // 4
    heads = query.shape[0] // requests
    base = 2 * pages
    slots = keys // PAGE
    per = slots // requests

    def iota(rows, cols, axis):
        return lax.broadcasted_iota(jnp.int32, (rows, cols), axis)

    size = tab_ref.shape[1]
    diagonal = iota(size, size, 0) == iota(size, size, 1)
    columns = [
        jnp.sum(jnp.where(diagonal, tab_ref[s : s + 1, :], 0), axis=1, keepdims=True)
        for s in range(n)
    ]
    entry = iota(slots, 1, 0)
    readers = entry // per

    def limits(column):
        lengths = jnp.zeros((slots, 1), jnp.int32)
        for r in range(requests):
            at = base + slots + r
            lengths = jnp.where(readers == r, column[at : at + 1, :], lengths)
        return lengths - PAGE * (entry % per)

    def lookup(hit, values):
        return jnp.sum(jnp.where(hit, values, 0), axis=0, keepdims=True)

    page = iota(1, keys, 1) // PAGE
    hit = columns[0][base : base + slots, :] == page
    limit = lookup(hit, limits(columns[0]))
    reader = lookup(hit, readers)
    is_slot = iota(base, 1, 0) % 2 == 1
    taken = jnp.zeros((1, keys), jnp.int32)
    odd_row = iota(base, base, 0)
    follows = (iota(base, base, 1) == odd_row - 1) & (odd_row % 2 == 1)
    for s in range(n):
        plan = columns[s][:base, :]
        owners = jnp.sum(jnp.where(follows, tab_ref[s : s + 1, :base], 0), axis=1, keepdims=True)
        here = is_slot & (owners == index)
        taken = taken + jnp.sum(jnp.where(here & (plan == page), 1, 0), axis=0, keepdims=True)
    limit = jnp.where(taken > 0, 0, limit)
    live = (iota(1, keys, 1) % PAGE) < limit
    bias = jnp.where(live & (reader == iota(8, keys, 0)), 0.0, MASKED)
    wide = jnp.concatenate(
        [jnp.broadcast_to(bias[r : r + 1], (heads, keys)) for r in range(requests)], axis=0
    )
    scores = dot_t(query, rows_ref[...]) * softmax_scale + wide
    own = dot_t(query, own_ref[...]) * softmax_scale
    mine = iota(*own.shape, 0) // heads == iota(*own.shape, 1)
    own = jnp.sum(jnp.where(mine, own, 0.0), axis=1, keepdims=True)
    own = jnp.where(index == 0, own, MASKED)
    peak = jnp.maximum(jnp.max(scores, axis=1, keepdims=True), own)
    weights = jnp.where(wide < 0.0, 0.0, jnp.exp(scores - peak))
    own_weight = jnp.where(index == 0, jnp.exp(own - peak), 0.0)
    total = jnp.sum(weights, axis=1, keepdims=True) + own_weight
    out = dot_n(weights.astype(BF16), rows_ref[:, :KVL])
    own_rows = own_ref[:, :KVL].astype(F32)
    latent = jnp.concatenate(
        [jnp.broadcast_to(own_rows[r : r + 1], (heads, KVL)) for r in range(requests)], axis=0
    )
    pack((out + own_weight * latent) / total, peak + jnp.log(total), packed_ref)

    width = bias_ref.shape[1]
    half = pages // 2
    spot = iota(1, width, 1) // PAGE
    which = jnp.where(spot // pages == 1, 1 - core, core) * half + spot % half
    partner = (spot % pages) // half == 1
    line = iota(base, width, 0)
    plan = jnp.where(partner, columns[n - 1][:base, :], columns[0][:base, :])
    plan = jnp.where(line % 2 == 1, plan, plan * (2 * slots))
    code = jnp.sum(jnp.where(line // 2 == which, plan, 0), axis=0, keepdims=True)
    limit = jnp.zeros((1, width), jnp.int32)
    reader = jnp.zeros((1, width), jnp.int32)
    for s in range(n):
        owner = (index + s) % n
        hit = columns[s][base : base + slots, :] + owner * (2 * slots) == code
        limit = limit + lookup(hit, limits(columns[s]))
        reader = reader + lookup(hit, readers)
    limit = jnp.where(index % 2 == 1, limit, 0)
    live = (iota(1, width, 1) % PAGE) < limit
    bias_ref[...] = jnp.where(live & (reader == iota(8, width, 0)), 0.0, MASKED)


def parted(ids, block):
    half = block.shape[0] // 2
    odd, stage = ids[2] % 2 == 1, ids[3]
    top, bottom = block[:half], block[half:]
    mine = jnp.where(stage == 0, top, bottom)
    away = jnp.where(stage == 0, bottom, top)
    twice = lambda part: jnp.concatenate([part, part], axis=0)
    return jnp.where(odd, block, twice(mine)), jnp.where(odd, block, twice(away))


def cross_near_kernel(ids, kept, got, send, keep):
    mine, away = parted(ids, kept[...] + got[...])
    keep[...] = mine
    send[...] = away


def cross_far_kernel(cols, ids, kept, got, send, keep):
    both = kept[...] + got[...]
    mine, away = parted(ids, both[:, :cols])
    keep[:, :cols] = mine
    keep[:, cols:] = both[:, cols:]
    send[:, :cols] = away
    send[:, cols:] = both[:, cols:]


def cross_rest_kernel(
    head, rest, keys, ids, kept_tail, got_tail, kept_head, got_head, kept_far, got_far, send, keep
):
    cols = send.shape[1]
    stage = ids[3]
    for i in range(2):
        start = i * (kept_head.shape[1] - head)
        at = slice(start, start + head)
        first = kept_head[:, at] + got_head[:, at]
        start = i * (kept_tail.shape[1] - rest)
        at = slice(start, start + rest)
        second = kept_tail[:, at] + got_tail[:, at]
        at = slice(cols + i * keys, cols + (i + 1) * keys)
        block = jnp.concatenate([first, second, kept_far[:, at] + got_far[:, at]], axis=1)
        half = block.shape[0] // 2
        top, bottom = block[:half], block[half:]
        at = slice(i * half, (i + 1) * half)
        keep[at, :] = jnp.where(stage == 0, top, bottom)
        send[at, :] = jnp.where(stage == 0, bottom, top).astype(BF16)


def keys_kernel(keys, keep0, got0, keep1, got1, cos, sin, turn, gain, out):
    rows, cols = keep0.shape
    for i in range(2):
        last = slice(cols + i * keys, cols + (i + 1) * keys)
        tail = keep1[:, last] + got1[:, last]
        if i == 0:
            block = keep0[...] + got0[...]
        else:
            block = keep1[:, :cols] + got1[:, :cols]
        raw = jnp.concatenate([tail, block], axis=1)
        at = slice(i * rows, (i + 1) * rows)
        latent = raw[:, :KVL]
        inverse = lax.rsqrt(jnp.sum(latent * latent, axis=1, keepdims=True) / KVL + norm_eps)
        out[at, :KVL] = (latent * inverse * gain[...]).astype(BF16)
        rope = raw[:, KVL:]
        partner = dot_n(rope, turn[...], precision=lax.Precision.HIGHEST)
        out[at, KVL:] = (rope * cos[at, :] + partner * sin[at, :]).astype(BF16)


def pack(out, level, *packed_refs):
    lead = level.astype(BF16).astype(F32)
    rest = (level - lead).astype(BF16).astype(F32)
    last = level - lead - rest
    lane = lax.broadcasted_iota(jnp.int32, (out.shape[0], 128), 1)
    tail = jnp.where(lane == 0, lead, jnp.where(lane == 1, rest, jnp.where(lane == 2, last, 0.0)))
    for packed_ref in packed_refs:
        packed_ref[:, :KVL] = out.astype(packed_ref.dtype)
        packed_ref[:, KVL:] = tail.astype(packed_ref.dtype)


def unpack(packed):
    level = jnp.sum(packed[:, KVL:].astype(F32), axis=1, keepdims=True)
    return packed[:, :KVL].astype(F32), level


def attend_kernel(query_ref, k0_ref, k1_ref, bias_ref, old_ref, far_ref, own_ref, packed_ref):
    query = query_ref[...]
    keys = k0_ref.shape[0]
    requests = bias_ref.shape[0] // 2
    heads = query.shape[0] // requests
    bias = bias_ref[...]
    wide = jnp.concatenate(
        [jnp.broadcast_to(bias[r : r + 1], (heads, 2 * keys)) for r in range(requests)], axis=0
    )
    scores = jnp.concatenate([dot_t(query, k0_ref[...]), dot_t(query, k1_ref[...])], axis=1)
    scores = scores * softmax_scale + wide
    old, old_level = unpack(old_ref[...])
    far, far_level = unpack(far_ref[...])
    peak = jnp.maximum(old_level, far_level)
    peak = jnp.maximum(peak, jnp.max(scores, axis=1, keepdims=True))
    weights = jnp.where(wide < 0.0, 0.0, jnp.exp(scores - peak))
    old_share, far_share = jnp.exp(old_level - peak), jnp.exp(far_level - peak)
    total = jnp.sum(weights, axis=1, keepdims=True) + old_share + far_share
    rounded = weights.astype(BF16)
    out = dot_n(rounded[:, :keys], k0_ref[:, :KVL]) + dot_n(rounded[:, keys:], k1_ref[:, :KVL])
    out = out + old * old_share + far * far_share
    pack(out / total, peak + jnp.log(total), own_ref, packed_ref)


def combine_kernel(own, across, out):
    first, level = unpack(own[...])
    second, other_level = unpack(across[...])
    top = jnp.maximum(level, other_level)
    share, other_share = jnp.exp(level - top), jnp.exp(other_level - top)
    out[...] = ((first * share + second * other_share) / (share + other_share)).astype(BF16)


def final_kernel(ids, own, partner, out):
    out[...] = jnp.where(ids[2] % 2 == 1, own[...], partner[...])


def return_first_kernel(keep0, got0, keep1, got1, low, send):
    rows, cols = low.shape
    low[...] = keep0[:rows, :] + got0[:rows, :]
    send[...] = (keep1[:rows, :cols] + got1[:rows, :cols]).astype(BF16)


def return_second_kernel(keep, got, high, send):
    rows = high.shape[0]
    both = keep[...] + got[...].astype(F32)
    high[...] = both[:rows]
    send[...] = both[rows:].astype(BF16)


def query_kernel(ids, low, high, got_first, got_second, gain, *refs):
    sends, scratch = refs[:-1], refs[-1]
    odd = ids[2] % 2 == 1
    cols = low.shape[1]
    cut = QL - 2 * cols
    got_low, got_high = got_first[...].astype(F32), got_second[...].astype(F32)
    first = jnp.where(odd, got_low, low[...])
    second = jnp.where(odd, got_high, high[...])
    third = jnp.where(odd, high[:, :cut], got_high[:, :cut])
    rows = jnp.concatenate([first, second, third], axis=1)
    inverse = lax.rsqrt(jnp.sum(rows * rows, axis=1, keepdims=True) / QL + norm_eps)
    rows = (rows * inverse * gain[...]).astype(BF16)
    scratch[...] = rows
    width = QL // len(sends)
    lane = 2 * ids[3] + ids[1]
    for k, send in enumerate(sends):
        target = jnp.bitwise_xor(lane, k)
        send[...] = scratch[:, pl.ds(pl.multiple_of(target * width, 128), width)]


def place_kernel(ids, *refs):
    gots, out = refs[:-1], refs[-1]
    rows = gots[0].shape[0]
    lane = 2 * ids[3] + ids[1]
    for k, got in enumerate(gots):
        source = jnp.bitwise_xor(lane, k)
        order = 2 * (source % 2) + source // 2
        out[pl.ds(pl.multiple_of(order * rows, 32), rows), :] = got[...]


def call(kernel, shapes, specs, args, scratch=()):
    return pl.pallas_call(
        kernel,
        scratch_shapes=scratch,
        out_shape=shapes,
        in_specs=specs,
        out_specs=[VMEM] * len(shapes) if isinstance(shapes, list) else VMEM,
        cost_estimate=pl.CostEstimate(flops=20_000_000, bytes_accessed=2_000_000, transcendentals=0),
        compiler_params=pltpu.CompilerParams(vmem_limit_bytes=VMEM_GRANT),
    )(*args)


def shaped(*dims, kind=F32):
    return jax.ShapeDtypeStruct(dims, kind)


def body_pairs(*args):
    return pairs_step(*args)


def pairs_step(
    hidden_x,
    proj_weight,
    q_gain,
    kv_gain,
    old_cache,
    page_plan,
    block_table,
    split_lens,
    dec_query,
    new_key,
):
    n = lax.axis_size(DEC)
    group, index = lax.axis_index(GRP), lax.axis_index(DEC)
    stage, core = lax.axis_index(STG), lax.axis_index(TP)
    ids = jnp.stack([group, core, index, stage]).astype(jnp.int32)
    tokens, feats = hidden_x.shape
    cols = proj_weight.shape[1]
    cut = QL - 2 * cols
    half = feats // 2
    pages = page_plan.shape[0]
    requests, heads, _ = dec_query.shape
    queries = requests * heads
    rows = tokens // 2
    quarter = rows // 2

    weight = proj_weight.T
    split = cols // 2 // 128 * 128
    pieces = [
        lax.dynamic_slice(weight, (0, group * half), (split, half)),
        lax.dynamic_slice(weight, (split, group * half), (cols - split, half)),
    ]
    partners = [(0, 1), (1, 0), (2, 3), (3, 2)]
    a_z, a_y, b_z, b_y = [None] * 2, [None] * 2, [None] * 2, [None] * 2
    for p in (1, 0):
        a_z[p] = lax.ppermute(pieces[p], DEC, [(0, 2), (3, 1), (1, 0), (2, 3)])
    packed = jnp.concatenate(
        [page_plan.reshape(-1), block_table.reshape(-1), split_lens.reshape(-1)]
    ).reshape(1, -1)
    tables = [packed]
    for s in range(1, n):
        tables.append(lax.ppermute(packed, DEC, [((i + s) % n, i) for i in range(n)]))
    tables = jnp.pad(
        jnp.concatenate(tables, axis=0), ((0, 8 - n), (0, -packed.shape[1] % 128))
    )
    x_far = lax.ppermute(hidden_x, DEC, partners)
    held = lax.optimization_barrier((pieces[0], pieces[1], a_z[0]))
    for p in (1, 0):
        a_y[p] = swap(a_z[p], GRP)
        b_z[p] = lax.ppermute(held[p], DEC, [(1, 2), (2, 1)])
    for p in (1, 0):
        b_y[p] = swap(b_z[p], GRP)
    query = dec_query.reshape(queries, KVW)
    padded_key = jnp.pad(new_key, ((0, 3 * requests), (0, 0)))
    old, bias = call(
        functools.partial(old_kernel, n, pages),
        [shaped(queries, KVL + 128), shaped(8, 2 * tokens)],
        [SMEM, VMEM, VMEM, VMEM, VMEM],
        (ids, tables, query, old_cache.reshape(-1, KVW), padded_key),
    )

    old_far = lax.ppermute(old, DEC, partners)

    partner = index + 1 - 2 * (index % 2)
    place = core * rows + jnp.arange(rows, dtype=jnp.int32)
    positions = jnp.concatenate([index * tokens + place, partner * tokens + place]).astype(F32)
    pair = jnp.arange(ROPE, dtype=jnp.int32) // 2
    frequency = jnp.power(F32(10000.0), -(2 * pair).astype(F32) / ROPE)
    angles = positions[:, None] * frequency[None, :]
    turn = call(turn_kernel, shaped(ROPE, ROPE), [], ())
    early_ids, cos, sin, turn, kv_scale, q_scale = lax.optimization_barrier(
        (ids, jnp.cos(angles), jnp.sin(angles), turn, kv_gain.reshape(1, -1), q_gain.reshape(1, -1))
    )

    a_refs = (a_z[0], a_y[0], a_z[1], a_y[1])
    keys = cols - cut
    send, kept0 = project(near_kernel, cols, (early_ids, hidden_x, weight, *a_refs))
    other0 = swap(send, TP)
    send0, keep0 = call(
        cross_near_kernel,
        [shaped(rows, cols)] * 2,
        [SMEM, VMEM, VMEM],
        (ids, kept0, other0),
    )
    got0 = swap(send0, STG)
    send, kept1 = project(
        functools.partial(far_kernel, keys),
        cols + 2 * keys,
        (ids, hidden_x, x_far, weight, *a_refs, b_z[1], b_y[1]),
    )
    other1 = swap(send, TP)
    send1, keep1 = call(
        functools.partial(cross_far_kernel, cols),
        [shaped(rows, cols + 2 * keys)] * 2,
        [SMEM, VMEM, VMEM],
        (ids, kept1, other1),
    )
    got1 = swap(send1, STG)
    used = (cols - split - keys, split)
    rest = []
    for k, p in enumerate((1, 0)):
        send, kept = project(
            functools.partial(rest_kernel, used[k]),
            -(-used[k] // 128) * 128 + used[k],
            (ids, hidden_x, x_far, a_z[p], a_y[p], b_z[p], b_y[p]),
        )
        rest += [kept, swap(send, TP)]
    send2, keep2 = call(
        functools.partial(cross_rest_kernel, split, used[0], keys),
        [shaped(rows, cols, kind=BF16), shaped(rows, cols)],
        [SMEM] + [VMEM] * 6,
        (ids, *rest, kept1, other1),
    )
    got2 = swap(send2, STG)

    key_rows = call(
        functools.partial(keys_kernel, keys),
        shaped(tokens, KVW, kind=BF16),
        [VMEM] * 8,
        (keep0, got0, keep1, got1, cos, sin, turn, kv_scale),
    )
    far_keys = swap(key_rows, TP)
    own_out, part_out = call(
        attend_kernel,
        [shaped(queries, KVL + 128), shaped(queries, KVL + 128, kind=BF16)],
        [VMEM] * 6,
        (query, key_rows, far_keys, bias, old, old_far),
    )
    across = lax.ppermute(part_out, DEC, [(1, 3), (3, 1)])
    merged = call(combine_kernel, shaped(queries, KVL, kind=BF16), [VMEM] * 2, (own_out, across))
    given = lax.ppermute(merged, DEC, partners)
    attn = call(
        final_kernel,
        shaped(queries, KVL, kind=BF16),
        [SMEM] + [VMEM] * 2,
        (ids, merged, given),
    )

    low, back0 = call(
        return_first_kernel,
        [shaped(quarter, cols), shaped(quarter, cols, kind=BF16)],
        [VMEM] * 4,
        (keep0, got0, keep1, got1),
    )
    back0 = lax.ppermute(back0, DEC, partners)
    high, back1 = call(
        return_second_kernel,
        [shaped(quarter, cols), shaped(quarter, cols, kind=BF16)],
        [VMEM] * 2,
        (keep2, got2),
    )
    back1 = lax.ppermute(back1, DEC, partners)
    lanes = 4
    width = QL // lanes
    tile = shaped(quarter, width, kind=BF16)
    blocks = call(
        query_kernel,
        [tile] * lanes,
        [SMEM] + [VMEM] * 5,
        (ids, low, high, back0, back1, q_scale),
        scratch=[pltpu.VMEM((quarter, QL), BF16)],
    )
    gots = [blocks[0]]
    for k in range(1, lanes):
        gots.append(lax.ppermute(blocks[k], (STG, TP), [(i, i ^ k) for i in range(lanes)]))
    q_latent = call(
        place_kernel, shaped(tokens, width, kind=BF16), [SMEM] + [VMEM] * lanes, (ids, *gots)
    )
    return (q_latent, attn.reshape(requests, heads, KVL))


def solution(mesh):
    sizes = dict(mesh.shape)
    pairs = sizes["dec"] == 4 and sizes["grp"] == sizes["stg"] == sizes["tp"] == 2
    return jax.shard_map(
        body_pairs if pairs else body_general,
        mesh=mesh,
        in_specs=(
            P(("grp", "dec"), ("stg", "tp")),
            P(("stg", "tp"), "dec"),
            P(),
            P(),
            P(("grp", "dec"), None, None),
            P(("grp", "dec"), None),
            P(("grp", "dec"), None, None),
            P("grp", "dec"),
            P("grp", ("stg", "tp"), None),
            P("grp", None),
        ),
        out_specs=(P(("grp", "dec"), ("stg", "tp")), P("grp", ("stg", "tp"), None)),
        check_vma=False,
    )
```

```python
import functools

import jax
import jax.numpy as jnp
from jax import lax
from jax.experimental import pallas as pl
from jax.experimental.pallas import tpu as pltpu
from jax.sharding import PartitionSpec as P


QL = 1536
KVL = 512
ROPE = 64
PAGE = 32
KVW = KVL + ROPE
MASKED = -1e30

softmax_scale = 192.0 ** (-0.5)
norm_eps = 1e-06


def combined_all(part, axis, combine):
    gathered = jax.tree.map(lambda a: lax.all_gather(a, axis), part)

    def take(source):
        return jax.tree.map(lambda a: lax.dynamic_index_in_dim(a, source, 0, False), gathered)

    return lax.fori_loop(
        1, lax.axis_size(axis), lambda source, state: combine(state, take(source)), take(0)
    )


def rope_rotate(matrix, col_start, positions):
    col_count = matrix.shape[1]
    columns = col_start + jnp.arange(col_count, dtype=jnp.int32)
    is_rope = columns >= KVL
    pair_index = jnp.maximum(columns - KVL, 0) // 2
    frequency = jnp.power(jnp.float32(10000.0), -(2 * pair_index).astype(jnp.float32) / ROPE)
    angles = positions[:, None] * frequency[None, :]
    cosine = jnp.where(is_rope[None, :], jnp.cos(angles), 1.0)
    sine_part = jnp.where(is_rope[None, :], jnp.sin(angles), 0.0)
    paired = matrix.reshape(matrix.shape[0], col_count // 2, 2)
    partner = jnp.stack([-paired[:, :, 1], paired[:, :, 0]], axis=2).reshape(matrix.shape)
    return matrix * cosine + partner * sine_part


def kv_finish(matrix, col_start, latent_sq, kv_gain, positions):
    col_count = matrix.shape[1]
    columns = col_start + jnp.arange(col_count, dtype=jnp.int32)
    gain_full = jnp.concatenate([kv_gain, jnp.ones((ROPE,), jnp.float32)])
    gain_cols = lax.dynamic_slice_in_dim(gain_full, col_start, col_count)
    inverse = lax.rsqrt(latent_sq / KVL + norm_eps)
    row_scale = jnp.where(columns[None, :] < KVL, inverse[:, None] * gain_cols[None, :], 1.0)
    return rope_rotate(matrix * row_scale, col_start, positions).astype(jnp.bfloat16)


def pack_pages(kv_pages, page_table, owner_count, capacity):
    owners = page_table[:, 0]
    slot_ids = page_table[:, 1]
    page_ids = jnp.arange(kv_pages.shape[0], dtype=jnp.int32)
    earlier = (owners[:, None] == owners[None, :]) & (page_ids[None, :] < page_ids[:, None])
    ranking = jnp.sum(earlier.astype(jnp.int32), axis=1)
    targets = owners * capacity + ranking
    places = jnp.arange(owner_count * capacity, dtype=jnp.int32)
    matches = targets[None, :] == places[:, None]
    source_ids = jnp.sum(jnp.where(matches, page_ids[None, :], 0), axis=1)
    filled = jnp.any(matches, axis=1)
    chosen = jnp.where(
        filled[:, None, None], jnp.take(kv_pages, source_ids, axis=0), jnp.zeros((), kv_pages.dtype)
    )
    labels = jnp.where(filled, jnp.take(slot_ids, source_ids), -1).astype(jnp.bfloat16)
    return (
        chosen.reshape(owner_count, capacity, kv_pages.shape[1], kv_pages.shape[2]),
        labels.reshape(owner_count, capacity),
    )


def place_pages(old_cache, got_pages, got_labels):
    flat_pages = got_pages.reshape(-1, old_cache.shape[1], old_cache.shape[2])
    label_ids = got_labels.reshape(-1).astype(jnp.int32)
    slot_ids = jnp.arange(old_cache.shape[0], dtype=jnp.int32)
    arrival_ids = jnp.arange(label_ids.shape[0], dtype=jnp.int32)
    matches = label_ids[None, :] == slot_ids[:, None]
    source_ids = jnp.sum(jnp.where(matches, arrival_ids[None, :], 0), axis=1)
    arrived = jnp.any(matches, axis=1)
    return jnp.where(arrived[:, None, None], jnp.take(flat_pages, source_ids, axis=0), old_cache)


def combine_parts(former, latter):
    overall = jnp.maximum(former[0], latter[0])
    front_scale = jnp.exp(former[0] - overall)
    back_scale = jnp.exp(latter[0] - overall)
    return (
        overall,
        former[1] * front_scale + latter[1] * back_scale,
        former[2] * front_scale[:, :, None] + latter[2] * back_scale[:, :, None],
    )


def body_general(
    hidden_x,
    proj_weight,
    q_gain,
    kv_gain,
    old_cache,
    page_plan,
    block_table,
    split_lens,
    dec_query,
    new_key,
):
    projected = jnp.dot(
        hidden_x,
        lax.all_gather(proj_weight, "dec", axis=1, tiled=True),
        preferred_element_type=jnp.float32,
    )
    query_part = projected[:, :QL]
    kv_part = projected[:, QL:]
    tokens_here = hidden_x.shape[0]
    positions = (
        lax.axis_index("dec") * tokens_here + jnp.arange(tokens_here, dtype=jnp.int32)
    ).astype(jnp.float32)
    lane_count = lax.axis_size(("stg", "tp"))
    lane_index = lax.axis_index(("stg", "tp"))
    owner_count = lax.axis_size("dec")
    page_count = page_plan.shape[0]
    capacity = max(2, -(-page_count // owner_count))
    query_width = QL // lane_count
    query_cols, kv_cols = (
        lax.psum_scatter(query_part, ("stg", "tp"), scatter_dimension=1, tiled=True),
        lax.psum_scatter(kv_part, ("stg", "tp"), scatter_dimension=1, tiled=True),
    )
    kv_width = kv_cols.shape[1]
    col_start = lane_index * kv_width
    columns = col_start + jnp.arange(kv_width, dtype=jnp.int32)
    latent_part_sq = jnp.sum(jnp.where(columns[None, :] < KVL, kv_cols * kv_cols, 0.0), axis=1)
    query_sq, latent_sq = lax.psum(
        (jnp.sum(query_cols * query_cols, axis=1), latent_part_sq), ("stg", "tp")
    )
    kv_rows = kv_finish(kv_cols, col_start, latent_sq, kv_gain, positions)
    kv_pages = kv_rows.reshape(page_count, PAGE, kv_width)
    send_pages, send_labels = pack_pages(kv_pages, page_plan, owner_count, capacity)
    got_slices, got_labels = (
        lax.all_to_all(send_pages, "dec", split_axis=0, concat_axis=0, tiled=True),
        lax.all_to_all(send_labels, "dec", split_axis=0, concat_axis=0, tiled=True),
    )
    got_pages = lax.all_gather(got_slices, ("stg", "tp"), axis=3, tiled=True)
    query_gain = lax.dynamic_slice_in_dim(q_gain, lane_index * query_width, query_width)
    q_latent = (
        query_cols * lax.rsqrt(query_sq / QL + norm_eps)[:, None] * query_gain[None, :]
    ).astype(jnp.bfloat16)
    cache = place_pages(old_cache, got_pages, got_labels)
    slot_table = block_table[0]
    request_count = slot_table.shape[0]
    key_rows = jnp.take(cache, slot_table.reshape(-1), axis=0).reshape(
        request_count, -1, cache.shape[2]
    )
    scores = (
        jnp.einsum("rhc,rlc->rhl", dec_query, key_rows, preferred_element_type=jnp.float32)
        * softmax_scale
    )
    live_mask = jnp.arange(key_rows.shape[1], dtype=jnp.int32)[None, :] < split_lens[:, 0][:, None]
    scores = jnp.where(live_mask[:, None, :], scores, -1e30)
    row_peak = jnp.max(scores, axis=2)
    weights = jnp.where(live_mask[:, None, :], jnp.exp(scores - row_peak[:, :, None]), 0.0)
    row_total = jnp.sum(weights, axis=2)
    rounded = weights.astype(jnp.bfloat16)
    partial_out = jnp.einsum(
        "rhl,rlc->rhc", rounded, key_rows[:, :, :KVL], preferred_element_type=jnp.float32
    )
    peak_all, total_all, output_all = combined_all(
        (row_peak, row_total, partial_out), "dec", combine_parts
    )
    self_score = (
        jnp.einsum("rhc,rc->rh", dec_query, new_key, preferred_element_type=jnp.float32)
        * softmax_scale
    )
    overall = jnp.maximum(peak_all, self_score)
    carried = jnp.exp(peak_all - overall)
    self_weight = jnp.exp(self_score - overall)
    denom = total_all * carried + self_weight
    numer = output_all * carried[:, :, None] + self_weight[:, :, None] * new_key[
        :, None, :KVL
    ].astype(jnp.float32)
    attn_latent = (numer / denom[:, :, None]).astype(jnp.bfloat16)
    return (q_latent, attn_latent)


VMEM = pl.BlockSpec(memory_space=pltpu.VMEM)
SMEM = pl.BlockSpec(memory_space=pltpu.SMEM)
VMEM_GRANT = 16 * 2**20
GRP, DEC, STG, TP = "grp", "dec", "stg", "tp"
TILE = 256
F32 = jnp.float32
BF16 = jnp.bfloat16


def swap(a, axis):
    return lax.ppermute(a, axis, [(0, 1), (1, 0)])


def dot_t(a, b, **kw):
    return lax.dot_general(a, b, (((1,), (1,)), ((), ())), preferred_element_type=F32, **kw)


def dot_n(a, b, **kw):
    return lax.dot_general(a, b, (((1,), (0,)), ((), ())), preferred_element_type=F32, **kw)


def chosen(outer, own, sent):
    return jnp.where(outer, own, sent)


def halves(ids, x_ref):
    half = x_ref.shape[1] // 2
    here = pl.ds(pl.multiple_of(ids[0] * half, 128), half)
    there = pl.ds(pl.multiple_of((1 - ids[0]) * half, 128), half)
    return here, there


def is_outer(ids):
    return (ids[2] == 0) | (ids[2] == 3)


def put(ids, out, send, keep, chunk, column):
    part = chunk // 2
    columns = slice(column, column + out.shape[1])
    for c in range(out.shape[0] // chunk):
        top, bottom = out[c * chunk : c * chunk + part], out[c * chunk + part : (c + 1) * chunk]
        at = slice(c * part, (c + 1) * part)
        send[at, columns] = jnp.where(ids[1] == 0, bottom, top)
        keep[at, columns] = jnp.where(ids[1] == 0, top, bottom)


def projected(ids, x_ref, w_here, w_there):
    here, there = halves(ids, x_ref)
    return dot_t(x_ref[:, here], w_here) + dot_t(x_ref[:, there], w_there)


def primary(ids, x_ref, own_ref, parts, send, keep, chunk):
    here, there = halves(ids, x_ref)
    outer = is_outer(ids)
    start = 0
    for z, y in parts:
        at = slice(start, start + z.shape[0])
        w_here = chosen(outer, own_ref[at, here], z[...])
        w_there = chosen(outer, own_ref[at, there], y[...])
        put(ids, projected(ids, x_ref, w_here, w_there), send, keep, chunk, start)
        start += z.shape[0]


def primary_kernel(chunk, ids, x_ref, own_ref, z0, y0, z1, y1, send, keep):
    primary(ids, x_ref, own_ref, ((z0, y0), (z1, y1)), send, keep, chunk)


def last_kernel(chunk, keys, ids, x_ref, far0, far1, own_ref, z0, y0, z1, y1, bz1, by1, send, keep):
    cols, head = own_ref.shape[0], z0.shape[0]
    full = z1.shape[0] // TILE * TILE
    outer = is_outer(ids)
    here, there = halves(ids, x_ref)
    parts = ((z0, y0), (z1.at[:full, :], y1.at[:full, :]))
    primary(ids, far1, own_ref, parts, send, keep, chunk)
    at, left, own = slice(z1.shape[0] - keys, None), slice(full, None), slice(head + full, None)
    k_here = chosen(outer, z1[at, :], bz1[at, :])
    k_there = chosen(outer, y1[at, :], by1[at, :])
    w_here = jnp.concatenate([chosen(outer, own_ref[own, here], z1[left, :]), k_here], axis=0)
    w_there = jnp.concatenate([chosen(outer, own_ref[own, there], y1[left, :]), k_there], axis=0)
    out = projected(ids, far1, w_here, w_there)
    put(ids, out[:, : cols - head - full], send, keep, chunk, head + full)
    put(ids, out[:, cols - head - full :], send, keep, chunk, cols + 3 * keys)
    out = projected(ids, x_ref, k_here, k_there)
    put(ids, out[:chunk], send, keep, chunk, cols)
    put(ids, out[chunk:], send, keep, chunk, cols + keys)
    put(ids, projected(ids, far0, k_here, k_there), send, keep, chunk, cols + 2 * keys)


def rest_kernel(chunk, used, ids, x_ref, far0, far1, z, y, bz, by, send, keep, rows):
    outer = is_outer(ids)
    w_here = chosen(outer, z[:used, :], bz[:used, :])
    w_there = chosen(outer, y[:used, :], by[:used, :])
    put(ids, projected(ids, x_ref, w_here, w_there), send, keep, chunk, 0)
    rows[:chunk, :] = far0[...]
    rows[chunk:, :] = far1[...]
    out = projected(ids, rows, w_here, w_there)
    put(ids, out, send, keep, chunk, send.shape[1] - used)


def project(kernel, rows, width, args, scratch=()):
    feats = args[1].shape[1]
    shape = jax.ShapeDtypeStruct((rows, width), F32)
    return pl.pallas_call(
        kernel,
        in_specs=[SMEM] + [VMEM] * (len(args) - 1),
        out_specs=[VMEM] * 2,
        out_shape=[shape] * 2,
        scratch_shapes=scratch,
        cost_estimate=pl.CostEstimate(
            flops=4 * rows * feats * width, bytes_accessed=8 * rows * width, transcendentals=0
        ),
        compiler_params=pltpu.CompilerParams(vmem_limit_bytes=VMEM_GRANT),
    )(*args)


def turn_kernel(out):
    source = lax.broadcasted_iota(jnp.int32, out.shape, 0)
    target = lax.broadcasted_iota(jnp.int32, out.shape, 1)
    down = (source == target + 1) & (target % 2 == 0)
    up = (source + 1 == target) & (target % 2 == 1)
    out[...] = jnp.where(down, -1.0, jnp.where(up, 1.0, 0.0))


def old_kernel(n, pages, ids, tab_ref, query_ref, rows_ref, own_ref, packed_ref, bias_ref):
    index, core = ids[2], ids[1]
    query = query_ref[...]
    keys = rows_ref.shape[0]
    requests = own_ref.shape[0] // 4
    heads = query.shape[0] // requests
    base = 2 * pages
    slots = keys // PAGE
    per = slots // requests

    def iota(rows, cols, axis):
        return lax.broadcasted_iota(jnp.int32, (rows, cols), axis)

    size = tab_ref.shape[1]
    diagonal = iota(size, size, 0) == iota(size, size, 1)
    columns = [
        jnp.sum(jnp.where(diagonal, tab_ref[s : s + 1, :], 0), axis=1, keepdims=True)
        for s in range(n)
    ]
    entry = iota(slots, 1, 0)
    readers = entry // per

    def limits(column):
        lengths = jnp.zeros((slots, 1), jnp.int32)
        for r in range(requests):
            at = base + slots + r
            lengths = jnp.where(readers == r, column[at : at + 1, :], lengths)
        return lengths - PAGE * (entry % per)

    def lookup(hit, values):
        return jnp.sum(jnp.where(hit, values, 0), axis=0, keepdims=True)

    page = iota(1, keys, 1) // PAGE
    hit = columns[0][base : base + slots, :] == page
    limit = lookup(hit, limits(columns[0]))
    reader = lookup(hit, readers)
    is_slot = iota(base, 1, 0) % 2 == 1
    taken = jnp.zeros((1, keys), jnp.int32)
    odd_row = iota(base, base, 0)
    follows = (iota(base, base, 1) == odd_row - 1) & (odd_row % 2 == 1)
    for s in range(n):
        plan = columns[s][:base, :]
        owners = jnp.sum(jnp.where(follows, tab_ref[s : s + 1, :base], 0), axis=1, keepdims=True)
        here = is_slot & (owners == index)
        taken = taken + jnp.sum(jnp.where(here & (plan == page), 1, 0), axis=0, keepdims=True)
    limit = jnp.where(taken > 0, 0, limit)
    live = (iota(1, keys, 1) % PAGE) < limit
    bias = jnp.where(live & (reader == iota(8, keys, 0)), 0.0, MASKED)
    wide = jnp.concatenate(
        [jnp.broadcast_to(bias[r : r + 1], (heads, keys)) for r in range(requests)], axis=0
    )
    scores = dot_t(query, rows_ref[...]) * softmax_scale + wide
    own = dot_t(query, own_ref[...]) * softmax_scale
    mine = iota(*own.shape, 0) // heads == iota(*own.shape, 1)
    own = jnp.sum(jnp.where(mine, own, 0.0), axis=1, keepdims=True)
    own = jnp.where(index == 0, own, MASKED)
    peak = jnp.maximum(jnp.max(scores, axis=1, keepdims=True), own)
    weights = jnp.where(wide < 0.0, 0.0, jnp.exp(scores - peak))
    own_weight = jnp.where(index == 0, jnp.exp(own - peak), 0.0)
    total = jnp.sum(weights, axis=1, keepdims=True) + own_weight
    out = dot_n(weights.astype(BF16), rows_ref[:, :KVL])
    own_rows = own_ref[:, :KVL].astype(F32)
    latent = jnp.concatenate(
        [jnp.broadcast_to(own_rows[r : r + 1], (heads, KVL)) for r in range(requests)], axis=0
    )
    pack((out + own_weight * latent) / total, peak + jnp.log(total), packed_ref)

    width = bias_ref.shape[1]
    half = pages // 2
    spot = iota(1, width, 1) // PAGE
    place = spot % half
    taker = jnp.where(spot // pages == 1, 1 - core, core)
    which = (place // (half // 2)) * half + taker * (half // 2) + place % (half // 2)
    partner = (spot % pages) // half == 1
    line = iota(base, width, 0)
    plan = jnp.where(partner, columns[n - 1][:base, :], columns[0][:base, :])
    plan = jnp.where(line % 2 == 1, plan, plan * (2 * slots))
    code = jnp.sum(jnp.where(line // 2 == which, plan, 0), axis=0, keepdims=True)
    limit = jnp.zeros((1, width), jnp.int32)
    reader = jnp.zeros((1, width), jnp.int32)
    for s in range(n):
        owner = (index + s) % n
        hit = columns[s][base : base + slots, :] + owner * (2 * slots) == code
        limit = limit + lookup(hit, limits(columns[s]))
        reader = reader + lookup(hit, readers)
    limit = jnp.where(index % 2 == 1, limit, 0)
    live = (iota(1, width, 1) % PAGE) < limit
    bias_ref[...] = jnp.where(live & (reader == iota(8, width, 0)), 0.0, MASKED)


def lane_rows(ids, block):
    half = block.shape[0] // 2
    top, bottom = block[:half], block[half:]
    stage = ids[3]
    return jnp.where(stage == 0, top, bottom), jnp.where(stage == 0, bottom, top)


def cross_kernel(cols, part, ids, kept, got, send, keep):
    odd = ids[2] % 2 == 1
    both = kept[...] + got[...]
    for c in range(both.shape[0] // part):
        at = slice(c * part, (c + 1) * part)
        block = both[at, :cols]
        mine, away = lane_rows(ids, block)
        keep[at, :cols] = jnp.where(odd, block, jnp.concatenate([mine, mine], axis=0))
        send[at, :cols] = jnp.where(odd, block, jnp.concatenate([away, away], axis=0))
    if both.shape[1] > cols:
        keep[:, cols:] = both[:, cols:]
        send[:, cols:] = both[:, cols:]


def cross_rest_kernel(
    head, rest, keys, ids, kept_tail, got_tail, kept_head, got_head, kept_last, got_last, send, keep
):
    cols = send.shape[1]
    part = kept_head.shape[0] // 2
    half = part // 2
    for i in range(4):
        side, c = divmod(i, 2)
        rows = slice(c * part, (c + 1) * part)
        start = side * (kept_head.shape[1] - head)
        at = slice(start, start + head)
        first = kept_head[rows, at] + got_head[rows, at]
        start = side * (kept_tail.shape[1] - rest)
        at = slice(start, start + rest)
        second = kept_tail[rows, at] + got_tail[rows, at]
        at = slice(cols + i * keys, cols + (i + 1) * keys)
        third = kept_last[:, at] + got_last[:, at]
        mine, away = lane_rows(ids, jnp.concatenate([first, second, third], axis=1))
        at = slice(i * half, (i + 1) * half)
        keep[at, :] = mine
        send[at, :] = away.astype(BF16)


def keys_kernel(keys, keep0, got0, keep1, got1, keep2, got2, cos, sin, turn, gain, out):
    cols = keep0.shape[1]
    part = keep1.shape[0]
    for i in range(4):
        last = slice(cols + i * keys, cols + (i + 1) * keys)
        tail = keep2[:, last] + got2[:, last]
        keep, got = ((keep0, got0), (keep0, got0), (keep1, got1), (keep2, got2))[i]
        rows = slice(part, 2 * part) if i == 1 else slice(0, part)
        block = keep[rows, :cols] + got[rows, :cols]
        raw = jnp.concatenate([tail, block], axis=1)
        at = slice(i * part, (i + 1) * part)
        latent = raw[:, :KVL]
        inverse = lax.rsqrt(jnp.sum(latent * latent, axis=1, keepdims=True) / KVL + norm_eps)
        out[at, :KVL] = (latent * inverse * gain[...]).astype(BF16)
        rope = raw[:, KVL:]
        partner = dot_n(rope, turn[...], precision=lax.Precision.HIGHEST)
        out[at, KVL:] = (rope * cos[at, :] + partner * sin[at, :]).astype(BF16)


def pack(out, level, *packed_refs):
    lead = level.astype(BF16).astype(F32)
    rest = (level - lead).astype(BF16).astype(F32)
    last = level - lead - rest
    lane = lax.broadcasted_iota(jnp.int32, (out.shape[0], 128), 1)
    tail = jnp.where(lane == 0, lead, jnp.where(lane == 1, rest, jnp.where(lane == 2, last, 0.0)))
    for packed_ref in packed_refs:
        packed_ref[:, :KVL] = out.astype(packed_ref.dtype)
        packed_ref[:, KVL:] = tail.astype(packed_ref.dtype)


def unpack(packed):
    level = jnp.sum(packed[:, KVL:].astype(F32), axis=1, keepdims=True)
    return packed[:, :KVL].astype(F32), level


def attend_kernel(query_ref, k0_ref, k1_ref, bias_ref, old_ref, far_ref, own_ref, packed_ref):
    query = query_ref[...]
    keys = k0_ref.shape[0]
    requests = bias_ref.shape[0] // 2
    heads = query.shape[0] // requests
    bias = bias_ref[...]
    wide = jnp.concatenate(
        [jnp.broadcast_to(bias[r : r + 1], (heads, 2 * keys)) for r in range(requests)], axis=0
    )
    scores = jnp.concatenate([dot_t(query, k0_ref[...]), dot_t(query, k1_ref[...])], axis=1)
    scores = scores * softmax_scale + wide
    old, old_level = unpack(old_ref[...])
    far, far_level = unpack(far_ref[...])
    peak = jnp.maximum(old_level, far_level)
    peak = jnp.maximum(peak, jnp.max(scores, axis=1, keepdims=True))
    weights = jnp.where(wide < 0.0, 0.0, jnp.exp(scores - peak))
    old_share, far_share = jnp.exp(old_level - peak), jnp.exp(far_level - peak)
    total = jnp.sum(weights, axis=1, keepdims=True) + old_share + far_share
    rounded = weights.astype(BF16)
    out = dot_n(rounded[:, :keys], k0_ref[:, :KVL]) + dot_n(rounded[:, keys:], k1_ref[:, :KVL])
    out = out + old * old_share + far * far_share
    pack(out / total, peak + jnp.log(total), own_ref, packed_ref)


def combine_kernel(own, across, out):
    first, level = unpack(own[...])
    second, other_level = unpack(across[...])
    top = jnp.maximum(level, other_level)
    share, other_share = jnp.exp(level - top), jnp.exp(other_level - top)
    out[...] = ((first * share + second * other_share) / (share + other_share)).astype(BF16)


def return_first_kernel(keep0, got0, keep1, got1, keep2, got2, low, send):
    rows, cols = low.shape
    half = rows // 2
    part = keep1.shape[0]
    for c, (keep, got) in enumerate(((keep1, got1), (keep2, got2))):
        at, near = slice(c * half, (c + 1) * half), slice(c * part, c * part + half)
        low[at, :] = keep0[near, :] + got0[near, :]
        send[at, :] = (keep[:half, :cols] + got[:half, :cols]).astype(BF16)


def return_second_kernel(keep, got, high, send):
    rows = high.shape[0]
    both = keep[...] + got[...].astype(F32)
    high[...] = both[:rows]
    send[...] = both[rows:].astype(BF16)


def query_kernel(ids, low, high, got_first, got_second, gain, *refs):
    sends, scratch = refs[:-1], refs[-1]
    odd = ids[2] % 2 == 1
    cols = low.shape[1]
    cut = QL - 2 * cols
    got_low, got_high = got_first[...].astype(F32), got_second[...].astype(F32)
    first = jnp.where(odd, got_low, low[...])
    second = jnp.where(odd, got_high, high[...])
    third = jnp.where(odd, high[:, :cut], got_high[:, :cut])
    rows = jnp.concatenate([first, second, third], axis=1)
    inverse = lax.rsqrt(jnp.sum(rows * rows, axis=1, keepdims=True) / QL + norm_eps)
    rows = (rows * inverse * gain[...]).astype(BF16)
    scratch[...] = rows
    width = QL // len(sends)
    lane = 2 * ids[3] + ids[1]
    for k, send in enumerate(sends):
        target = jnp.bitwise_xor(lane, k)
        send[...] = scratch[:, pl.ds(pl.multiple_of(target * width, 128), width)]


def place_kernel(ids, *refs):
    gots, out = refs[:-1], refs[-1]
    half = gots[0].shape[0] // 2
    chunk = out.shape[0] // 2
    lane = 2 * ids[3] + ids[1]
    for k, got in enumerate(gots):
        source = jnp.bitwise_xor(lane, k)
        start = (source % 2) * (2 * half) + (source // 2) * half
        for c in range(2):
            at = pl.ds(pl.multiple_of(c * chunk + start, 16), half)
            out[at, :] = got[c * half : (c + 1) * half, :]


def call(kernel, shapes, specs, args, scratch=()):
    return pl.pallas_call(
        kernel,
        scratch_shapes=scratch,
        out_shape=shapes,
        in_specs=specs,
        out_specs=[VMEM] * len(shapes) if isinstance(shapes, list) else VMEM,
        cost_estimate=pl.CostEstimate(flops=20_000_000, bytes_accessed=2_000_000, transcendentals=0),
        compiler_params=pltpu.CompilerParams(vmem_limit_bytes=VMEM_GRANT),
    )(*args)


def shaped(*dims, kind=F32):
    return jax.ShapeDtypeStruct(dims, kind)


def body_pairs(*args):
    return pairs_step(*args)


def pairs_step(
    hidden_x,
    proj_weight,
    q_gain,
    kv_gain,
    old_cache,
    page_plan,
    block_table,
    split_lens,
    dec_query,
    new_key,
):
    n = lax.axis_size(DEC)
    group, index = lax.axis_index(GRP), lax.axis_index(DEC)
    stage, core = lax.axis_index(STG), lax.axis_index(TP)
    ids = jnp.stack([group, core, index, stage]).astype(jnp.int32)
    tokens, feats = hidden_x.shape
    cols = proj_weight.shape[1]
    cut = QL - 2 * cols
    half = feats // 2
    pages = page_plan.shape[0]
    requests, heads, _ = dec_query.shape
    queries = requests * heads
    rows = tokens // 2
    quarter = rows // 2

    weight = proj_weight.T
    split = cols // 2 // 128 * 128
    pieces = [
        lax.dynamic_slice(weight, (0, group * half), (split, half)),
        lax.dynamic_slice(weight, (split, group * half), (cols - split, half)),
    ]
    partners = [(0, 1), (1, 0), (2, 3), (3, 2)]
    a_z, a_y, b_z, b_y = [None] * 2, [None] * 2, [None] * 2, [None] * 2
    for p in (1, 0):
        a_z[p] = lax.ppermute(pieces[p], DEC, [(0, 2), (3, 1), (1, 0), (2, 3)])
    packed = jnp.concatenate(
        [page_plan.reshape(-1), block_table.reshape(-1), split_lens.reshape(-1)]
    ).reshape(1, -1)
    tables = [packed]
    for s in range(1, n):
        tables.append(lax.ppermute(packed, DEC, [((i + s) % n, i) for i in range(n)]))
    tables = jnp.pad(
        jnp.concatenate(tables, axis=0), ((0, 8 - n), (0, -packed.shape[1] % 128))
    )
    x_far = []
    for c in range(2):
        x_far.append(lax.ppermute(hidden_x[c * rows : (c + 1) * rows], DEC, partners))
    held = lax.optimization_barrier((pieces[0], pieces[1], a_z[0]))
    for p in (1, 0):
        a_y[p] = swap(a_z[p], GRP)
        b_z[p] = lax.ppermute(held[p], DEC, [(1, 2), (2, 1)])
    for p in (1, 0):
        b_y[p] = swap(b_z[p], GRP)
    query = dec_query.reshape(queries, KVW)
    padded_key = jnp.pad(new_key, ((0, 3 * requests), (0, 0)))
    old, bias = call(
        functools.partial(old_kernel, n, pages),
        [shaped(queries, KVL + 128), shaped(8, 2 * tokens)],
        [SMEM, VMEM, VMEM, VMEM, VMEM],
        (ids, tables, query, old_cache.reshape(-1, KVW), padded_key),
    )

    old_far = lax.ppermute(old, DEC, partners)

    partner = index + 1 - 2 * (index % 2)
    place = jnp.arange(rows, dtype=jnp.int32)
    place = place + core * quarter + (place // quarter) * quarter
    positions = jnp.concatenate([index * tokens + place, partner * tokens + place]).astype(F32)
    pair = jnp.arange(ROPE, dtype=jnp.int32) // 2
    frequency = jnp.power(F32(10000.0), -(2 * pair).astype(F32) / ROPE)
    angles = positions[:, None] * frequency[None, :]
    turn = call(turn_kernel, shaped(ROPE, ROPE), [], ())
    early_ids, cos, sin, turn, kv_scale, q_scale = lax.optimization_barrier(
        (ids, jnp.cos(angles), jnp.sin(angles), turn, kv_gain.reshape(1, -1), q_gain.reshape(1, -1))
    )

    a_refs = (a_z[0], a_y[0], a_z[1], a_y[1])
    keys = cols - cut

    def crossed(kernel, count, width, args):
        send, kept = project(kernel, count, width, args)
        other = swap(send, TP)
        send, keep = call(
            functools.partial(cross_kernel, cols, quarter),
            [shaped(count, width)] * 2,
            [SMEM, VMEM, VMEM],
            (ids, kept, other),
        )
        return (keep, swap(send, STG)), (kept, other)

    near, _ = crossed(
        functools.partial(primary_kernel, rows), rows, cols, (early_ids, hidden_x, weight, *a_refs)
    )
    far, _ = crossed(
        functools.partial(primary_kernel, rows), quarter, cols, (ids, x_far[0], weight, *a_refs)
    )
    last, last_sums = crossed(
        functools.partial(last_kernel, rows, keys),
        quarter,
        cols + 4 * keys,
        (ids, hidden_x, *x_far, weight, *a_refs, b_z[1], b_y[1]),
    )
    used = (cols - split - keys, split)
    rest = []
    for k, p in enumerate((1, 0)):
        send, kept = project(
            functools.partial(rest_kernel, rows, used[k]),
            rows,
            -(-used[k] // 128) * 128 + used[k],
            (ids, hidden_x, *x_far, a_z[p], a_y[p], b_z[p], b_y[p]),
            scratch=[pltpu.VMEM((tokens, feats), BF16)],
        )
        rest += [kept, swap(send, TP)]
    send2, keep2 = call(
        functools.partial(cross_rest_kernel, split, used[0], keys),
        [shaped(rows, cols, kind=BF16), shaped(rows, cols)],
        [SMEM] + [VMEM] * 6,
        (ids, *rest, *last_sums),
    )
    got2 = swap(send2, STG)

    key_rows = call(
        functools.partial(keys_kernel, keys),
        shaped(tokens, KVW, kind=BF16),
        [VMEM] * 10,
        (*near, *far, *last, cos, sin, turn, kv_scale),
    )
    far_keys = swap(key_rows, TP)
    own_out, part_out = call(
        attend_kernel,
        [shaped(queries, KVL + 128), shaped(queries, KVL + 128, kind=BF16)],
        [VMEM] * 6,
        (query, key_rows, far_keys, bias, old, old_far),
    )
    across = lax.ppermute(part_out, DEC, [(1, 3), (3, 1)])
    merged = call(combine_kernel, shaped(queries, KVL, kind=BF16), [VMEM] * 2, (own_out, across))
    given = lax.ppermute(merged, DEC, partners)
    attn = jnp.where(index % 2 == 1, merged, given)

    low, back0 = call(
        return_first_kernel,
        [shaped(quarter, cols), shaped(quarter, cols, kind=BF16)],
        [VMEM] * 6,
        (*near, *far, *last),
    )
    back0 = lax.ppermute(back0, DEC, partners)
    high, back1 = call(
        return_second_kernel,
        [shaped(quarter, cols), shaped(quarter, cols, kind=BF16)],
        [VMEM] * 2,
        (keep2, got2),
    )
    back1 = lax.ppermute(back1, DEC, partners)
    lanes = 4
    width = QL // lanes
    tile = shaped(quarter, width, kind=BF16)
    blocks = call(
        query_kernel,
        [tile] * lanes,
        [SMEM] + [VMEM] * 5,
        (ids, low, high, back0, back1, q_scale),
        scratch=[pltpu.VMEM((quarter, QL), BF16)],
    )
    gots = [blocks[0]]
    for k in range(1, lanes):
        gots.append(lax.ppermute(blocks[k], (STG, TP), [(i, i ^ k) for i in range(lanes)]))
    q_latent = call(
        place_kernel, shaped(tokens, width, kind=BF16), [SMEM] + [VMEM] * lanes, (ids, *gots)
    )
    return (q_latent, attn.reshape(requests, heads, KVL))


def solution(mesh):
    sizes = dict(mesh.shape)
    pairs = sizes["dec"] == 4 and sizes["grp"] == sizes["stg"] == sizes["tp"] == 2
    return jax.shard_map(
        body_pairs if pairs else body_general,
        mesh=mesh,
        in_specs=(
            P(("grp", "dec"), ("stg", "tp")),
            P(("stg", "tp"), "dec"),
            P(),
            P(),
            P(("grp", "dec"), None, None),
            P(("grp", "dec"), None),
            P(("grp", "dec"), None, None),
            P("grp", "dec"),
            P("grp", ("stg", "tp"), None),
            P("grp", None),
        ),
        out_specs=(P(("grp", "dec"), ("stg", "tp")), P("grp", ("stg", "tp"), None)),
        check_vma=False,
    )
```

```python
import functools

import jax
import jax.numpy as jnp
from jax import lax
from jax.experimental import pallas as pl
from jax.experimental.pallas import tpu as pltpu
from jax.sharding import PartitionSpec as P


QL = 1536
KVL = 512
ROPE = 64
PAGE = 32
KVW = KVL + ROPE
MASKED = -1e30

softmax_scale = 192.0 ** (-0.5)
norm_eps = 1e-06


def combined_all(part, axis, combine):
    gathered = jax.tree.map(lambda a: lax.all_gather(a, axis), part)

    def take(source):
        return jax.tree.map(lambda a: lax.dynamic_index_in_dim(a, source, 0, False), gathered)

    return lax.fori_loop(
        1, lax.axis_size(axis), lambda source, state: combine(state, take(source)), take(0)
    )


def rope_rotate(matrix, col_start, positions):
    col_count = matrix.shape[1]
    columns = col_start + jnp.arange(col_count, dtype=jnp.int32)
    is_rope = columns >= KVL
    pair_index = jnp.maximum(columns - KVL, 0) // 2
    frequency = jnp.power(jnp.float32(10000.0), -(2 * pair_index).astype(jnp.float32) / ROPE)
    angles = positions[:, None] * frequency[None, :]
    cosine = jnp.where(is_rope[None, :], jnp.cos(angles), 1.0)
    sine_part = jnp.where(is_rope[None, :], jnp.sin(angles), 0.0)
    paired = matrix.reshape(matrix.shape[0], col_count // 2, 2)
    partner = jnp.stack([-paired[:, :, 1], paired[:, :, 0]], axis=2).reshape(matrix.shape)
    return matrix * cosine + partner * sine_part


def kv_finish(matrix, col_start, latent_sq, kv_gain, positions):
    col_count = matrix.shape[1]
    columns = col_start + jnp.arange(col_count, dtype=jnp.int32)
    gain_full = jnp.concatenate([kv_gain, jnp.ones((ROPE,), jnp.float32)])
    gain_cols = lax.dynamic_slice_in_dim(gain_full, col_start, col_count)
    inverse = lax.rsqrt(latent_sq / KVL + norm_eps)
    row_scale = jnp.where(columns[None, :] < KVL, inverse[:, None] * gain_cols[None, :], 1.0)
    return rope_rotate(matrix * row_scale, col_start, positions).astype(jnp.bfloat16)


def pack_pages(kv_pages, page_table, owner_count, capacity):
    owners = page_table[:, 0]
    slot_ids = page_table[:, 1]
    page_ids = jnp.arange(kv_pages.shape[0], dtype=jnp.int32)
    earlier = (owners[:, None] == owners[None, :]) & (page_ids[None, :] < page_ids[:, None])
    ranking = jnp.sum(earlier.astype(jnp.int32), axis=1)
    targets = owners * capacity + ranking
    places = jnp.arange(owner_count * capacity, dtype=jnp.int32)
    matches = targets[None, :] == places[:, None]
    source_ids = jnp.sum(jnp.where(matches, page_ids[None, :], 0), axis=1)
    filled = jnp.any(matches, axis=1)
    chosen = jnp.where(
        filled[:, None, None], jnp.take(kv_pages, source_ids, axis=0), jnp.zeros((), kv_pages.dtype)
    )
    labels = jnp.where(filled, jnp.take(slot_ids, source_ids), -1).astype(jnp.bfloat16)
    return (
        chosen.reshape(owner_count, capacity, kv_pages.shape[1], kv_pages.shape[2]),
        labels.reshape(owner_count, capacity),
    )


def place_pages(old_cache, got_pages, got_labels):
    flat_pages = got_pages.reshape(-1, old_cache.shape[1], old_cache.shape[2])
    label_ids = got_labels.reshape(-1).astype(jnp.int32)
    slot_ids = jnp.arange(old_cache.shape[0], dtype=jnp.int32)
    arrival_ids = jnp.arange(label_ids.shape[0], dtype=jnp.int32)
    matches = label_ids[None, :] == slot_ids[:, None]
    source_ids = jnp.sum(jnp.where(matches, arrival_ids[None, :], 0), axis=1)
    arrived = jnp.any(matches, axis=1)
    return jnp.where(arrived[:, None, None], jnp.take(flat_pages, source_ids, axis=0), old_cache)


def combine_parts(former, latter):
    overall = jnp.maximum(former[0], latter[0])
    front_scale = jnp.exp(former[0] - overall)
    back_scale = jnp.exp(latter[0] - overall)
    return (
        overall,
        former[1] * front_scale + latter[1] * back_scale,
        former[2] * front_scale[:, :, None] + latter[2] * back_scale[:, :, None],
    )


def body_general(
    hidden_x,
    proj_weight,
    q_gain,
    kv_gain,
    old_cache,
    page_plan,
    block_table,
    split_lens,
    dec_query,
    new_key,
):
    projected = jnp.dot(
        hidden_x,
        lax.all_gather(proj_weight, "dec", axis=1, tiled=True),
        preferred_element_type=jnp.float32,
    )
    query_part = projected[:, :QL]
    kv_part = projected[:, QL:]
    tokens_here = hidden_x.shape[0]
    positions = (
        lax.axis_index("dec") * tokens_here + jnp.arange(tokens_here, dtype=jnp.int32)
    ).astype(jnp.float32)
    lane_count = lax.axis_size(("stg", "tp"))
    lane_index = lax.axis_index(("stg", "tp"))
    owner_count = lax.axis_size("dec")
    page_count = page_plan.shape[0]
    capacity = max(2, -(-page_count // owner_count))
    query_width = QL // lane_count
    query_cols, kv_cols = (
        lax.psum_scatter(query_part, ("stg", "tp"), scatter_dimension=1, tiled=True),
        lax.psum_scatter(kv_part, ("stg", "tp"), scatter_dimension=1, tiled=True),
    )
    kv_width = kv_cols.shape[1]
    col_start = lane_index * kv_width
    columns = col_start + jnp.arange(kv_width, dtype=jnp.int32)
    latent_part_sq = jnp.sum(jnp.where(columns[None, :] < KVL, kv_cols * kv_cols, 0.0), axis=1)
    query_sq, latent_sq = lax.psum(
        (jnp.sum(query_cols * query_cols, axis=1), latent_part_sq), ("stg", "tp")
    )
    kv_rows = kv_finish(kv_cols, col_start, latent_sq, kv_gain, positions)
    kv_pages = kv_rows.reshape(page_count, PAGE, kv_width)
    send_pages, send_labels = pack_pages(kv_pages, page_plan, owner_count, capacity)
    got_slices, got_labels = (
        lax.all_to_all(send_pages, "dec", split_axis=0, concat_axis=0, tiled=True),
        lax.all_to_all(send_labels, "dec", split_axis=0, concat_axis=0, tiled=True),
    )
    got_pages = lax.all_gather(got_slices, ("stg", "tp"), axis=3, tiled=True)
    query_gain = lax.dynamic_slice_in_dim(q_gain, lane_index * query_width, query_width)
    q_latent = (
        query_cols * lax.rsqrt(query_sq / QL + norm_eps)[:, None] * query_gain[None, :]
    ).astype(jnp.bfloat16)
    cache = place_pages(old_cache, got_pages, got_labels)
    slot_table = block_table[0]
    request_count = slot_table.shape[0]
    key_rows = jnp.take(cache, slot_table.reshape(-1), axis=0).reshape(
        request_count, -1, cache.shape[2]
    )
    scores = (
        jnp.einsum("rhc,rlc->rhl", dec_query, key_rows, preferred_element_type=jnp.float32)
        * softmax_scale
    )
    live_mask = jnp.arange(key_rows.shape[1], dtype=jnp.int32)[None, :] < split_lens[:, 0][:, None]
    scores = jnp.where(live_mask[:, None, :], scores, -1e30)
    row_peak = jnp.max(scores, axis=2)
    weights = jnp.where(live_mask[:, None, :], jnp.exp(scores - row_peak[:, :, None]), 0.0)
    row_total = jnp.sum(weights, axis=2)
    rounded = weights.astype(jnp.bfloat16)
    partial_out = jnp.einsum(
        "rhl,rlc->rhc", rounded, key_rows[:, :, :KVL], preferred_element_type=jnp.float32
    )
    peak_all, total_all, output_all = combined_all(
        (row_peak, row_total, partial_out), "dec", combine_parts
    )
    self_score = (
        jnp.einsum("rhc,rc->rh", dec_query, new_key, preferred_element_type=jnp.float32)
        * softmax_scale
    )
    overall = jnp.maximum(peak_all, self_score)
    carried = jnp.exp(peak_all - overall)
    self_weight = jnp.exp(self_score - overall)
    denom = total_all * carried + self_weight
    numer = output_all * carried[:, :, None] + self_weight[:, :, None] * new_key[
        :, None, :KVL
    ].astype(jnp.float32)
    attn_latent = (numer / denom[:, :, None]).astype(jnp.bfloat16)
    return (q_latent, attn_latent)


VMEM = pl.BlockSpec(memory_space=pltpu.VMEM)
SMEM = pl.BlockSpec(memory_space=pltpu.SMEM)
VMEM_GRANT = 16 * 2**20
GRP, DEC, STG, TP = "grp", "dec", "stg", "tp"
TILE = 256
F32 = jnp.float32
BF16 = jnp.bfloat16


def swap(a, axis):
    return lax.ppermute(a, axis, [(0, 1), (1, 0)])


def dot_t(a, b, **kw):
    return lax.dot_general(a, b, (((1,), (1,)), ((), ())), preferred_element_type=F32, **kw)


def dot_n(a, b, **kw):
    return lax.dot_general(a, b, (((1,), (0,)), ((), ())), preferred_element_type=F32, **kw)


def chosen(outer, own, sent):
    return jnp.where(outer, own, sent)


def halves(ids, x_ref):
    half = x_ref.shape[1] // 2
    here = pl.ds(pl.multiple_of(ids[0] * half, 128), half)
    there = pl.ds(pl.multiple_of((1 - ids[0]) * half, 128), half)
    return here, there


def is_outer(ids):
    return (ids[2] == 0) | (ids[2] == 3)


def put(ids, out, send, keep, chunk, column):
    part = chunk // 2
    columns = slice(column, column + out.shape[1])
    for c in range(out.shape[0] // chunk):
        top, bottom = out[c * chunk : c * chunk + part], out[c * chunk + part : (c + 1) * chunk]
        at = slice(c * part, (c + 1) * part)
        send[at, columns] = jnp.where(ids[1] == 0, bottom, top)
        keep[at, columns] = jnp.where(ids[1] == 0, top, bottom)


def projected(ids, x_ref, w_here, w_there):
    here, there = halves(ids, x_ref)
    return dot_t(x_ref[:, here], w_here) + dot_t(x_ref[:, there], w_there)


def primary(ids, x_ref, own_ref, parts, send, keep, chunk):
    here, there = halves(ids, x_ref)
    outer = is_outer(ids)
    start = 0
    for z, y in parts:
        at = slice(start, start + z.shape[0])
        w_here = chosen(outer, own_ref[at, here], z[...])
        w_there = chosen(outer, own_ref[at, there], y[...])
        put(ids, projected(ids, x_ref, w_here, w_there), send, keep, chunk, start)
        start += z.shape[0]


def primary_kernel(chunk, ids, x_ref, own_ref, z0, y0, z1, y1, send, keep):
    primary(ids, x_ref, own_ref, ((z0, y0), (z1, y1)), send, keep, chunk)


def last_kernel(chunk, keys, ids, x_ref, far0, far1, own_ref, z0, y0, z1, y1, bz1, by1, send, keep):
    cols, head = own_ref.shape[0], z0.shape[0]
    full = z1.shape[0] // TILE * TILE
    outer = is_outer(ids)
    here, there = halves(ids, x_ref)
    parts = ((z0, y0), (z1.at[:full, :], y1.at[:full, :]))
    primary(ids, far1, own_ref, parts, send, keep, chunk)
    at, left, own = slice(z1.shape[0] - keys, None), slice(full, None), slice(head + full, None)
    own_keys = slice(bz1.shape[0] - keys, None)
    k_here = chosen(outer, z1[at, :], bz1[own_keys, :])
    k_there = chosen(outer, y1[at, :], by1[own_keys, :])
    w_here = jnp.concatenate([chosen(outer, own_ref[own, here], z1[left, :]), k_here], axis=0)
    w_there = jnp.concatenate([chosen(outer, own_ref[own, there], y1[left, :]), k_there], axis=0)
    out = projected(ids, far1, w_here, w_there)
    put(ids, out[:, : cols - head - full], send, keep, chunk, head + full)
    put(ids, out[:, cols - head - full :], send, keep, chunk, cols + 3 * keys)
    out = projected(ids, x_ref, k_here, k_there)
    put(ids, out[:chunk], send, keep, chunk, cols)
    put(ids, out[chunk:], send, keep, chunk, cols + keys)
    put(ids, projected(ids, far0, k_here, k_there), send, keep, chunk, cols + 2 * keys)


def rest_kernel(chunk, used, ids, x_ref, far0, far1, z, y, *refs):
    pieces, (send, keep, rows) = refs[:-3], refs[-3:]
    outer = is_outer(ids)
    bz = jnp.concatenate([piece[...] for piece in pieces[0::2]], axis=0)
    by = jnp.concatenate([piece[...] for piece in pieces[1::2]], axis=0)
    w_here = chosen(outer, z[:used, :], bz[:used, :])
    w_there = chosen(outer, y[:used, :], by[:used, :])
    put(ids, projected(ids, x_ref, w_here, w_there), send, keep, chunk, 0)
    rows[:chunk, :] = far0[...]
    rows[chunk:, :] = far1[...]
    out = projected(ids, rows, w_here, w_there)
    put(ids, out, send, keep, chunk, send.shape[1] - used)


def project(kernel, rows, width, args, scratch=()):
    feats = args[1].shape[1]
    shape = jax.ShapeDtypeStruct((rows, width), F32)
    return pl.pallas_call(
        kernel,
        in_specs=[SMEM] + [VMEM] * (len(args) - 1),
        out_specs=[VMEM] * 2,
        out_shape=[shape] * 2,
        scratch_shapes=scratch,
        cost_estimate=pl.CostEstimate(
            flops=4 * rows * feats * width, bytes_accessed=8 * rows * width, transcendentals=0
        ),
        compiler_params=pltpu.CompilerParams(vmem_limit_bytes=VMEM_GRANT),
    )(*args)


def turn_kernel(out):
    source = lax.broadcasted_iota(jnp.int32, out.shape, 0)
    target = lax.broadcasted_iota(jnp.int32, out.shape, 1)
    down = (source == target + 1) & (target % 2 == 0)
    up = (source + 1 == target) & (target % 2 == 1)
    out[...] = jnp.where(down, -1.0, jnp.where(up, 1.0, 0.0))


def old_kernel(n, pages, ids, tab_ref, query_ref, rows_ref, own_ref, packed_ref, bias_ref):
    index, core = ids[2], ids[1]
    query = query_ref[...]
    keys = rows_ref.shape[0]
    requests = own_ref.shape[0] // 4
    heads = query.shape[0] // requests
    base = 2 * pages
    slots = keys // PAGE
    per = slots // requests

    def iota(rows, cols, axis):
        return lax.broadcasted_iota(jnp.int32, (rows, cols), axis)

    size = tab_ref.shape[1]
    diagonal = iota(size, size, 0) == iota(size, size, 1)
    columns = [
        jnp.sum(jnp.where(diagonal, tab_ref[s : s + 1, :], 0), axis=1, keepdims=True)
        for s in range(n)
    ]
    entry = iota(slots, 1, 0)
    readers = entry // per

    def limits(column):
        lengths = jnp.zeros((slots, 1), jnp.int32)
        for r in range(requests):
            at = base + slots + r
            lengths = jnp.where(readers == r, column[at : at + 1, :], lengths)
        return lengths - PAGE * (entry % per)

    def lookup(hit, values):
        return jnp.sum(jnp.where(hit, values, 0), axis=0, keepdims=True)

    page = iota(1, keys, 1) // PAGE
    hit = columns[0][base : base + slots, :] == page
    limit = lookup(hit, limits(columns[0]))
    reader = lookup(hit, readers)
    is_slot = iota(base, 1, 0) % 2 == 1
    taken = jnp.zeros((1, keys), jnp.int32)
    odd_row = iota(base, base, 0)
    follows = (iota(base, base, 1) == odd_row - 1) & (odd_row % 2 == 1)
    for s in range(n):
        plan = columns[s][:base, :]
        owners = jnp.sum(jnp.where(follows, tab_ref[s : s + 1, :base], 0), axis=1, keepdims=True)
        here = is_slot & (owners == index)
        taken = taken + jnp.sum(jnp.where(here & (plan == page), 1, 0), axis=0, keepdims=True)
    limit = jnp.where(taken > 0, 0, limit)
    live = (iota(1, keys, 1) % PAGE) < limit
    bias = jnp.where(live & (reader == iota(8, keys, 0)), 0.0, MASKED)
    wide = jnp.concatenate(
        [jnp.broadcast_to(bias[r : r + 1], (heads, keys)) for r in range(requests)], axis=0
    )
    scores = dot_t(query, rows_ref[...]) * softmax_scale + wide
    own = dot_t(query, own_ref[...]) * softmax_scale
    mine = iota(*own.shape, 0) // heads == iota(*own.shape, 1)
    own = jnp.sum(jnp.where(mine, own, 0.0), axis=1, keepdims=True)
    own = jnp.where(index == 0, own, MASKED)
    peak = jnp.maximum(jnp.max(scores, axis=1, keepdims=True), own)
    weights = jnp.where(wide < 0.0, 0.0, jnp.exp(scores - peak))
    own_weight = jnp.where(index == 0, jnp.exp(own - peak), 0.0)
    total = jnp.sum(weights, axis=1, keepdims=True) + own_weight
    out = dot_n(weights.astype(BF16), rows_ref[:, :KVL])
    own_rows = own_ref[:, :KVL].astype(F32)
    latent = jnp.concatenate(
        [jnp.broadcast_to(own_rows[r : r + 1], (heads, KVL)) for r in range(requests)], axis=0
    )
    pack((out + own_weight * latent) / total, peak + jnp.log(total), packed_ref)

    width = bias_ref.shape[1]
    half = pages // 2
    spot = iota(1, width, 1) // PAGE
    place = spot % half
    taker = jnp.where(spot // pages == 1, 1 - core, core)
    which = (place // (half // 2)) * half + taker * (half // 2) + place % (half // 2)
    partner = (spot % pages) // half == 1
    line = iota(base, width, 0)
    plan = jnp.where(partner, columns[n - 1][:base, :], columns[0][:base, :])
    plan = jnp.where(line % 2 == 1, plan, plan * (2 * slots))
    code = jnp.sum(jnp.where(line // 2 == which, plan, 0), axis=0, keepdims=True)
    limit = jnp.zeros((1, width), jnp.int32)
    reader = jnp.zeros((1, width), jnp.int32)
    for s in range(n):
        owner = (index + s) % n
        hit = columns[s][base : base + slots, :] + owner * (2 * slots) == code
        limit = limit + lookup(hit, limits(columns[s]))
        reader = reader + lookup(hit, readers)
    limit = jnp.where(index % 2 == 1, limit, 0)
    live = (iota(1, width, 1) % PAGE) < limit
    bias_ref[...] = jnp.where(live & (reader == iota(8, width, 0)), 0.0, MASKED)


def lane_rows(ids, block):
    half = block.shape[0] // 2
    top, bottom = block[:half], block[half:]
    stage = ids[3]
    return jnp.where(stage == 0, top, bottom), jnp.where(stage == 0, bottom, top)


def cross_kernel(cols, part, ids, kept, got, send, keep):
    odd = ids[2] % 2 == 1
    both = kept[...] + got[...]
    for c in range(both.shape[0] // part):
        at = slice(c * part, (c + 1) * part)
        block = both[at, :cols]
        mine, away = lane_rows(ids, block)
        keep[at, :cols] = jnp.where(odd, block, jnp.concatenate([mine, mine], axis=0))
        send[at, :cols] = jnp.where(odd, block, jnp.concatenate([away, away], axis=0))
    if both.shape[1] > cols:
        keep[:, cols:] = both[:, cols:]
        send[:, cols:] = both[:, cols:]


def cross_rest_kernel(
    head, rest, keys, ids, kept_tail, got_tail, kept_head, got_head, kept_last, got_last, send, keep
):
    cols = send.shape[1]
    part = kept_head.shape[0] // 2
    half = part // 2
    for i in range(4):
        side, c = divmod(i, 2)
        rows = slice(c * part, (c + 1) * part)
        start = side * (kept_head.shape[1] - head)
        at = slice(start, start + head)
        first = kept_head[rows, at] + got_head[rows, at]
        start = side * (kept_tail.shape[1] - rest)
        at = slice(start, start + rest)
        second = kept_tail[rows, at] + got_tail[rows, at]
        at = slice(cols + i * keys, cols + (i + 1) * keys)
        third = kept_last[:, at] + got_last[:, at]
        mine, away = lane_rows(ids, jnp.concatenate([first, second, third], axis=1))
        at = slice(i * half, (i + 1) * half)
        keep[at, :] = mine
        send[at, :] = away.astype(BF16)


def keys_kernel(keys, keep0, got0, keep1, got1, keep2, got2, cos, sin, turn, gain, out):
    cols = keep0.shape[1]
    part = keep1.shape[0]
    for i in range(4):
        last = slice(cols + i * keys, cols + (i + 1) * keys)
        tail = keep2[:, last] + got2[:, last]
        keep, got = ((keep0, got0), (keep0, got0), (keep1, got1), (keep2, got2))[i]
        rows = slice(part, 2 * part) if i == 1 else slice(0, part)
        block = keep[rows, :cols] + got[rows, :cols]
        raw = jnp.concatenate([tail, block], axis=1)
        at = slice(i * part, (i + 1) * part)
        latent = raw[:, :KVL]
        inverse = lax.rsqrt(jnp.sum(latent * latent, axis=1, keepdims=True) / KVL + norm_eps)
        out[at, :KVL] = (latent * inverse * gain[...]).astype(BF16)
        rope = raw[:, KVL:]
        partner = dot_n(rope, turn[...], precision=lax.Precision.HIGHEST)
        out[at, KVL:] = (rope * cos[at, :] + partner * sin[at, :]).astype(BF16)


def pack(out, level, *packed_refs):
    lead = level.astype(BF16).astype(F32)
    rest = (level - lead).astype(BF16).astype(F32)
    last = level - lead - rest
    lane = lax.broadcasted_iota(jnp.int32, (out.shape[0], 128), 1)
    tail = jnp.where(lane == 0, lead, jnp.where(lane == 1, rest, jnp.where(lane == 2, last, 0.0)))
    for packed_ref in packed_refs:
        packed_ref[:, :KVL] = out.astype(packed_ref.dtype)
        packed_ref[:, KVL:] = tail.astype(packed_ref.dtype)


def unpack(packed):
    level = jnp.sum(packed[:, KVL:].astype(F32), axis=1, keepdims=True)
    return packed[:, :KVL].astype(F32), level


def attend_kernel(query_ref, k0_ref, k1_ref, bias_ref, old_ref, far_ref, own_ref, packed_ref):
    query = query_ref[...]
    keys = k0_ref.shape[0]
    requests = bias_ref.shape[0] // 2
    heads = query.shape[0] // requests
    bias = bias_ref[...]
    wide = jnp.concatenate(
        [jnp.broadcast_to(bias[r : r + 1], (heads, 2 * keys)) for r in range(requests)], axis=0
    )
    scores = jnp.concatenate([dot_t(query, k0_ref[...]), dot_t(query, k1_ref[...])], axis=1)
    scores = scores * softmax_scale + wide
    old, old_level = unpack(old_ref[...])
    far, far_level = unpack(far_ref[...])
    peak = jnp.maximum(old_level, far_level)
    peak = jnp.maximum(peak, jnp.max(scores, axis=1, keepdims=True))
    weights = jnp.where(wide < 0.0, 0.0, jnp.exp(scores - peak))
    old_share, far_share = jnp.exp(old_level - peak), jnp.exp(far_level - peak)
    total = jnp.sum(weights, axis=1, keepdims=True) + old_share + far_share
    rounded = weights.astype(BF16)
    out = dot_n(rounded[:, :keys], k0_ref[:, :KVL]) + dot_n(rounded[:, keys:], k1_ref[:, :KVL])
    out = out + old * old_share + far * far_share
    pack(out / total, peak + jnp.log(total), own_ref, packed_ref)


def combine_kernel(own, across, out):
    first, level = unpack(own[...])
    second, other_level = unpack(across[...])
    top = jnp.maximum(level, other_level)
    share, other_share = jnp.exp(level - top), jnp.exp(other_level - top)
    out[...] = ((first * share + second * other_share) / (share + other_share)).astype(BF16)


def return_first_kernel(keep0, got0, keep1, got1, keep2, got2, low, send):
    rows, cols = low.shape
    half = rows // 2
    part = keep1.shape[0]
    for c, (keep, got) in enumerate(((keep1, got1), (keep2, got2))):
        at, near = slice(c * half, (c + 1) * half), slice(c * part, c * part + half)
        low[at, :] = keep0[near, :] + got0[near, :]
        send[at, :] = (keep[:half, :cols] + got[:half, :cols]).astype(BF16)


def return_second_kernel(keep, got, high, send):
    rows = high.shape[0]
    both = keep[...] + got[...].astype(F32)
    high[...] = both[:rows]
    send[...] = both[rows:].astype(BF16)


def query_kernel(ids, low, high, got_first, got_second, gain, *refs):
    sends, scratch = refs[:-1], refs[-1]
    odd = ids[2] % 2 == 1
    cols = low.shape[1]
    cut = QL - 2 * cols
    got_low, got_high = got_first[...].astype(F32), got_second[...].astype(F32)
    first = jnp.where(odd, got_low, low[...])
    second = jnp.where(odd, got_high, high[...])
    third = jnp.where(odd, high[:, :cut], got_high[:, :cut])
    rows = jnp.concatenate([first, second, third], axis=1)
    inverse = lax.rsqrt(jnp.sum(rows * rows, axis=1, keepdims=True) / QL + norm_eps)
    rows = (rows * inverse * gain[...]).astype(BF16)
    scratch[...] = rows
    width = QL // len(sends)
    lane = 2 * ids[3] + ids[1]
    for k, send in enumerate(sends):
        target = jnp.bitwise_xor(lane, k)
        send[...] = scratch[:, pl.ds(pl.multiple_of(target * width, 128), width)]


def place_kernel(ids, *refs):
    gots, out = refs[:-1], refs[-1]
    half = gots[0].shape[0] // 2
    chunk = out.shape[0] // 2
    lane = 2 * ids[3] + ids[1]
    for k, got in enumerate(gots):
        source = jnp.bitwise_xor(lane, k)
        start = (source % 2) * (2 * half) + (source // 2) * half
        for c in range(2):
            at = pl.ds(pl.multiple_of(c * chunk + start, 16), half)
            out[at, :] = got[c * half : (c + 1) * half, :]


def call(kernel, shapes, specs, args, scratch=()):
    return pl.pallas_call(
        kernel,
        scratch_shapes=scratch,
        out_shape=shapes,
        in_specs=specs,
        out_specs=[VMEM] * len(shapes) if isinstance(shapes, list) else VMEM,
        cost_estimate=pl.CostEstimate(flops=20_000_000, bytes_accessed=2_000_000, transcendentals=0),
        compiler_params=pltpu.CompilerParams(vmem_limit_bytes=VMEM_GRANT),
    )(*args)


def shaped(*dims, kind=F32):
    return jax.ShapeDtypeStruct(dims, kind)


def body_pairs(*args):
    return pairs_step(*args)


def pairs_step(
    hidden_x,
    proj_weight,
    q_gain,
    kv_gain,
    old_cache,
    page_plan,
    block_table,
    split_lens,
    dec_query,
    new_key,
):
    n = lax.axis_size(DEC)
    group, index = lax.axis_index(GRP), lax.axis_index(DEC)
    stage, core = lax.axis_index(STG), lax.axis_index(TP)
    ids = jnp.stack([group, core, index, stage]).astype(jnp.int32)
    tokens, feats = hidden_x.shape
    cols = proj_weight.shape[1]
    cut = QL - 2 * cols
    half = feats // 2
    pages = page_plan.shape[0]
    requests, heads, _ = dec_query.shape
    queries = requests * heads
    rows = tokens // 2
    quarter = rows // 2

    weight = proj_weight.T
    split = cols // 2 // 128 * 128
    pieces = [
        lax.dynamic_slice(weight, (0, group * half), (split, half)),
        lax.dynamic_slice(weight, (split, group * half), (cols - split, half)),
    ]
    partners = [(0, 1), (1, 0), (2, 3), (3, 2)]
    a_z, a_y, b_z, b_y = [None] * 2, [None] * 2, [None] * 3, [None] * 3
    for p in (1, 0):
        a_z[p] = lax.ppermute(pieces[p], DEC, [(0, 2), (3, 1), (1, 0), (2, 3)])
    packed = jnp.concatenate(
        [page_plan.reshape(-1), block_table.reshape(-1), split_lens.reshape(-1)]
    ).reshape(1, -1)
    tables = [packed]
    for s in range(1, n):
        tables.append(lax.ppermute(packed, DEC, [((i + s) % n, i) for i in range(n)]))
    tables = jnp.pad(
        jnp.concatenate(tables, axis=0), ((0, 8 - n), (0, -packed.shape[1] % 128))
    )
    x_far = []
    for c in range(2):
        x_far.append(lax.ppermute(hidden_x[c * rows : (c + 1) * rows], DEC, partners))
    middle = (cols - split) * 3 // 10 // 16 * 16
    held = lax.optimization_barrier((pieces[0], pieces[1][middle:], pieces[1][:middle], a_z[0]))
    for p in (1, 0):
        a_y[p] = swap(a_z[p], GRP)
    for p in (1, 2, 0):
        b_z[p] = lax.ppermute(held[p], DEC, [(1, 2), (2, 1)])
        b_y[p] = swap(b_z[p], GRP)

    query = dec_query.reshape(queries, KVW)
    padded_key = jnp.pad(new_key, ((0, 3 * requests), (0, 0)))
    old, bias = call(
        functools.partial(old_kernel, n, pages),
        [shaped(queries, KVL + 128), shaped(8, 2 * tokens)],
        [SMEM, VMEM, VMEM, VMEM, VMEM],
        (ids, tables, query, old_cache.reshape(-1, KVW), padded_key),
    )

    old_far = lax.ppermute(old, DEC, partners)

    partner = index + 1 - 2 * (index % 2)
    place = jnp.arange(rows, dtype=jnp.int32)
    place = place + core * quarter + (place // quarter) * quarter
    positions = jnp.concatenate([index * tokens + place, partner * tokens + place]).astype(F32)
    pair = jnp.arange(ROPE, dtype=jnp.int32) // 2
    frequency = jnp.power(F32(10000.0), -(2 * pair).astype(F32) / ROPE)
    angles = positions[:, None] * frequency[None, :]
    turn = call(turn_kernel, shaped(ROPE, ROPE), [], ())
    early_ids, cos, sin, turn, kv_scale, q_scale = lax.optimization_barrier(
        (ids, jnp.cos(angles), jnp.sin(angles), turn, kv_gain.reshape(1, -1), q_gain.reshape(1, -1))
    )

    a_refs = (a_z[0], a_y[0], a_z[1], a_y[1])
    keys = cols - cut

    def crossed(kernel, count, width, args):
        send, kept = project(kernel, count, width, args)
        other = swap(send, TP)
        send, keep = call(
            functools.partial(cross_kernel, cols, quarter),
            [shaped(count, width)] * 2,
            [SMEM, VMEM, VMEM],
            (ids, kept, other),
        )
        return (keep, swap(send, STG)), (kept, other)

    near, _ = crossed(
        functools.partial(primary_kernel, rows), rows, cols, (early_ids, hidden_x, weight, *a_refs)
    )
    far, _ = crossed(
        functools.partial(primary_kernel, rows), quarter, cols, (ids, x_far[0], weight, *a_refs)
    )
    last, last_sums = crossed(
        functools.partial(last_kernel, rows, keys),
        quarter,
        cols + 4 * keys,
        (ids, hidden_x, *x_far, weight, *a_refs, b_z[1], b_y[1]),
    )
    used = (cols - split - keys, split)
    b_parts = ((b_z[0], b_y[0]), (b_z[2], b_y[2], b_z[1], b_y[1]))
    rest = []
    for k, p in enumerate((1, 0)):
        send, kept = project(
            functools.partial(rest_kernel, rows, used[k]),
            rows,
            -(-used[k] // 128) * 128 + used[k],
            (ids, hidden_x, *x_far, a_z[p], a_y[p], *b_parts[p]),
            scratch=[pltpu.VMEM((tokens, feats), BF16)],
        )
        rest += [kept, swap(send, TP)]
    send2, keep2 = call(
        functools.partial(cross_rest_kernel, split, used[0], keys),
        [shaped(rows, cols, kind=BF16), shaped(rows, cols)],
        [SMEM] + [VMEM] * 6,
        (ids, *rest, *last_sums),
    )
    got2 = swap(send2, STG)

    key_rows = call(
        functools.partial(keys_kernel, keys),
        shaped(tokens, KVW, kind=BF16),
        [VMEM] * 10,
        (*near, *far, *last, cos, sin, turn, kv_scale),
    )
    far_keys = swap(key_rows, TP)
    own_out, part_out = call(
        attend_kernel,
        [shaped(queries, KVL + 128), shaped(queries, KVL + 128, kind=BF16)],
        [VMEM] * 6,
        (query, key_rows, far_keys, bias, old, old_far),
    )
    across = lax.ppermute(part_out, DEC, [(1, 3), (3, 1)])
    merged = call(combine_kernel, shaped(queries, KVL, kind=BF16), [VMEM] * 2, (own_out, across))
    given = lax.ppermute(merged, DEC, partners)
    attn = jnp.where(index % 2 == 1, merged, given)

    low, back0 = call(
        return_first_kernel,
        [shaped(quarter, cols), shaped(quarter, cols, kind=BF16)],
        [VMEM] * 6,
        (*near, *far, *last),
    )
    back0 = lax.ppermute(back0, DEC, partners)
    high, back1 = call(
        return_second_kernel,
        [shaped(quarter, cols), shaped(quarter, cols, kind=BF16)],
        [VMEM] * 2,
        (keep2, got2),
    )
    back1 = lax.ppermute(back1, DEC, partners)
    lanes = 4
    width = QL // lanes
    tile = shaped(quarter, width, kind=BF16)
    blocks = call(
        query_kernel,
        [tile] * lanes,
        [SMEM] + [VMEM] * 5,
        (ids, low, high, back0, back1, q_scale),
        scratch=[pltpu.VMEM((quarter, QL), BF16)],
    )
    gots = [blocks[0]]
    for k in range(1, lanes):
        gots.append(lax.ppermute(blocks[k], (STG, TP), [(i, i ^ k) for i in range(lanes)]))
    q_latent = call(
        place_kernel, shaped(tokens, width, kind=BF16), [SMEM] + [VMEM] * lanes, (ids, *gots)
    )
    return (q_latent, attn.reshape(requests, heads, KVL))


def solution(mesh):
    sizes = dict(mesh.shape)
    pairs = sizes["dec"] == 4 and sizes["grp"] == sizes["stg"] == sizes["tp"] == 2
    return jax.shard_map(
        body_pairs if pairs else body_general,
        mesh=mesh,
        in_specs=(
            P(("grp", "dec"), ("stg", "tp")),
            P(("stg", "tp"), "dec"),
            P(),
            P(),
            P(("grp", "dec"), None, None),
            P(("grp", "dec"), None),
            P(("grp", "dec"), None, None),
            P("grp", "dec"),
            P("grp", ("stg", "tp"), None),
            P("grp", None),
        ),
        out_specs=(P(("grp", "dec"), ("stg", "tp")), P("grp", ("stg", "tp"), None)),
        check_vma=False,
    )
```
